32 devices in a mesh: replica: 8 (over y, x, core), shard: 4 (over z).
Axes of the slice: x: 2, y: 2, z: 4, core: 2. Of those that a mesh axis runs over, the one named last changes fastest.
Arguments:
- tokens: bfloat16 [16384, 1024], P(('replica', 'shard')), may hold values from -16 to 16
- cotangent: bfloat16 [16384, 1024], P(('replica', 'shard')), may hold values from -6 to 6
- seg_ids: int32 [16384], P(('replica', 'shard')), may hold values from -1 to 3, as said below
- qkv_weight: float32 [1024, 3072], P('shard'), may hold values from -1 to 1
- out_weight: float32 [1024, 1024], P('shard'), may hold values from -0.5 to 0.5
- up_weight: float32 [1024, 4096], P('shard'), may hold values from -0.1875 to 0.1875
- down_weight: float32 [4096, 1024], P('shard'), may hold values from -0.09375 to 0.09375
- vectors: float32 [13312], P('shard'), may hold values from -2 to 2
- qkv_moments: float32 [2, 1024, 3072], P(None, 'shard'), may hold values from -1 to 1, as said below
- out_moments: float32 [2, 1024, 1024], P(None, 'shard'), may hold values from -1 to 1, as said below
- up_moments: float32 [2, 1024, 4096], P(None, 'shard'), may hold values from -1 to 1, as said below
- down_moments: float32 [2, 4096, 1024], P(None, 'shard'), may hold values from -1 to 1, as said below
- vector_moments: float32 [2, 13312], P(None, 'shard'), may hold values from -1 to 1, as said below
Outputs:
- block_output: bfloat16 [16384, 1024], P(('replica', 'shard'))
- input_grad: bfloat16 [16384, 1024], P(('replica', 'shard'))
- qkv_grad: float32 [1024, 3072], P('shard')
- out_grad: float32 [1024, 1024], P('shard')
- up_grad: float32 [1024, 4096], P('shard')
- down_grad: float32 [4096, 1024], P('shard')
- vector_grad: float32 [13312], P('shard')
- updated_qkv: float32 [1024, 3072], P('shard')
- updated_out: float32 [1024, 1024], P('shard')
- updated_up: float32 [1024, 4096], P('shard')
- updated_down: float32 [4096, 1024], P('shard')
- updated_vectors: float32 [13312], P('shard')
- moments_qkv: float32 [2, 1024, 3072], P(None, 'shard')
- moments_out: float32 [2, 1024, 1024], P(None, 'shard')
- moments_up: float32 [2, 1024, 4096], P(None, 'shard')
- moments_down: float32 [2, 4096, 1024], P(None, 'shard')
- moments_vector: float32 [2, 13312], P(None, 'shard')
The draws below stay inside these ranges and needn't reach their ends.
Inputs may be any that keep to these rules, and one draw needn't show every extreme that they name: `seg_ids`: within each device's block of 512 slots the live tokens come first and carry document ids that never fall, the last live token in document 4 - 1; the rest of the block is padding with id -1. Every block has at least 128 live tokens; some block has no padding and some has exactly 128 live tokens. `qkv_moments`: entry 0 along the first dimension is the first moment, entry 1 the second moment, which is positive. `out_moments`: entry 0 along the first dimension is the first moment, entry 1 the second moment, which is positive. `up_moments`: entry 0 along the first dimension is the first moment, entry 1 the second moment, which is positive. `down_moments`: entry 0 along the first dimension is the first moment, entry 1 the second moment, which is positive. `vector_moments`: entry 0 along the first dimension is the first moment, entry 1 the second moment, which is positive.
All inputs are finite; a program needn't handle non-finite values.
Results may differ from the reference program's by a relative error of at most 0.024.
Values may be sent and summed in bfloat16 or wider, within the bound.
A program may use at most 256 MiB of HBM per device.

```python
import math
import jax
import jax.numpy as jnp
from jax import lax

D = 1024
H = 4
HD = 256
ROT = 64
FF = 4096
TOK_DEV = 512
DOCS = 4
STEP = 3
HH = 1024
VEC = 13312
TOKENS = 16384


def draw_tokens(key, part):
    subkeys = jax.random.split(jax.random.fold_in(key, 11), 1)
    values = jnp.clip(jax.random.normal(subkeys[0], (TOKENS, D), jnp.float32), -6.0, 6.0)
    return values.astype(jnp.bfloat16)


def draw_seg_ids(key, part):
    subkeys = jax.random.split(jax.random.fold_in(key, 17), 2)
    blocks = TOKENS // TOK_DEV
    fill_level = jax.random.randint(subkeys[0], (blocks,), 0, 17)
    fill_level = fill_level.at[0].set(16).at[1].set(0)
    quarter = TOK_DEV // 4
    live_count = quarter + (TOK_DEV - quarter) * fill_level * fill_level // 256
    cut_points = jax.random.randint(subkeys[1], (blocks, DOCS - 1), 1, live_count[:, None])
    indices = jnp.arange(TOK_DEV)
    doc_ids = jnp.sum((cut_points[:, None, :] <= indices[None, :, None]).astype(jnp.int32), axis=2)
    doc_ids = jnp.where(indices[None, :] < live_count[:, None], doc_ids, -1)
    return doc_ids.reshape(TOKENS).astype(jnp.int32)


def draw_qkv_weight(key, part):
    subkeys = jax.random.split(jax.random.fold_in(key, 23), 1)
    weight = jnp.clip(jax.random.normal(subkeys[0], (D, 3 * HH), jnp.float32), -6.0, 6.0) * D ** (-0.5)
    return weight


def draw_vectors(key, part):
    subkeys = jax.random.split(jax.random.fold_in(key, 37), 2)
    indices = jnp.arange(VEC)
    is_gain = (indices < D) | (indices >= 2 * D) & (indices < 3 * D)
    gain_draw = jax.random.uniform(subkeys[0], (VEC,), jnp.float32, 0.6, 1.4)
    biases = 0.2 * jnp.clip(jax.random.normal(subkeys[1], (VEC,), jnp.float32), -6.0, 6.0)
    return jnp.where(is_gain, gain_draw, biases)


def moment_pair(key, stream_id, array_shape):
    subkeys = jax.random.split(jax.random.fold_in(key, stream_id), 2)
    first_moment = 0.03 * jnp.clip(jax.random.normal(subkeys[0], array_shape, jnp.float32), -6.0, 6.0)
    second_moment = jnp.exp(jax.random.uniform(subkeys[1], array_shape, jnp.float32, math.log(0.001), math.log(0.01)))
    return jnp.stack([first_moment, second_moment])


def draw_qkv_moments(key, part):
    return moment_pair(key, 41, (D, 3 * HH))


def draw_out_moments(key, part):
    return moment_pair(key, 43, (HH, D))


def draw_up_moments(key, part):
    return moment_pair(key, 47, (D, FF))


def draw_down_moments(key, part):
    return moment_pair(key, 53, (FF, D))


def draw_vector_moments(key, part):
    return moment_pair(key, 59, (VEC,))


def level_of(key, extent, cuts, low, high):
    loudness, own = 1.0, jax.random.fold_in(key, 6)
    for axis_at, blocks in cuts:
        steps = jnp.exp(jax.random.uniform(jax.random.fold_in(own, axis_at), (blocks,), jnp.float32, low / len(cuts), high / len(cuts)))
        loudness = loudness * jnp.repeat(steps, extent[axis_at] // blocks).reshape([-1 if axis == axis_at else 1 for axis in range(len(extent))])
    return loudness


def bell_draw(key, shape, scale, limit, cuts=(), held_as=jnp.bfloat16):
    factor_of = level_of(key, shape, cuts, -0.22, 0.18) if cuts else 1.0
    drawn = jax.random.normal(key, shape, jnp.float32) * scale * factor_of
    return jnp.minimum(jnp.maximum(drawn, -limit), limit).astype(held_as)


def setup_inputs(seed: int = 0) -> dict:
    arg_keys = jax.random.split(jax.random.key(seed), 14)
    return {
        "tokens": draw_tokens(jax.random.fold_in(arg_keys[13], 71), 0),
        "cotangent": bell_draw(arg_keys[1], (TOKENS, D), 1.0, 6.0, ((0, 32),)),
        "seg_ids": draw_seg_ids(jax.random.fold_in(arg_keys[13], 71), 0),
        "qkv_weight": draw_qkv_weight(jax.random.fold_in(arg_keys[13], 71), 0),
        "out_weight": bell_draw(arg_keys[4], (HH, D), (HH // 8) ** -0.5, 0.5, ((0, 4),), jnp.float32),
        "up_weight": bell_draw(arg_keys[5], (D, FF), D ** -0.5, 0.1875, ((0, 4),), jnp.float32),
        "down_weight": bell_draw(arg_keys[6], (FF, D), FF ** -0.5, 0.09375, ((0, 4),), jnp.float32),
        "vectors": draw_vectors(jax.random.fold_in(arg_keys[13], 71), 0),
        "qkv_moments": draw_qkv_moments(jax.random.fold_in(arg_keys[13], 71), 0),
        "out_moments": draw_out_moments(jax.random.fold_in(arg_keys[13], 71), 0),
        "up_moments": draw_up_moments(jax.random.fold_in(arg_keys[13], 71), 0),
        "down_moments": draw_down_moments(jax.random.fold_in(arg_keys[13], 71), 0),
        "vector_moments": draw_vector_moments(jax.random.fold_in(arg_keys[13], 71), 0),
    }


norm_eps = 1e-05
rope_base = 10000.0
learn_rate = 0.01
beta_first = 0.9
beta_second = 0.95
adam_eps = 1e-08
weight_decay = 0.1
root_half = 0.7071067811865476
inv_root_tau = 0.3989422804014327

def contract(einsum_form, left_side, right_side):
    return jnp.einsum(einsum_form, left_side.astype(jnp.float32), right_side.astype(jnp.float32), precision=lax.Precision.HIGHEST)

def split_vector(vector, model_width, inner_width, hidden_units):
    widths = [model_width, model_width, model_width, model_width, 3 * inner_width, model_width, hidden_units, model_width]
    pieces = []
    offset = 0
    for piece_width in widths:
        pieces.append(vector[offset:offset + piece_width])
        offset = offset + piece_width
    return pieces

def gelu_parts(hidden_pre):
    cumulative = 0.5 * (1.0 + lax.erf(hidden_pre * root_half))
    density = jnp.exp(-0.5 * hidden_pre * hidden_pre) * inv_root_tau
    return (hidden_pre * cumulative, cumulative + hidden_pre * density)

def rotary_tables(segment):
    row_count = segment.shape[0]
    indices = jnp.arange(row_count)
    same_doc = segment[:, None] == segment[None, :]
    earlier = indices[None, :] < indices[:, None]
    position = lax.optimization_barrier(jnp.sum((same_doc & earlier).astype(jnp.int32), axis=1))
    half_rot = ROT // 2
    frequency = rope_base ** (-2.0 * jnp.arange(half_rot).astype(jnp.float32) / ROT)
    angles = position.astype(jnp.float32)[:, None] * frequency[None, :]
    return (jnp.cos(angles), jnp.sin(angles))

def rotate(tensor, cosine_tab, sine_tab):
    half_rot = cosine_tab.shape[1]
    lower_half = tensor[..., :half_rot]
    upper_half = tensor[..., half_rot:2 * half_rot]
    remain = tensor[..., 2 * half_rot:]
    cos_rows = cosine_tab[:, None, :]
    sin_rows = sine_tab[:, None, :]
    return jnp.concatenate([lower_half * cos_rows - upper_half * sin_rows, upper_half * cos_rows + lower_half * sin_rows, remain], axis=-1)

def unrotate(tensor, cosine_tab, sine_tab):
    half_rot = cosine_tab.shape[1]
    lower_half = tensor[..., :half_rot]
    upper_half = tensor[..., half_rot:2 * half_rot]
    remain = tensor[..., 2 * half_rot:]
    cos_rows = cosine_tab[:, None, :]
    sin_rows = sine_tab[:, None, :]
    return jnp.concatenate([lower_half * cos_rows + upper_half * sin_rows, upper_half * cos_rows - lower_half * sin_rows, remain], axis=-1)

def allowed_rows(segment, offset, block_rows):
    row_seg = lax.dynamic_slice_in_dim(segment, offset, block_rows, 0)
    row_ids = offset + jnp.arange(block_rows).astype(jnp.int32)
    col_ids = jnp.arange(segment.shape[0]).astype(jnp.int32)
    return (row_seg[:, None] == segment[None, :]) & (col_ids[None, :] <= row_ids[:, None])

def attend(queries, keys_in, values_in, segment, score_scale):
    row_count = queries.shape[0]
    block_rows = min(row_count, 512)
    starts = (jnp.arange(row_count // block_rows) * block_rows).astype(jnp.int32)

    def one_block(offset):
        query_rows = lax.dynamic_slice_in_dim(queries, offset, block_rows, 0)
        allowed = allowed_rows(segment, offset, block_rows)
        scores = contract('thd,uhd->htu', query_rows, keys_in) * score_scale
        masked = jnp.where(allowed[None], scores, -jnp.inf)
        largest = lax.optimization_barrier(jnp.max(masked, axis=-1, keepdims=True))
        summed = lax.optimization_barrier(jnp.sum(jnp.exp(masked - largest), axis=-1, keepdims=True))
        log_total = largest + jnp.log(summed)
        prob_half = jnp.exp(masked - log_total).astype(jnp.bfloat16)
        context = contract('htu,uhd->thd', prob_half, values_in).astype(jnp.bfloat16)
        return (context, log_total)
    contexts, log_totals = lax.map(one_block, starts)
    return (contexts.reshape(queries.shape), log_totals)

def attend_back(queries, keys_in, values_in, grad_context, log_totals, segment, score_scale):
    row_count = queries.shape[0]
    block_rows = min(row_count, 512)
    starts = (jnp.arange(row_count // block_rows) * block_rows).astype(jnp.int32)

    def one_block(running, element):
        offset, log_total = element
        query_rows = lax.dynamic_slice_in_dim(queries, offset, block_rows, 0)
        grad_rows = lax.dynamic_slice_in_dim(grad_context, offset, block_rows, 0)
        allowed = allowed_rows(segment, offset, block_rows)
        scores = contract('thd,uhd->htu', query_rows, keys_in) * score_scale
        prob_exact = jnp.exp(jnp.where(allowed[None], scores, -jnp.inf) - log_total)
        prob_half = prob_exact.astype(jnp.bfloat16)
        grad_prob = contract('thd,uhd->htu', grad_rows, values_in)
        row_delta = lax.optimization_barrier(jnp.sum(prob_exact * grad_prob, axis=-1, keepdims=True))
        grad_score = (prob_exact * (grad_prob - row_delta) * score_scale).astype(jnp.bfloat16)
        grad_query = contract('htu,uhd->thd', grad_score, keys_in)
        grad_keys = running[0] + contract('htu,thd->uhd', grad_score, query_rows)
        grad_values = running[1] + contract('htu,thd->uhd', prob_half, grad_rows)
        return ((grad_keys, grad_values), grad_query)
    zero_fill = jnp.zeros(keys_in.shape, jnp.float32)
    (grad_keys, grad_values), grad_queries = lax.scan(one_block, (zero_fill, zero_fill), (starts, log_totals))
    return (grad_queries.reshape(queries.shape), grad_keys, grad_values)

def forward_pass(tokens, segment, weights):
    qkv_half, out_half, up_half, down_half, vector_half = weights
    model_width = tokens.shape[1]
    inner_width = out_half.shape[0]
    hidden_units = up_half.shape[1]
    pieces = [member.astype(jnp.float32) for member in split_vector(vector_half, model_width, inner_width, hidden_units)]
    gain_one, bias_one, gain_two, bias_two, qkv_bias, out_bias, up_bias, down_bias = pieces
    inputs = tokens.astype(jnp.float32)
    average = lax.optimization_barrier(jnp.mean(inputs, axis=1, keepdims=True))
    centred = inputs - average
    inverse = lax.rsqrt(lax.optimization_barrier(jnp.mean(centred * centred, axis=1, keepdims=True)) + norm_eps)
    normed = centred * inverse
    attn_in = (normed * gain_one + bias_one).astype(jnp.bfloat16)
    mlp_in = (normed * gain_two + bias_two).astype(jnp.bfloat16)
    projected = contract('td,df->tf', attn_in, qkv_half) + qkv_bias
    row_count = tokens.shape[0]
    shape_heads = (row_count, H, HD)
    cosine_tab, sine_tab = rotary_tables(segment)
    queries = rotate(projected[:, :inner_width].reshape(shape_heads), cosine_tab, sine_tab).astype(jnp.bfloat16)
    keys_rot = rotate(projected[:, inner_width:2 * inner_width].reshape(shape_heads), cosine_tab, sine_tab).astype(jnp.bfloat16)
    values_in = projected[:, 2 * inner_width:].reshape(shape_heads).astype(jnp.bfloat16)
    context, log_totals = attend(queries, keys_rot, values_in, segment, HD ** (-0.5))
    context_flat = context.reshape(row_count, inner_width)
    attn_out = contract('td,dm->tm', context_flat, out_half) + out_bias
    hidden_pre = contract('td,df->tf', mlp_in, up_half) + up_bias
    gelu_value, gelu_slope = gelu_parts(hidden_pre)
    activated = gelu_value.astype(jnp.bfloat16)
    mlp_out = contract('tf,fm->tm', activated, down_half) + down_bias
    live_rows = (segment >= 0).astype(jnp.float32)[:, None]
    output = (live_rows * (inputs + attn_out + mlp_out)).astype(jnp.bfloat16)
    saved = (normed, inverse, attn_in, mlp_in, queries, keys_rot, values_in, context_flat, log_totals, gelu_slope, activated, cosine_tab, sine_tab)
    return (output, saved)

def backward_pass(cotangent, segment, weights, saved, grad_scale):
    qkv_half, out_half, up_half, down_half, vector_half = weights
    normed, inverse, attn_in, mlp_in, queries, keys_rot, values_in, context_flat, log_totals, gelu_slope, activated, cosine_tab, sine_tab = saved
    model_width = cotangent.shape[1]
    inner_width = out_half.shape[0]
    hidden_units = up_half.shape[1]
    row_count = cotangent.shape[0]
    pieces = split_vector(vector_half, model_width, inner_width, hidden_units)
    gain_one = pieces[0].astype(jnp.float32)
    gain_two = pieces[2].astype(jnp.float32)
    live_half = (segment >= 0).astype(jnp.bfloat16)[:, None]
    grad_out = cotangent * live_half
    grad_exact = grad_out.astype(jnp.float32)
    grad_hidden = contract('tm,fm->tf', grad_out, down_half) * gelu_slope
    grad_hidden_half = grad_hidden.astype(jnp.bfloat16)
    grad_context = contract('tm,dm->td', grad_out, out_half).astype(jnp.bfloat16)
    grad_queries, grad_keys, grad_values = attend_back(queries, keys_rot, values_in, grad_context.reshape(queries.shape), log_totals, segment, HD ** (-0.5))
    grad_query_flat = unrotate(grad_queries, cosine_tab, sine_tab).reshape(row_count, inner_width)
    grad_key_flat = unrotate(grad_keys, cosine_tab, sine_tab).reshape(row_count, inner_width)
    grad_qkv = jnp.concatenate([grad_query_flat, grad_key_flat, grad_values.reshape(row_count, inner_width)], axis=1)
    grad_qkv_half = grad_qkv.astype(jnp.bfloat16)
    grad_attn_in = contract('tf,df->td', grad_qkv_half, qkv_half)
    grad_mlp_in = contract('tf,df->td', grad_hidden_half, up_half)
    grad_normed = grad_attn_in * gain_one + grad_mlp_in * gain_two
    first_mean = lax.optimization_barrier(jnp.mean(grad_normed, axis=1, keepdims=True))
    second_mean = lax.optimization_barrier(jnp.mean(grad_normed * normed, axis=1, keepdims=True))
    grad_input = (grad_exact + inverse * (grad_normed - first_mean - normed * second_mean)).astype(jnp.bfloat16)
    vector_terms = jnp.concatenate([lax.optimization_barrier(jnp.sum(grad_attn_in * normed, axis=0)), lax.optimization_barrier(jnp.sum(grad_attn_in, axis=0)), lax.optimization_barrier(jnp.sum(grad_mlp_in * normed, axis=0)), lax.optimization_barrier(jnp.sum(grad_mlp_in, axis=0)), lax.optimization_barrier(jnp.sum(grad_qkv, axis=0)), lax.optimization_barrier(jnp.sum(grad_exact, axis=0)), lax.optimization_barrier(jnp.sum(grad_hidden, axis=0)), lax.optimization_barrier(jnp.sum(grad_exact, axis=0))]) * grad_scale
    partials = (contract('td,tf->df', attn_in, grad_qkv_half) * grad_scale, contract('td,tm->dm', context_flat, grad_out) * grad_scale, contract('td,tf->df', mlp_in, grad_hidden_half) * grad_scale, contract('tf,tm->fm', activated, grad_out) * grad_scale, vector_terms)
    return (grad_input, partials)

def adam_update(master, moments, gradient, decay_rate):
    first_new = beta_first * moments[0] + (1.0 - beta_first) * gradient
    second_new = beta_second * moments[1] + (1.0 - beta_second) * gradient * gradient
    first_hat = first_new / (1.0 - beta_first ** STEP)
    second_hat = second_new / (1.0 - beta_second ** STEP)
    updated = master - learn_rate * (first_hat / (jnp.sqrt(second_hat) + adam_eps) + decay_rate * master)
    return (updated, jnp.stack([first_new, second_new]))

def reference(tokens, cotangent, seg_ids, qkv_weight, out_weight, up_weight, down_weight, vectors, qkv_moments, out_moments, up_moments, down_moments, vector_moments):
    masters = (qkv_weight, out_weight, up_weight, down_weight, vectors)
    halves = tuple((member.astype(jnp.bfloat16) for member in masters))
    grad_scale = TOKENS ** (-0.5)
    model_width = tokens.shape[1]
    block_count = TOKENS // TOK_DEV
    block_tokens = tokens.reshape(block_count, TOK_DEV, model_width)
    block_cotangent = cotangent.reshape(block_count, TOK_DEV, model_width)
    block_segments = seg_ids.reshape(block_count, TOK_DEV)

    def one_device(running, element):
        token_rows, cotangent_rows, segment_rows = element
        output, saved = forward_pass(token_rows, segment_rows, halves)
        grad_input, partials = backward_pass(cotangent_rows, segment_rows, halves, saved, grad_scale)
        rounded = tuple((lax.optimization_barrier(member.astype(jnp.bfloat16)).astype(jnp.float32) for member in partials))
        running = tuple((so_far + addend for so_far, addend in zip(running, rounded)))
        return (running, (output, grad_input))
    starting = tuple((jnp.zeros(member.shape, jnp.float32) for member in masters))
    summed, (outputs, grad_inputs) = lax.scan(one_device, starting, (block_tokens, block_cotangent, block_segments))
    block_output = outputs.reshape(TOKENS, model_width)
    input_grad = grad_inputs.reshape(TOKENS, model_width)
    moment_list = (qkv_moments, out_moments, up_moments, down_moments, vector_moments)
    decays = (weight_decay, weight_decay, weight_decay, weight_decay, 0.0)
    updated_list = []
    renewed_list = []
    for master, moment, gradient, decay_rate in zip(masters, moment_list, summed, decays):
        updated, renewed = adam_update(master, moment, gradient, decay_rate)
        updated_list.append(updated)
        renewed_list.append(renewed)
    return (block_output, input_grad, summed[0], summed[1], summed[2], summed[3], summed[4], updated_list[0], updated_list[1], updated_list[2], updated_list[3], updated_list[4], renewed_list[0], renewed_list[1], renewed_list[2], renewed_list[3], renewed_list[4])
```

```python
import functools
import math

import jax
import jax.numpy as jnp
from jax import lax
from jax.experimental import pallas as pl
from jax.experimental.pallas import tpu as pltpu
from jax.sharding import PartitionSpec as P

H = 4
ROT = 64
STEP = 3
norm_eps = 1e-05
rope_base = 10000.0
learn_rate = 0.01
beta_first = 0.9
beta_second = 0.95
adam_eps = 1e-08
weight_decay = 0.1
root_half = 0.7071067811865476
inv_root_tau = 0.3989422804014327

MESH = pl.DeviceIdType.MESH
f32, bf16 = jnp.float32, jnp.bfloat16
ANY = pl.BlockSpec(memory_space=pl.ANY)
VMEM = pl.BlockSpec(memory_space=pltpu.VMEM)
DMA = pltpu.SemaphoreType.DMA
TILE = 256
LAG = 2
AHEAD = 3


class Place:
    def __init__(self, replicas, shards):
        self.replicas, self.shards = replicas, shards
        self.steps = int(math.log2(replicas)) - 1
        self.half = 2**self.steps
        self.r = lax.axis_index("replica")
        self.s = lax.axis_index("shard")
        self.core = self.r % 2
        self.m = self.mixed(self.r // 2)
        self.base = self.core * self.half
        self.twin_base = (1 - self.core) * self.half
        self.piece = self.base + self.m
        self.twin = (self.r + 1 - 2 * self.core, self.s)
        self.partner, self.mine, self.theirs = [], [], []
        for k in range(self.steps):
            flip = 2**k
            other = self.m + flip * (1 - 2 * ((self.m // flip) % 2))
            self.partner.append((2 * self.mixed(other) + self.core, self.s))
            self.mine.append((self.m // flip) * flip)
            self.theirs.append((other // flip) * flip)

    def mixed(self, plane):
        n = self.steps
        turned = sum(((plane // 2**i) % 2) * 2 ** (n - 1 - i) for i in range(n))
        return (1 - self.core) * plane + self.core * turned

    def across(self, d):
        return (self.r, (self.s + d) % self.shards)

    def source(self, d):
        return (self.s + self.shards - d) % self.shards

    def greet(self):
        barrier = pltpu.get_barrier_semaphore()
        peers = [self.across(d) for d in range(1, self.shards)] + self.partner + [self.twin]
        for peer in peers:
            pl.semaphore_signal(barrier, inc=1, device_id=peer, device_id_type=MESH)
        pl.semaphore_wait(barrier, len(peers))


def remote(src, dst, send, recv, peer):
    return pltpu.make_async_remote_copy(
        src_ref=src, dst_ref=dst, send_sem=send, recv_sem=recv, device_id=peer, device_id_type=MESH
    )


class Gather:
    def __init__(self, place, wg, send, recv):
        self.p, self.wg, self.send, self.recv = place, wg, send, recv
        self.chunks = wg.shape[0]
        self.rows = wg.shape[2] // place.replicas
        self.stages = place.steps + 2
        self.n = place.shards - 1
        self.units = self.chunks * self.n
        self.ticks = self.units + (self.stages - 1) * LAG

    def span(self, t, shard, first, count):
        start = pl.multiple_of(first * self.rows, self.rows)
        return self.wg.at[t, shard, pl.ds(start, count * self.rows), :]

    def copy(self, stage, t, d):
        p = self.p
        if stage == 0:
            ref, peer = self.span(t, p.s, p.piece, 1), p.across(d)
        elif stage <= p.steps:
            k = stage - 1
            ref, peer = self.span(t, p.source(d), p.base + p.mine[k], 2**k), p.partner[k]
        else:
            ref, peer = self.span(t, p.source(d), p.base, p.half), p.twin
        u = t * self.n + d - 1
        return remote(ref, ref, self.send.at[stage, u], self.recv.at[stage, u], peer)

    def launch(self, t):
        for d in range(1, self.n + 1):
            self.copy(0, t, d).start()

    def ready(self, t):
        return (t + 1) * self.n + (self.stages - 1) * LAG

    def tick(self, u):
        for stage in range(self.stages):
            v = u - stage * LAG

            @pl.when((v >= 0) & (v < self.units))
            def _(stage=stage, v=v):
                t, d = v // self.n, v % self.n + 1
                self.copy(stage, t, d).wait_recv()
                if stage + 1 < self.stages:
                    self.copy(stage + 1, t, d).start()

        @pl.when((u % self.n == self.n - 1) & (u // self.n + AHEAD < self.chunks))
        def _():
            self.launch(u // self.n + AHEAD)

    def finish(self):
        @pl.loop(0, self.chunks)
        def _(t):
            for d in range(1, self.n + 1):
                for stage in range(self.stages):
                    self.copy(stage, t, d).wait_send()


def dot(a, b, dims=((1,), (0,))):
    return lax.dot_general(a, b, (dims, ((), ())), preferred_element_type=f32)


def forward_kernel(
    replicas, shards, hidden, grad_scale,
    own, vec, tok, cot, seg,
    wa, grads, mlp, gmlp, attn_in, normed, inverse, gout, vg, vgrad,
    wg, mlp_in, mlp_in_t, stage_up, stage_down, vsend, vrecv, send, recv, own_sem, out_sem, grad_sem,
):
    p = Place(replicas, shards)
    chunks, _, rows, model = wg.shape
    tokens = tok.shape[0]
    ff_chunks = hidden // model
    tiles = model // TILE
    per_tile = TILE // rows
    o_gain1, o_bias1, o_gain2, o_bias2 = (i * model for i in range(4))
    o_out = 7 * model
    o_up = 8 * model
    o_down = o_up + hidden

    def load(t):
        return pltpu.make_async_copy(own.at[t], wg.at[t, p.s], own_sem.at[t])

    for t in range(chunks):
        load(t).start()
    width = vec.shape[1]

    def slot(shard):
        return vg.at[:, pl.ds(pl.multiple_of(shard * width, 128), width)]

    slot(p.s)[...] = vec[...].astype(bf16).astype(f32)
    p.greet()
    g = Gather(p, wg, send, recv)

    @pl.loop(0, chunks)
    def _(t):
        load(t).wait()

    def vcopy(d):
        return remote(slot(p.s), slot(p.s), vsend.at[d - 1], vrecv.at[d - 1], p.across(d))

    for d in range(1, shards):
        vcopy(d).start()
    for t in range(AHEAD):
        g.launch(t)

    band = 64

    @pl.loop(0, tokens // band)
    def _(i):
        at = pl.ds(pl.multiple_of(i * band, band), band)
        x = tok[at, :].astype(f32)
        mean = jnp.mean(x, axis=1, keepdims=True)
        centred = x - mean
        inv = lax.rsqrt(jnp.mean(centred * centred, axis=1, keepdims=True) + norm_eps)
        inverse[at, :] = inv
        normed[at, :] = centred * inv
        live = (seg[at, :] >= 0).astype(f32)
        gout[at, :] = (cot[at, :].astype(f32) * live).astype(bf16)

    for d in range(1, shards):
        vcopy(d).wait_recv()

    @pl.loop(0, tokens // band)
    def _(i):
        at = pl.ds(pl.multiple_of(i * band, band), band)
        x = normed[at, :]
        attn_in[at, :] = (x * vg[:, o_gain1:o_bias1] + vg[:, o_bias1:o_gain2]).astype(bf16)
        mlp_in[at, :] = (x * vg[:, o_gain2:o_bias2] + vg[:, o_bias2 : 4 * model]).astype(bf16)
        mlp[at, :] = jnp.broadcast_to(vg[:, o_down : o_down + model], (band, model))
        gmlp[at, :] = jnp.zeros((band, model), f32)

    for i in range(tokens // 128):
        at = slice(i * 128, i * 128 + 128)
        mlp_in_t[:, at] = mlp_in[at, :].T

    vgrad[...] = jnp.zeros_like(vgrad)

    first = g.ready(1)

    @pl.loop(0, first)
    def _(u):
        g.tick(u)

    per_j = 2 * g.n

    def grad_out_copy(which, j):
        ref = (stage_up, stage_down)[which]
        return pltpu.make_async_copy(ref.at[j % 2], grads.at[2 * j + which], grad_sem.at[which, j % 2])

    def flat(s0, j):
        return [
            pl.multiple_of((s0 * per_tile + i) * (hidden // shards) + j * rows, rows)
            for i in range(per_tile)
        ]

    @pl.loop(0, ff_chunks * tiles)
    def _(it):
        j, n = it // tiles, it % tiles
        lo, hi = first + (it * per_j) // tiles, first + ((it + 1) * per_j) // tiles

        def maybe(i):
            @pl.when((lo + i < hi) & (lo + i < g.ticks))
            def _():
                g.tick(lo + i)

        most = -(-per_j // tiles)
        cols = pl.ds(pl.multiple_of(n * TILE, TILE), TILE)

        @pl.when((n == 0) & (j >= 2))
        def _():
            grad_out_copy(0, j).wait()
            grad_out_copy(1, j).wait()

        maybe(0)
        up = wg[2 * j, :, :, cols].reshape(model, TILE)
        down = wg[2 * j + 1, pl.ds(n * per_tile, per_tile)].reshape(TILE, model)
        bias = jnp.concatenate([vg[:, pl.ds(o_up + f, rows)] for f in flat(n, j)], axis=1)
        h = dot(mlp_in[...], up) + bias
        cum = 0.5 * (1.0 + lax.erf(h * root_half))
        density = jnp.exp(-0.5 * h * h) * inv_root_tau
        act = (h * cum).astype(bf16)
        gh = dot(gout[...], down, ((1,), (1,))) * (cum + h * density)
        ghh = gh.astype(bf16)
        total = jnp.sum(gh, axis=0, keepdims=True) * grad_scale
        for i, f in enumerate(flat(n, j)):
            vgrad[:, pl.ds(o_up + f, rows)] = total[:, i * rows : (i + 1) * rows]
        for i in range(1, most):
            maybe(i)
        mlp[...] += dot(act, down)
        stage_down[j % 2, pl.ds(n * per_tile, per_tile)] = (
            (dot(act, gout[...], ((0,), (0,))) * grad_scale).astype(bf16).reshape(per_tile, rows, model)
        )
        gmlp[...] += dot(ghh, up, ((1,), (1,)))
        stage_up[j % 2, :, :, cols] = (
            (dot(mlp_in_t[...], ghh) * grad_scale).astype(bf16).reshape(shards, rows, TILE)
        )

        @pl.when(n == tiles - 1)
        def _():
            grad_out_copy(0, j).start()
            grad_out_copy(1, j).start()

    def out(t):
        return pltpu.make_async_copy(wg.at[t], wa.at[t - 2 * ff_chunks], out_sem.at[t - 2 * ff_chunks])

    done = first + ff_chunks * per_j

    @pl.loop(done, g.ticks)
    def _(u):
        g.tick(u)

    for t in range(2 * ff_chunks, chunks):
        out(t).start()

    def column_sums(i, carry):
        at = pl.ds(pl.multiple_of(i * band, band), band)
        gm = gmlp[at, :]
        new = (gm * normed[at, :], gm, gout[at, :].astype(f32))
        return tuple(a + jnp.sum(b, axis=0, keepdims=True) for a, b in zip(carry, new))

    zero = jnp.zeros((1, model), f32)
    sums = lax.fori_loop(0, tokens // band, column_sums, (zero, zero, zero))
    vgrad[:, o_gain2:o_bias2] = sums[0] * grad_scale
    vgrad[:, o_bias2 : 4 * model] = sums[1] * grad_scale
    vgrad[:, o_out : o_out + model] = sums[2] * grad_scale
    vgrad[:, o_down : o_down + model] = sums[2] * grad_scale

    for d in range(1, shards):
        vcopy(d).wait_send()
    g.finish()
    for j in range(max(ff_chunks - 2, 0), ff_chunks):
        grad_out_copy(0, j).wait()
        grad_out_copy(1, j).wait()
    for t in range(2 * ff_chunks, chunks):
        out(t).wait()


def forward_call(mesh, own, vec, tok, cot, seg, hidden, grad_scale):
    replicas, shards = mesh.shape["replica"], mesh.shape["shard"]
    chunks, rows, model = own.shape
    tokens = tok.shape[0]
    stages = int(math.log2(replicas)) + 1
    width = vec.shape[1]
    units = chunks * (shards - 1)
    ff_chunks = hidden // model
    sds = jax.ShapeDtypeStruct
    outs = (
        (sds((chunks - 2 * ff_chunks, shards, rows, model), bf16), ANY),
        (sds((chunks, shards, rows, model), bf16), ANY),
        (sds((tokens, model), f32), VMEM),
        (sds((tokens, model), f32), VMEM),
        (sds((tokens, model), bf16), VMEM),
        (sds((tokens, model), f32), VMEM),
        (sds((tokens, 1), f32), VMEM),
        (sds((tokens, model), bf16), VMEM),
        (sds((1, width * shards), f32), VMEM),
        (sds((1, width * shards), f32), VMEM),
    )
    return pl.pallas_call(
        functools.partial(forward_kernel, replicas, shards, hidden, grad_scale),
        out_shape=[o[0] for o in outs],
        in_specs=[ANY, VMEM, VMEM, VMEM, VMEM],
        out_specs=[o[1] for o in outs],
        scratch_shapes=[
            pltpu.VMEM((chunks, shards, rows, model), bf16),
            pltpu.VMEM((tokens, model), bf16),
            pltpu.VMEM((model, tokens), bf16),
            pltpu.VMEM((2, shards, rows, model), bf16),
            pltpu.VMEM((2, shards, rows, model), bf16),
            DMA((shards - 1,)),
            DMA((shards - 1,)),
            DMA((stages, units)),
            DMA((stages, units)),
            DMA((chunks,)),
            DMA((chunks - 2 * ff_chunks,)),
            DMA((2, 2)),
        ],
        compiler_params=pltpu.CompilerParams(
            collective_id=0, has_side_effects=True, vmem_limit_bytes=60 << 20
        ),
        name="gather_mlp",
    )(own, vec, tok, cot, seg)


def chunked(qkv, out, up, down, rows, model, shards):
    hidden = up.shape[1]
    n = hidden // model
    ups = up.reshape(rows, shards, n, rows).transpose(2, 0, 1, 3).reshape(n, rows, model)
    downs = down.reshape(n, rows, model)
    pairs = jnp.stack([ups, downs], axis=1).reshape(2 * n, rows, model)
    rest = qkv.reshape(rows, 3, model).transpose(1, 0, 2)
    return jnp.concatenate([pairs, rest, out[None]], axis=0)


def unchunked(x, hidden, shards):
    rows, model = x.shape[1:]
    n = hidden // model
    pairs = x[: 2 * n].reshape(n, 2, rows, model)
    up = pairs[:, 0].reshape(n, rows, shards, rows).transpose(1, 2, 0, 3).reshape(rows, hidden)
    down = pairs[:, 1].reshape(n * rows, model)
    qkv = x[2 * n : 2 * n + 3].transpose(1, 0, 2).reshape(rows, 3 * model)
    return qkv, x[2 * n + 3], up, down


def rotary_tables(segment, head):
    count = segment.shape[0]
    index = jnp.arange(count)
    same = segment[:, None] == segment[None, :]
    position = jnp.sum((same & (index[None, :] < index[:, None])).astype(jnp.int32), axis=1)
    half = ROT // 2
    frequency = rope_base ** (-2.0 * jnp.arange(half).astype(f32) / ROT)
    angles = position.astype(f32)[:, None] * frequency[None, :]
    return jnp.cos(angles), jnp.sin(angles)


def rotate(x, cosine, sine, sign):
    half = cosine.shape[1]
    a, b, rest = x[..., :half], x[..., half : 2 * half], x[..., 2 * half :]
    c, s = cosine[:, None, :], sign * sine[:, None, :]
    return jnp.concatenate([a * c - b * s, b * c + a * s, rest], axis=-1)


def attention_xla(wa, attn_in, gout, seg, vg, cosine, sine, tokens, model, grad_scale):
    ein = functools.partial(jnp.einsum, preferred_element_type=f32)
    head = model // H
    wq, wk, wv, wo = (wa[i].reshape(model, model) for i in range(4))
    bias = vg[0, 4 * model : 7 * model]
    shape = (tokens, H, head)
    q = rotate((ein("td,df->tf", attn_in, wq) + bias[:model]).reshape(shape), cosine, sine, 1.0).astype(bf16)
    k = rotate((ein("td,df->tf", attn_in, wk) + bias[model : 2 * model]).reshape(shape), cosine, sine, 1.0).astype(bf16)
    v = (ein("td,df->tf", attn_in, wv) + bias[2 * model :]).reshape(shape).astype(bf16)
    scale = head ** (-0.5)
    idx = jnp.arange(tokens)
    allowed = (seg[:, None] == seg[None, :]) & (idx[None, :] <= idx[:, None])
    masked = jnp.where(allowed[None], ein("thd,uhd->htu", q, k) * scale, -jnp.inf)
    largest = jnp.max(masked, axis=-1, keepdims=True)
    log_total = largest + jnp.log(jnp.sum(jnp.exp(masked - largest), axis=-1, keepdims=True))
    prob = jnp.exp(masked - log_total)
    prob_half = prob.astype(bf16)
    ctx = ein("htu,uhd->thd", prob_half, v).astype(bf16)
    gctx = ein("tm,dm->td", gout, wo).astype(bf16).reshape(shape)
    gp = ein("thd,uhd->htu", gctx, v)
    gs = (prob * (gp - jnp.sum(prob * gp, axis=-1, keepdims=True)) * scale).astype(bf16)
    gq = rotate(ein("htu,uhd->thd", gs, k), cosine, sine, -1.0).reshape(tokens, model)
    gk = rotate(ein("htu,thd->uhd", gs, q), cosine, sine, -1.0).reshape(tokens, model)
    gv = ein("htu,thd->uhd", prob_half, gctx).reshape(tokens, model)
    ctx = ctx.reshape(tokens, model)
    attn_out = ein("td,dm->tm", ctx, wo) + vg[0, 7 * model : 8 * model]
    halves = [x.astype(bf16) for x in (gq, gk, gv)]
    gattn = sum(ein("tf,df->td", x, w) for x, w in zip(halves, (wq, wk, wv)))
    wgrads = [(ein("td,tf->df", attn_in, x) * grad_scale).astype(bf16) for x in halves]
    wgrads.append((ein("td,tm->dm", ctx, gout) * grad_scale).astype(bf16))
    sums = [jnp.sum(x, axis=0) * grad_scale for x in (gq, gk, gv)]
    return attn_out, gattn, wgrads, sums


class Reduce:
    def __init__(self, place, grads, lo, rc, r, rz, total, sems, parts):
        self.p, self.grads, self.lo, self.rc, self.r, self.rz, self.total = place, grads, lo, rc, r, rz, total
        self.csem, self.ksem, self.zsem, self.gsem, self.lsem = sems
        self.parts = parts
        self.cols = total.shape[2] // parts
        self.rows = total.shape[1] // place.replicas
        self.units = total.shape[0] * parts
        self.n = place.shards - 1
        self.stages = 2 * place.steps + 4
        self.ticks = self.units + self.stages - 1

    def where(self, u):
        t, part = u // self.parts, u % self.parts
        return t, pl.ds(pl.multiple_of(part * self.cols, self.cols), self.cols)

    def band(self, first, count):
        return pl.ds(pl.multiple_of(first * self.rows, self.rows), count * self.rows)

    def load(self, u):
        t, cols = self.where(u)
        src = self.grads.at[t, :, self.band(self.p.base, self.p.half), cols]
        return pltpu.make_async_copy(src, self.lo.at[u % 2], self.lsem.at[u % 2])

    def core_copy(self, u):
        t, cols = self.where(u)
        src = self.grads.at[t, :, self.band(self.p.twin_base, self.p.half), cols]
        return remote(src, self.rc.at[u], self.csem.at[0, u], self.csem.at[1, u], self.p.twin)

    def held(self, k):
        p = self.p
        return (self.rc, 0) if k == p.steps else (self.r[k], p.mine[k])

    def plane_copy(self, k, u):
        ref, first = self.held(k + 1)
        src = ref.at[u, :, self.band(self.p.theirs[k] - first, 2**k), :]
        return remote(src, self.r[k].at[u], self.ksem.at[0, k, u], self.ksem.at[1, k, u], self.p.partner[k])

    def shard_copy(self, u, d):
        p = self.p
        to = p.across(d)
        src = self.held(0)[0].at[u, to[1]]
        return remote(src, self.rz.at[u, d - 1], self.zsem.at[0, u, d - 1], self.zsem.at[1, u, d - 1], to)

    def total_copy(self, k, u):
        p = self.p
        t, cols = self.where(u)
        first, count, peer = (
            (p.base + p.mine[k], 2**k, p.partner[k]) if k < p.steps else (p.base, p.half, p.twin)
        )
        ref = self.total.at[t, self.band(first, count), cols]
        return remote(ref, ref, self.gsem.at[0, k, u], self.gsem.at[1, k, u], peer)

    def add(self, stage, u):
        p = self.p
        if stage == 0:
            self.load(u).start()
        elif stage == 1:
            self.core_copy(u).wait_recv()
            self.load(u).wait()
            self.rc[u] = self.rc[u] + self.lo[u % 2]
        elif stage < 2 + p.steps:
            k = p.steps - (stage - 1)
            self.plane_copy(k, u).wait_recv()
            ref, first = self.held(k + 1)
            self.r[k][u] = self.r[k][u] + ref[u, :, self.band(p.mine[k] - first, 2**k), :]
        elif stage == 2 + p.steps:
            for d in range(1, self.n + 1):
                self.shard_copy(u, d).wait_recv()
            acc = self.held(0)[0][u, p.s].astype(f32)
            for d in range(1, self.n + 1):
                acc += self.rz[u, d - 1].astype(f32)
            t, cols = self.where(u)
            self.total[t, self.band(p.piece, 1), cols] = acc.astype(bf16)
        else:
            self.total_copy(stage - 3 - p.steps, u).wait_recv()

    def send(self, stage, u):
        p = self.p
        if stage == 0:
            self.core_copy(u).start()
        elif stage < 1 + p.steps:
            self.plane_copy(p.steps - stage, u).start()
        elif stage == 1 + p.steps:
            for d in range(1, self.n + 1):
                self.shard_copy(u, d).start()
        elif stage < self.stages - 1:
            self.total_copy(stage - 2 - p.steps, u).start()

    def tick(self, u):
        for do in (self.add, self.send):
            for stage in range(self.stages):
                v = u - stage

                @pl.when((v >= 0) & (v < self.units))
                def _(stage=stage, v=v):
                    do(stage, v)

    def finish(self):
        @pl.loop(0, self.units)
        def _(u):
            self.core_copy(u).wait_send()
            for k in range(self.p.steps):
                self.plane_copy(k, u).wait_send()
            for d in range(1, self.n + 1):
                self.shard_copy(u, d).wait_send()
            for k in range(self.p.steps + 1):
                self.total_copy(k, u).wait_send()


PARTS = 2


def reduce_kernel(replicas, shards, grads, vgrad, out, vtotal, lo, rc, *rest):
    steps = int(math.log2(replicas)) - 1
    r, rest = rest[:steps], rest[steps:]
    rz, total, vz, vr, csem, ksem, zsem, gsem, lsem, vsem, wsem, osem = rest
    p = Place(replicas, shards)
    p.greet()
    red = Reduce(p, grads, lo, rc, r, rz, total, (csem, ksem, zsem, gsem, lsem), PARTS)

    @pl.loop(0, red.ticks)
    def _(u):
        red.tick(u)

    red.finish()
    copy = pltpu.make_async_copy(total, out, osem)
    copy.start()
    copy.wait()
    vtotal[...] = vgrad[...]


def reduce_call(mesh, grads, vgrad):
    replicas, shards = mesh.shape["replica"], mesh.shape["shard"]
    chunks, _, rows, model = grads.shape
    steps = int(math.log2(replicas)) - 1
    units, cols, piece = chunks * PARTS, model // PARTS, rows // replicas
    half = 2**steps
    sds = jax.ShapeDtypeStruct
    return pl.pallas_call(
        functools.partial(reduce_kernel, replicas, shards),
        out_shape=[sds((chunks, rows, model), bf16), sds(vgrad.shape, f32)],
        in_specs=[ANY, VMEM],
        out_specs=[ANY, VMEM],
        scratch_shapes=[
            pltpu.VMEM((2, shards, half * piece, cols), bf16),
            pltpu.VMEM((units, shards, half * piece, cols), bf16),
            *(pltpu.VMEM((units, shards, 2**k * piece, cols), bf16) for k in range(steps)),
            pltpu.VMEM((units, shards - 1, piece, cols), bf16),
            pltpu.VMEM((chunks, rows, model), bf16),
            pltpu.VMEM((shards, 1, vgrad.shape[1] // shards), f32),
            pltpu.VMEM((replicas, 1, vgrad.shape[1] // shards), f32),
            DMA((2, units)),
            DMA((2, steps, units)),
            DMA((2, units, shards - 1)),
            DMA((2, steps + 1, units)),
            DMA((2,)),
            DMA((2, shards)),
            DMA((2, replicas)),
            DMA(()),
        ],
        compiler_params=pltpu.CompilerParams(
            collective_id=1, has_side_effects=True, vmem_limit_bytes=60 << 20
        ),
        name="reduce",
    )(grads, vgrad)


def adam(master, moments, gradient, decay):
    first = beta_first * moments[0] + (1.0 - beta_first) * gradient
    second = beta_second * moments[1] + (1.0 - beta_second) * gradient * gradient
    a = first / (1.0 - beta_first**STEP)
    b = second / (1.0 - beta_second**STEP)
    new = master - learn_rate * (a / (jnp.sqrt(b) + adam_eps) + decay * master)
    return new, jnp.stack([first, second])


def local(mesh, tokens, cotangent, seg_ids, qkv, out, up, down, vectors, *moments):
    shards = mesh.shape["shard"]
    count, model = tokens.shape
    hidden = up.shape[1]
    rows = qkv.shape[0]
    ff = hidden // model
    total_tokens = count * mesh.shape["replica"] * shards
    grad_scale = total_tokens ** (-0.5)
    own = chunked(*(w.astype(bf16) for w in (qkv, out, up, down)), rows, model, shards)
    wa, grads, mlp, gmlp, attn_in, normed, inverse, gout, vg, vgrad = forward_call(
        mesh, own, vectors[None], tokens, cotangent, seg_ids[:, None], hidden, grad_scale
    )
    cosine, sine = rotary_tables(seg_ids, model // H)
    attn_out, gattn, wgrads, sums = attention_xla(
        wa, attn_in, gout, seg_ids, vg, cosine, sine, count, model, grad_scale
    )
    live = (seg_ids >= 0).astype(f32)[:, None]
    block_output = (live * (tokens.astype(f32) + attn_out + mlp)).astype(bf16)
    grad_normed = gattn * vg[:, :model] + gmlp * vg[:, 2 * model : 3 * model]
    m1 = jnp.mean(grad_normed, axis=1, keepdims=True)
    m2 = jnp.mean(grad_normed * normed, axis=1, keepdims=True)
    input_grad = (gout.astype(f32) + inverse * (grad_normed - m1 - normed * m2)).astype(bf16)
    head = [jnp.sum(gattn * normed, axis=0) * grad_scale, jnp.sum(gattn, axis=0) * grad_scale]
    vgrad = jnp.concatenate([*head, vgrad[0, 2 * model : 4 * model], *sums, vgrad[0, 7 * model :]])
    grads = grads.at[2 * ff :].set(jnp.stack(wgrads).reshape(4, shards, rows, model))
    total, _ = reduce_call(mesh, grads, vgrad[None])
    vshare = lax.psum_scatter(vgrad.astype(bf16), "shard", scatter_dimension=0, tiled=True)
    vsum = lax.psum(vshare, "replica").astype(f32)
    summed = [x.astype(f32) for x in unchunked(total, hidden, shards)] + [vsum]
    updated, renewed = [], []
    for w, m, g, decay in zip((qkv, out, up, down, vectors), moments, summed, (weight_decay,) * 4 + (0.0,)):
        a, b = adam(w, m, g, decay)
        updated.append(a)
        renewed.append(b)
    return (block_output, input_grad, *summed, *updated, *renewed)


def solution(mesh):
    rows = P(("replica", "shard"), None)
    first, second = P("shard", None), P(None, "shard", None)
    weights, moments = (first,) * 4 + (P("shard"),), (second,) * 4 + (P(None, "shard"),)
    return jax.shard_map(
        functools.partial(local, mesh),
        mesh=mesh,
        in_specs=(rows, rows, P(("replica", "shard")), *weights, *moments),
        out_specs=(rows, rows, *weights, *weights, *moments),
        check_vma=False,
    )
```

```python
import functools
import math

import jax
import jax.numpy as jnp
from jax import lax
from jax.experimental import pallas as pl
from jax.experimental.pallas import tpu as pltpu
from jax.sharding import PartitionSpec as P

H = 4
ROT = 64
STEP = 3
norm_eps = 1e-05
rope_base = 10000.0
learn_rate = 0.01
beta_first = 0.9
beta_second = 0.95
adam_eps = 1e-08
weight_decay = 0.1
root_half = 0.7071067811865476
inv_root_tau = 0.3989422804014327

MESH = pl.DeviceIdType.MESH
f32, bf16 = jnp.float32, jnp.bfloat16
ANY = pl.BlockSpec(memory_space=pl.ANY)
VMEM = pl.BlockSpec(memory_space=pltpu.VMEM)
DMA = pltpu.SemaphoreType.DMA
TILE = 256
LANES = 128
PARTS = 2
RLAG = 2
RAW = 3
CAST = 64
LAG = 2
AHEAD = 3


class Place:
    def __init__(self, replicas, shards):
        self.replicas, self.shards = replicas, shards
        self.steps = int(math.log2(replicas)) - 1
        self.half = 2**self.steps
        self.r = lax.axis_index("replica")
        self.s = lax.axis_index("shard")
        self.core = self.r % 2
        self.m = self.mixed(self.r // 2)
        self.base = self.core * self.half
        self.twin_base = (1 - self.core) * self.half
        self.piece = self.base + self.m
        self.twin = (self.r + 1 - 2 * self.core, self.s)
        self.partner, self.mine, self.theirs = [], [], []
        for k in range(self.steps):
            flip = 2**k
            other = self.m + flip * (1 - 2 * ((self.m // flip) % 2))
            self.partner.append((2 * self.mixed(other) + self.core, self.s))
            self.mine.append((self.m // flip) * flip)
            self.theirs.append((other // flip) * flip)

    def mixed(self, plane):
        n = self.steps
        turned = sum(((plane // 2**i) % 2) * 2 ** (n - 1 - i) for i in range(n))
        return (1 - self.core) * plane + self.core * turned

    def across(self, d):
        return (self.r, (self.s + d) % self.shards)

    def source(self, d):
        return (self.s + self.shards - d) % self.shards

    def greet(self):
        barrier = pltpu.get_barrier_semaphore()
        peers = [self.across(d) for d in range(1, self.shards)] + self.partner + [self.twin]
        for peer in peers:
            pl.semaphore_signal(barrier, inc=1, device_id=peer, device_id_type=MESH)
        pl.semaphore_wait(barrier, len(peers))


def remote(src, dst, send, recv, peer):
    return pltpu.make_async_remote_copy(
        src_ref=src, dst_ref=dst, send_sem=send, recv_sem=recv, device_id=peer, device_id_type=MESH
    )


class Gather:
    def __init__(self, place, wg, send, recv):
        self.p, self.wg, self.send, self.recv = place, wg, send, recv
        self.chunks = wg.shape[0]
        self.rows = wg.shape[2] // place.replicas
        self.stages = place.steps + 2
        self.n = place.shards - 1
        self.units = self.chunks * self.n
        self.ticks = self.units + (self.stages - 1) * LAG

    def span(self, t, shard, first, count):
        start = pl.multiple_of(first * self.rows, self.rows)
        return self.wg.at[t, shard, pl.ds(start, count * self.rows), :]

    def copy(self, stage, t, d):
        p = self.p
        if stage == 0:
            ref, peer = self.span(t, p.s, p.piece, 1), p.across(d)
        elif stage <= p.steps:
            k = stage - 1
            ref, peer = self.span(t, p.source(d), p.base + p.mine[k], 2**k), p.partner[k]
        else:
            ref, peer = self.span(t, p.source(d), p.base, p.half), p.twin
        u = t * self.n + d - 1
        return remote(ref, ref, self.send.at[stage, u], self.recv.at[stage, u], peer)

    def launch(self, t):
        for d in range(1, self.n + 1):
            self.copy(0, t, d).start()

    def ready(self, t):
        return (t + 1) * self.n + (self.stages - 1) * LAG

    def tick(self, u):
        for stage in range(self.stages):
            v = u - stage * LAG

            @pl.when((v >= 0) & (v < self.units))
            def _(stage=stage, v=v):
                t, d = v // self.n, v % self.n + 1
                self.copy(stage, t, d).wait_recv()
                if stage + 1 < self.stages:
                    self.copy(stage + 1, t, d).start()

        @pl.when((u % self.n == self.n - 1) & (u // self.n + AHEAD < self.chunks))
        def _():
            self.launch(u // self.n + AHEAD)

    def finish(self):
        @pl.loop(0, self.chunks)
        def _(t):
            for d in range(1, self.n + 1):
                for stage in range(self.stages):
                    self.copy(stage, t, d).wait_send()


def dot(a, b, dims=((1,), (0,))):
    return lax.dot_general(a, b, (dims, ((), ())), preferred_element_type=f32)


def forward_kernel(
    replicas, shards, hidden, grad_scale,
    qkv, out_w, up_w, down_w, vec, tok, cot, seg,
    wa, grads, mlp, gmlp, attn_in, inverse, gout, vg, vgrad,
    wg, raw, normed, mlp_in, mlp_in_t, stage_up, stage_down, vsend, vrecv, send, recv, own_sem, out_sem, grad_sem,
):
    p = Place(replicas, shards)
    chunks, _, rows, model = wg.shape
    tokens = tok.shape[0]
    ff_chunks = hidden // model
    tiles = model // TILE
    per_tile = TILE // rows
    o_gain1, o_bias1, o_gain2, o_bias2 = (i * model for i in range(4))
    o_out = 7 * model
    o_up = 8 * model
    o_down = o_up + hidden

    def loads(t):
        slot, j = t % RAW, t // 2
        dst, sem = raw.at[slot], own_sem.at[slot]
        if t >= 2 * ff_chunks:
            i = t - 2 * ff_chunks
            src = qkv.at[:, i * model : (i + 1) * model] if i < 3 else out_w
            return [pltpu.make_async_copy(src, dst, sem.at[0])]
        if t % 2:
            return [pltpu.make_async_copy(down_w.at[j * rows : (j + 1) * rows, :], dst, sem.at[0])]
        wide = hidden // shards
        return [
            pltpu.make_async_copy(
                up_w.at[:, i * wide + j * rows : i * wide + (j + 1) * rows],
                dst.at[:, i * rows : (i + 1) * rows],
                sem.at[i],
            )
            for i in range(shards)
        ]

    def start(t):
        for c in loads(t):
            c.start()

    for t in range(RAW):
        start(t)
    width = vec.shape[1]

    def slot(shard):
        return vg.at[:, pl.ds(pl.multiple_of(shard * width, 128), width)]

    slot(p.s)[...] = vec[...].astype(bf16).astype(f32)
    p.greet()
    g = Gather(p, wg, send, recv)

    def vcopy(d):
        return remote(slot(p.s), slot(p.s), vsend.at[d - 1], vrecv.at[d - 1], p.across(d))

    for d in range(1, shards):
        vcopy(d).start()
    for t in range(chunks):
        for c in loads(t):
            c.wait()

        @pl.loop(0, rows // CAST)
        def _(i, t=t):
            at = pl.ds(pl.multiple_of(i * CAST, CAST), CAST)
            wg[t, p.s, at, :] = raw[t % RAW, at, :].astype(bf16)

        if t + RAW < chunks:
            start(t + RAW)
        if 1 <= t <= AHEAD:
            g.launch(t - 1)

    band = 64

    @pl.loop(0, tokens // band)
    def _(i):
        at = pl.ds(pl.multiple_of(i * band, band), band)
        x = tok[at, :].astype(f32)
        mean = jnp.mean(x, axis=1, keepdims=True)
        centred = x - mean
        inv = lax.rsqrt(jnp.mean(centred * centred, axis=1, keepdims=True) + norm_eps)
        inverse[at, :] = inv
        normed[at, :] = centred * inv
        live = (seg[at, :] >= 0).astype(f32)
        gout[at, :] = (cot[at, :].astype(f32) * live).astype(bf16)

    for d in range(1, shards):
        vcopy(d).wait_recv()

    @pl.loop(0, tokens // band)
    def _(i):
        at = pl.ds(pl.multiple_of(i * band, band), band)
        x = normed[at, :]
        attn_in[at, :] = (x * vg[:, o_gain1:o_bias1] + vg[:, o_bias1:o_gain2]).astype(bf16)
        mlp_in[at, :] = (x * vg[:, o_gain2:o_bias2] + vg[:, o_bias2 : 4 * model]).astype(bf16)
        mlp[at, :] = jnp.broadcast_to(vg[:, o_down : o_down + model], (band, model))
        gmlp[at, :] = jnp.zeros((band, model), f32)

    for i in range(tokens // 128):
        at = slice(i * 128, i * 128 + 128)
        mlp_in_t[:, at] = mlp_in[at, :].T

    vgrad[...] = jnp.zeros_like(vgrad)

    first = g.ready(1)

    @pl.loop(0, first)
    def _(u):
        g.tick(u)

    per_j = 2 * g.n

    def grad_out_copy(which, j):
        ref = (stage_up, stage_down)[which]
        return pltpu.make_async_copy(ref.at[j % 2], grads.at[2 * j + which], grad_sem.at[which, j % 2])

    def flat(s0, j):
        return [
            pl.multiple_of((s0 * per_tile + i) * (hidden // shards) + j * rows, rows)
            for i in range(per_tile)
        ]

    @pl.loop(0, ff_chunks * tiles)
    def _(it):
        j, n = it // tiles, it % tiles
        lo, hi = first + (it * per_j) // tiles, first + ((it + 1) * per_j) // tiles

        def maybe(i):
            @pl.when((lo + i < hi) & (lo + i < g.ticks))
            def _():
                g.tick(lo + i)

        most = -(-per_j // tiles)
        cols = pl.ds(pl.multiple_of(n * TILE, TILE), TILE)

        @pl.when((n == 0) & (j >= 2))
        def _():
            grad_out_copy(0, j).wait()
            grad_out_copy(1, j).wait()

        maybe(0)
        up = wg[2 * j, :, :, cols].reshape(model, TILE)
        down = wg[2 * j + 1, pl.ds(n * per_tile, per_tile)].reshape(TILE, model)
        bias = jnp.concatenate([vg[:, pl.ds(o_up + f, rows)] for f in flat(n, j)], axis=1)
        h = dot(mlp_in[...], up) + bias
        cum = 0.5 * (1.0 + lax.erf(h * root_half))
        density = jnp.exp(-0.5 * h * h) * inv_root_tau
        act = (h * cum).astype(bf16)
        gh = dot(gout[...], down, ((1,), (1,))) * (cum + h * density)
        ghh = gh.astype(bf16)
        total = jnp.sum(gh, axis=0, keepdims=True) * grad_scale
        for i, f in enumerate(flat(n, j)):
            vgrad[:, pl.ds(o_up + f, rows)] = total[:, i * rows : (i + 1) * rows]
        for i in range(1, most):
            maybe(i)
        mlp[...] += dot(act, down)
        stage_down[j % 2, pl.ds(n * per_tile, per_tile)] = (
            (dot(act, gout[...], ((0,), (0,))) * grad_scale).astype(bf16).reshape(per_tile, rows, model)
        )
        gmlp[...] += dot(ghh, up, ((1,), (1,)))
        stage_up[j % 2, :, :, cols] = (
            (dot(mlp_in_t[...], ghh) * grad_scale).astype(bf16).reshape(shards, rows, TILE)
        )

        @pl.when(n == tiles - 1)
        def _():
            grad_out_copy(0, j).start()
            grad_out_copy(1, j).start()

    def out(t):
        return pltpu.make_async_copy(wg.at[t], wa.at[t - 2 * ff_chunks], out_sem.at[t - 2 * ff_chunks])

    done = first + ff_chunks * per_j

    @pl.loop(done, g.ticks)
    def _(u):
        g.tick(u)

    for t in range(2 * ff_chunks, chunks):
        out(t).start()

    def column_sums(i, carry):
        at = pl.ds(pl.multiple_of(i * band, band), band)
        gm = gmlp[at, :]
        new = (gm * normed[at, :], gm, gout[at, :].astype(f32))
        return tuple(a + jnp.sum(b, axis=0, keepdims=True) for a, b in zip(carry, new))

    zero = jnp.zeros((1, model), f32)
    sums = lax.fori_loop(0, tokens // band, column_sums, (zero, zero, zero))
    vgrad[:, o_gain2:o_bias2] = sums[0] * grad_scale
    vgrad[:, o_bias2 : 4 * model] = sums[1] * grad_scale
    vgrad[:, o_out : o_out + model] = sums[2] * grad_scale
    vgrad[:, o_down : o_down + model] = sums[2] * grad_scale

    for d in range(1, shards):
        vcopy(d).wait_send()
    g.finish()
    for j in range(max(ff_chunks - 2, 0), ff_chunks):
        grad_out_copy(0, j).wait()
        grad_out_copy(1, j).wait()
    for t in range(2 * ff_chunks, chunks):
        out(t).wait()


def forward_call(mesh, qkv, out, up, down, vec, tok, cot, seg, grad_scale):
    replicas, shards = mesh.shape["replica"], mesh.shape["shard"]
    rows, hidden = up.shape
    tokens, model = tok.shape
    ff_chunks = hidden // model
    chunks = 2 * ff_chunks + 4
    stages = int(math.log2(replicas)) + 1
    width = vec.shape[1]
    units = chunks * (shards - 1)
    sds = jax.ShapeDtypeStruct
    outs = (
        (sds((4, shards, rows, model), bf16), ANY),
        (sds((chunks, shards, rows, model), bf16), ANY),
        (sds((tokens, model), f32), VMEM),
        (sds((tokens, model), f32), VMEM),
        (sds((tokens, model), bf16), VMEM),
        (sds((tokens, 1), f32), VMEM),
        (sds((tokens, model), bf16), VMEM),
        (sds((1, width * shards), f32), VMEM),
        (sds((1, width * shards), f32), VMEM),
    )
    return pl.pallas_call(
        functools.partial(forward_kernel, replicas, shards, hidden, grad_scale),
        out_shape=[o[0] for o in outs],
        in_specs=[ANY] * 4 + [VMEM] * 4,
        out_specs=[o[1] for o in outs],
        scratch_shapes=[
            pltpu.VMEM((chunks, shards, rows, model), bf16),
            pltpu.VMEM((RAW, rows, model), f32),
            pltpu.VMEM((tokens, model), f32),
            pltpu.VMEM((tokens, model), bf16),
            pltpu.VMEM((model, tokens), bf16),
            pltpu.VMEM((2, shards, rows, model), bf16),
            pltpu.VMEM((2, shards, rows, model), bf16),
            DMA((shards - 1,)),
            DMA((shards - 1,)),
            DMA((stages, units)),
            DMA((stages, units)),
            DMA((RAW, shards)),
            DMA((4,)),
            DMA((2, 2)),
        ],
        compiler_params=pltpu.CompilerParams(
            collective_id=0, has_side_effects=True, vmem_limit_bytes=60 << 20
        ),
        name="gather_mlp",
    )(qkv, out, up, down, vec, tok, cot, seg)


def rotary_tables(segment):
    count = segment.shape[0]
    index = jnp.arange(count)
    same = segment[:, None] == segment[None, :]
    position = jnp.sum((same & (index[None, :] < index[:, None])).astype(jnp.int32), axis=1)
    half = ROT // 2
    frequency = rope_base ** (-2.0 * jnp.arange(half).astype(f32) / ROT)
    angles = position.astype(f32)[:, None] * frequency[None, :]
    cosine, sine = jnp.cos(angles), jnp.sin(angles)
    rest = LANES - ROT
    cosines = jnp.concatenate([cosine, cosine, jnp.ones((count, rest), f32)], axis=1)
    sines = jnp.concatenate([-sine, sine, jnp.zeros((count, rest), f32)], axis=1)
    return cosines, sines


class Reduce:
    def __init__(self, place, grads, lo, rc, r, rz, total, sems, parts):
        self.p, self.grads, self.lo, self.rc, self.r, self.rz, self.total = place, grads, lo, rc, r, rz, total
        self.csem, self.ksem, self.zsem, self.gsem, self.lsem = sems
        self.parts = parts
        self.cols = total.shape[2] // parts
        self.rows = total.shape[1] // place.replicas
        self.units = total.shape[0] * parts
        self.n = place.shards - 1
        self.stages = 2 * place.steps + 4
        self.ticks = self.units + (self.stages - 1) * RLAG
        self.slots = lo.shape[0]

    def where(self, u):
        t, part = u // self.parts, u % self.parts
        return t, pl.ds(pl.multiple_of(part * self.cols, self.cols), self.cols)

    def band(self, first, count):
        return pl.ds(pl.multiple_of(first * self.rows, self.rows), count * self.rows)

    def load(self, u):
        t, cols = self.where(u)
        src = self.grads.at[t, :, self.band(self.p.base, self.p.half), cols]
        return pltpu.make_async_copy(src, self.lo.at[u % self.slots], self.lsem.at[u % self.slots])

    def core_copy(self, u):
        t, cols = self.where(u)
        src = self.grads.at[t, :, self.band(self.p.twin_base, self.p.half), cols]
        return remote(src, self.rc.at[u], self.csem.at[0, u], self.csem.at[1, u], self.p.twin)

    def held(self, k):
        p = self.p
        return (self.rc, 0) if k == p.steps else (self.r[k], p.mine[k])

    def plane_copy(self, k, u):
        ref, first = self.held(k + 1)
        src = ref.at[u, :, self.band(self.p.theirs[k] - first, 2**k), :]
        return remote(src, self.r[k].at[u], self.ksem.at[0, k, u], self.ksem.at[1, k, u], self.p.partner[k])

    def shard_copy(self, u, d):
        p = self.p
        to = p.across(d)
        src = self.held(0)[0].at[u, to[1]]
        return remote(src, self.rz.at[u, d - 1], self.zsem.at[0, u, d - 1], self.zsem.at[1, u, d - 1], to)

    def total_copy(self, k, u):
        p = self.p
        t, cols = self.where(u)
        first, count, peer = (
            (p.base + p.mine[k], 2**k, p.partner[k]) if k < p.steps else (p.base, p.half, p.twin)
        )
        ref = self.total.at[t, self.band(first, count), cols]
        return remote(ref, ref, self.gsem.at[0, k, u], self.gsem.at[1, k, u], peer)

    def add(self, stage, u):
        p = self.p
        if stage == 0:
            self.load(u).start()
        elif stage == 1:
            self.core_copy(u).wait_recv()
            self.load(u).wait()
            self.rc[u] = self.rc[u] + self.lo[u % self.slots]
        elif stage < 2 + p.steps:
            k = p.steps - (stage - 1)
            self.plane_copy(k, u).wait_recv()
            ref, first = self.held(k + 1)
            self.r[k][u] = self.r[k][u] + ref[u, :, self.band(p.mine[k] - first, 2**k), :]
        elif stage == 2 + p.steps:
            for d in range(1, self.n + 1):
                self.shard_copy(u, d).wait_recv()
            acc = self.held(0)[0][u, p.s].astype(f32)
            for d in range(1, self.n + 1):
                acc += self.rz[u, d - 1].astype(f32)
            t, cols = self.where(u)
            self.total[t, self.band(p.piece, 1), cols] = acc.astype(bf16)
        else:
            self.total_copy(stage - 3 - p.steps, u).wait_recv()

    def send(self, stage, u):
        p = self.p
        if stage == 0:
            self.core_copy(u).start()
        elif stage < 1 + p.steps:
            self.plane_copy(p.steps - stage, u).start()
        elif stage == 1 + p.steps:
            for d in range(1, self.n + 1):
                self.shard_copy(u, d).start()
        elif stage < self.stages - 1:
            self.total_copy(stage - 2 - p.steps, u).start()

    def tick(self, u):
        for do in (self.add, self.send):
            for stage in range(self.stages):
                v = u - stage * RLAG

                @pl.when((v >= 0) & (v < self.units))
                def _(stage=stage, v=v):
                    do(stage, v)

    def finish(self):
        @pl.loop(0, self.units)
        def _(u):
            self.core_copy(u).wait_send()
            for k in range(self.p.steps):
                self.plane_copy(k, u).wait_send()
            for d in range(1, self.n + 1):
                self.shard_copy(u, d).wait_send()
            for k in range(self.p.steps + 1):
                self.total_copy(k, u).wait_send()


def turned(x, cosines, sines, sign):
    first = x[:, :LANES]
    lane = lax.broadcasted_iota(jnp.int32, first.shape, 1)
    other = jnp.where(lane < ROT // 2, pltpu.roll(first, LANES - ROT // 2, 1), pltpu.roll(first, ROT // 2, 1))
    return jnp.concatenate([first * cosines + sign * (other * sines), x[:, LANES:]], axis=1)


def one_head(band, q, k, v, gctx, ctx, dq, dk, dv, seg, seg_row, scale):
    dk[...] = jnp.zeros_like(dk)
    dv[...] = jnp.zeros_like(dv)
    for i in range(q.shape[0] // band):
        at, end = slice(i * band, (i + 1) * band), (i + 1) * band
        qi, gi, ki, vi = q[at, :], gctx[at, :], k[:end, :], v[:end, :]
        row = lax.broadcasted_iota(jnp.int32, (band, end), 0) + i * band
        col = lax.broadcasted_iota(jnp.int32, (band, end), 1)
        allowed = (seg[at, :] == seg_row[:, :end]) & (col <= row)
        masked = jnp.where(allowed, dot(qi, ki, ((1,), (1,))) * scale, -jnp.inf)
        largest = jnp.max(masked, axis=1, keepdims=True)
        log_total = largest + jnp.log(jnp.sum(jnp.exp(masked - largest), axis=1, keepdims=True))
        prob = jnp.exp(masked - log_total)
        half = prob.astype(bf16)
        ctx[at, :] = dot(half, vi).astype(bf16)
        gp = dot(gi, vi, ((1,), (1,)))
        delta = jnp.sum(prob * gp, axis=1, keepdims=True)
        gs = (prob * (gp - delta) * scale).astype(bf16)
        dq[at, :] = dot(gs, ki)
        dk[:end, :] += dot(gs, qi, ((0,), (0,)))
        dv[:end, :] += dot(half, gi, ((0,), (0,)))


def backward_kernel(
    replicas, shards, grad_scale,
    wa, grads_in, attn_in, gout, inverse, mlp, gmlp, tok, seg, seg_row, cosines, sines, vg, vgrad_in,
    grads, total_out, bout, ig, vshare,
    lo, rc, *rest,
):
    steps = int(math.log2(replicas)) - 1
    r, rest = rest[:steps], rest[steps:]
    rz, total, wqkv, wout, gqkv, gwout, attn_in_t, gattn, attn_out, *rest = rest
    qb, kb, vb, gb, ctx, dq, dk, dv, vgrad, vz, vx, *rest = rest
    csem, ksem, zsem, gsem, lsem, wsem, ssem, vzsem, vxsem, osem = rest
    p = Place(replicas, shards)
    red = Reduce(p, grads, lo, rc, r, rz, total, (csem, ksem, zsem, gsem, lsem), PARTS)
    tokens, model = attn_in.shape
    rows = total.shape[1]
    head = model // H
    scale = head ** (-0.5)
    per_head = head // rows
    chunk0 = total.shape[0] - 4
    width = vz.shape[2]
    band = 64

    def head_copies(h, inward):
        slot = h % 2
        cols = pl.ds(pl.multiple_of(h * head, head), head)
        mine = pl.ds(h * per_head, per_head)
        if inward:
            pairs = [(wa.at[w, :, :, cols], wqkv.at[slot, w]) for w in range(3)]
            pairs.append((wa.at[3, mine], wout.at[slot]))
            sems = wsem
        else:
            pairs = [(gqkv.at[slot, w], grads.at[chunk0 + w, :, :, cols]) for w in range(3)]
            pairs.append((gwout.at[slot], grads.at[chunk0 + 3, mine]))
            sems = ssem
        return [pltpu.make_async_copy(a, b, sems.at[slot, i]) for i, (a, b) in enumerate(pairs)]

    for c in head_copies(0, True):
        c.start()
    p.greet()
    red.tick(0)
    for i in range(tokens // 128):
        at = slice(i * 128, i * 128 + 128)
        attn_in_t[:, at] = attn_in[at, :].T
    gattn[...] = jnp.zeros_like(gattn)
    vgrad[...] = vgrad_in[...]

    @pl.loop(0, tokens // band)
    def _(i):
        at = pl.ds(pl.multiple_of(i * band, band), band)
        attn_out[at, :] = mlp[at, :] + tok[at, :].astype(f32) + vg[:, 7 * model : 8 * model]

    red.tick(1)

    @pl.loop(0, H)
    def _(h):
        slot = h % 2

        @pl.when(h + 1 < H)
        def _():
            for c in head_copies(h + 1, True):
                c.start()

        @pl.when(h >= 2)
        def _():
            for c in head_copies(h - 2, False):
                c.wait()

        for c in head_copies(h, True):
            c.wait()
        red.tick(2 + 2 * h)
        x = attn_in[...]
        w = [wqkv[slot, i].reshape(model, head) for i in range(3)]
        wo = wout[slot].reshape(head, model)

        def at_head(base):
            return pl.ds(pl.multiple_of(base + h * head, head), head)

        def project(i):
            return dot(x, w[i]) + vg[:, at_head((4 + i) * model)]

        qb[...] = turned(project(0), cosines[...], sines[...], 1.0).astype(bf16)
        kb[...] = turned(project(1), cosines[...], sines[...], 1.0).astype(bf16)
        vb[...] = project(2).astype(bf16)
        gb[...] = dot(gout[...], wo, ((1,), (1,))).astype(bf16)
        one_head(128, qb, kb, vb, gb, ctx, dq, dk, dv, seg, seg_row, scale)
        red.tick(3 + 2 * h)
        back = (
            turned(dq[...], cosines[...], sines[...], -1.0),
            turned(dk[...], cosines[...], sines[...], -1.0),
            dv[...],
        )
        sums = gattn[...]
        for i, d in enumerate(back):
            vgrad[:, at_head((4 + i) * model)] = jnp.sum(d, axis=0, keepdims=True) * grad_scale
            half = d.astype(bf16)
            sums += dot(half, w[i], ((1,), (1,)))
            gqkv[slot, i] = (dot(attn_in_t[...], half) * grad_scale).astype(bf16).reshape(shards, rows, head)
        gattn[...] = sums
        attn_out[...] += dot(ctx[...], wo)
        gwout[slot] = (
            (dot(ctx[...], gout[...], ((0,), (0,))) * grad_scale).astype(bf16).reshape(per_head, rows, model)
        )
        for c in head_copies(h, False):
            c.start()

    done = 2 + 2 * H
    gain_one, gain_two = vg[:, :model], vg[:, 2 * model : 3 * model]

    def last(i, carry):
        at = pl.ds(pl.multiple_of(i * band, band), band)
        x = tok[at, :].astype(f32)
        inv = inverse[at, :]
        normed = (x - jnp.mean(x, axis=1, keepdims=True)) * inv
        ga = gattn[at, :]
        gn = ga * gain_one + gmlp[at, :] * gain_two
        m1 = jnp.mean(gn, axis=1, keepdims=True)
        m2 = jnp.mean(gn * normed, axis=1, keepdims=True)
        ig[at, :] = (gout[at, :].astype(f32) + inv * (gn - m1 - normed * m2)).astype(bf16)
        live = (seg[at, :] >= 0).astype(f32)
        bout[at, :] = (live * attn_out[at, :]).astype(bf16)
        return (
            carry[0] + jnp.sum(ga * normed, axis=0, keepdims=True),
            carry[1] + jnp.sum(ga, axis=0, keepdims=True),
        )

    zero = jnp.zeros((1, model), f32)
    sums = lax.fori_loop(0, tokens // band, last, (zero, zero))
    vgrad[:, :model] = sums[0] * grad_scale
    vgrad[:, model : 2 * model] = sums[1] * grad_scale
    vgrad[...] = vgrad[...].astype(bf16).astype(f32)
    for h in range(max(H - 2, 0), H):
        for c in head_copies(h, False):
            c.wait()

    def part(shard):
        return pl.ds(pl.multiple_of(shard * width, LANES), width)

    def vcopy(d):
        to = p.across(d)
        return remote(vgrad.at[:, part(to[1])], vz.at[d - 1], vzsem.at[0, d - 1], vzsem.at[1, d - 1], to)

    peers = [*p.partner, p.twin]

    def vexchange(k):
        return remote(vx.at[2 * k], vx.at[2 * k + 1], vxsem.at[0, k], vxsem.at[1, k], peers[k])

    def vstart(i):
        if i == 0:
            for d in range(1, shards):
                vcopy(d).start()
        else:
            vexchange(i - 1).start()

    def vfinish(i):
        if i == 0:
            acc = vgrad[:, part(p.s)]
            for d in range(1, shards):
                vcopy(d).wait_recv()
                acc += vz[d - 1]
        else:
            vexchange(i - 1).wait_recv()
            acc = vx[2 * i - 2] + vx[2 * i - 1]
        if i < len(peers):
            vx[2 * i] = acc
        else:
            vshare[...] = acc

    for i in range(len(peers) + 1):
        red.tick(done + 2 * i)
        vstart(i)
        red.tick(done + 2 * i + 1)
        vfinish(i)
    done += 2 * len(peers) + 2

    @pl.loop(done, red.ticks)
    def _(u):
        red.tick(u)

    copy = pltpu.make_async_copy(total, total_out, osem)
    copy.start()
    for d in range(1, shards):
        vcopy(d).wait_send()
    for i in range(len(peers)):
        vexchange(i).wait_send()
    red.finish()
    copy.wait()


def backward_call(mesh, grad_scale, wa, grads, attn_in, gout, inverse, mlp, gmlp, tok, seg, cosines, sines, vg, vgrad):
    replicas, shards = mesh.shape["replica"], mesh.shape["shard"]
    chunks, _, rows, model = grads.shape
    tokens = tok.shape[0]
    steps = int(math.log2(replicas)) - 1
    units, cols, piece = chunks * PARTS, model // PARTS, rows // replicas
    half = 2**steps
    head = model // H
    width = vg.shape[1] // shards
    per_head = head // rows
    sds = jax.ShapeDtypeStruct
    vm = pltpu.VMEM
    return pl.pallas_call(
        functools.partial(backward_kernel, replicas, shards, grad_scale),
        out_shape=[
            sds(grads.shape, bf16),
            sds((chunks, rows, model), bf16),
            sds((tokens, model), bf16),
            sds((tokens, model), bf16),
            sds((1, width), f32),
        ],
        in_specs=[ANY, ANY] + [VMEM] * 12,
        out_specs=[ANY, ANY, VMEM, VMEM, VMEM],
        input_output_aliases={1: 0},
        scratch_shapes=[
            vm((RLAG + 1, shards, half * piece, cols), bf16),
            vm((units, shards, half * piece, cols), bf16),
            *(vm((units, shards, 2**k * piece, cols), bf16) for k in range(steps)),
            vm((units, shards - 1, piece, cols), bf16),
            vm((chunks, rows, model), bf16),
            vm((2, 3, shards, rows, head), bf16),
            vm((2, per_head, rows, model), bf16),
            vm((2, 3, shards, rows, head), bf16),
            vm((2, per_head, rows, model), bf16),
            vm((model, tokens), bf16),
            vm((tokens, model), f32),
            vm((tokens, model), f32),
            *[vm((tokens, head), bf16)] * 5,
            *[vm((tokens, head), f32)] * 3,
            vm((1, width * shards), f32),
            vm((shards - 1, 1, width), f32),
            vm((2 * steps + 2, 1, width), f32),
            DMA((2, units)),
            DMA((2, steps, units)),
            DMA((2, units, shards - 1)),
            DMA((2, steps + 1, units)),
            DMA((RLAG + 1,)),
            DMA((2, 4)),
            DMA((2, 4)),
            DMA((2, shards - 1)),
            DMA((2, steps + 1)),
            DMA(()),
        ],
        compiler_params=pltpu.CompilerParams(
            collective_id=1, has_side_effects=True, vmem_limit_bytes=61 << 20
        ),
        name="attention_reduce",
    )(wa, grads, attn_in, gout, inverse, mlp, gmlp, tok, seg, seg.reshape(1, -1), cosines, sines, vg, vgrad)


def adam(master, first, second, gradient, decay):
    first = beta_first * first + (1.0 - beta_first) * gradient
    second = beta_second * second + (1.0 - beta_second) * gradient * gradient
    a = first / (1.0 - beta_first**STEP)
    b = second / (1.0 - beta_second**STEP)
    return master - learn_rate * (a / (jnp.sqrt(b) + adam_eps) + decay * master), first, second


def adam_kernel(total, w, m, grad, new_w, new_m):
    g = total[0].astype(f32)
    grad[...] = g
    new_w[...], new_m[0], new_m[1] = adam(w[...], m[0], m[1], g, weight_decay)


def adam_call(total, w, m, grid, block, chunk_at, weight_at):
    wspec = pl.BlockSpec(block, weight_at)
    mspec = pl.BlockSpec((2, *block), lambda *i: (0, *weight_at(*i)))
    sds = jax.ShapeDtypeStruct
    return pl.pallas_call(
        adam_kernel,
        grid=grid,
        out_shape=[sds(w.shape, f32), sds(w.shape, f32), sds(m.shape, f32)],
        in_specs=[pl.BlockSpec((1, *block), chunk_at), wspec, mspec],
        out_specs=[wspec, wspec, mspec],
        compiler_params=pltpu.CompilerParams(vmem_limit_bytes=48 << 20),
        name="adam",
    )(total, w, m)


def local(mesh, tokens, cotangent, seg_ids, qkv, out, up, down, vectors, *moments):
    shards = mesh.shape["shard"]
    count, model = tokens.shape
    hidden = up.shape[1]
    rows = qkv.shape[0]
    ff = hidden // model
    grad_scale = (count * mesh.shape["replica"] * shards) ** (-0.5)
    seg = seg_ids[:, None]
    wa, grads, mlp, gmlp, attn_in, inverse, gout, vg, vgrad = forward_call(
        mesh, qkv, out, up, down, vectors[None], tokens, cotangent, seg, grad_scale
    )
    cosines, sines = rotary_tables(seg_ids)
    _, total, block_output, input_grad, vshare = backward_call(
        mesh, grad_scale, wa, grads, attn_in, gout, inverse, mlp, gmlp, tokens, seg, cosines, sines, vg, vgrad
    )
    band = rows // 2
    steps = (
        adam_call(
            total, qkv, moments[0], (3, 2), (band, model), lambda j, b: (2 * ff + j, b, 0), lambda j, b: (b, j)
        ),
        adam_call(
            total, out, moments[1], (2,), (band, model), lambda b: (2 * ff + 3, b, 0), lambda b: (b, 0)
        ),
        adam_call(
            total, up, moments[2], (ff, shards), (rows, rows), lambda j, i: (2 * j, 0, i), lambda j, i: (0, i * ff + j)
        ),
        adam_call(
            total, down, moments[3], (ff, 2), (band, model), lambda j, b: (2 * j + 1, b, 0), lambda j, b: (2 * j + b, 0)
        ),
    )
    vsum = vshare[0]
    new_v, *vm = adam(vectors, moments[4][0], moments[4][1], vsum, 0.0)
    grads_out, updated, renewed = zip(*steps)
    return (block_output, input_grad, *grads_out, vsum, *updated, new_v, *renewed, jnp.stack(vm))


def solution(mesh):
    rows = P(("replica", "shard"), None)
    first, second = P("shard", None), P(None, "shard", None)
    weights, moments = (first,) * 4 + (P("shard"),), (second,) * 4 + (P(None, "shard"),)
    return jax.shard_map(
        functools.partial(local, mesh),
        mesh=mesh,
        in_specs=(rows, rows, P(("replica", "shard")), *weights, *moments),
        out_specs=(rows, rows, *weights, *weights, *moments),
        check_vma=False,
    )
```

```python
import functools
import math

import jax
import jax.numpy as jnp
from jax import lax
from jax.experimental import pallas as pl
from jax.experimental.pallas import tpu as pltpu
from jax.sharding import PartitionSpec as P

H = 4
ROT = 64
STEP = 3
norm_eps = 1e-05
rope_base = 10000.0
learn_rate = 0.01
beta_first = 0.9
beta_second = 0.95
adam_eps = 1e-08
weight_decay = 0.1
root_half = 0.7071067811865476
inv_root_tau = 0.3989422804014327

MESH = pl.DeviceIdType.MESH
f32, bf16 = jnp.float32, jnp.bfloat16
ANY = pl.BlockSpec(memory_space=pl.ANY)
VMEM = pl.BlockSpec(memory_space=pltpu.VMEM)
DMA = pltpu.SemaphoreType.DMA
TILE = 256
LANES = 128
PARTS = 2
RLAG = 2
RAW = 2
CAST = 64
EARLY = 5
TICKS_8 = 4
LAG = 2
AHEAD = 3


class Place:
    def __init__(self, replicas, shards):
        self.replicas, self.shards = replicas, shards
        self.steps = int(math.log2(replicas)) - 1
        self.half = 2**self.steps
        self.r = lax.axis_index("replica")
        self.s = lax.axis_index("shard")
        self.core = self.r % 2
        self.m = self.mixed(self.r // 2)
        self.base = self.core * self.half
        self.twin_base = (1 - self.core) * self.half
        self.piece = self.base + self.m
        self.twin = (self.r + 1 - 2 * self.core, self.s)
        self.partner, self.mine, self.theirs = [], [], []
        for k in range(self.steps):
            flip = 2**k
            other = self.m + flip * (1 - 2 * ((self.m // flip) % 2))
            self.partner.append((2 * self.mixed(other) + self.core, self.s))
            self.mine.append((self.m // flip) * flip)
            self.theirs.append((other // flip) * flip)

    def mixed(self, plane):
        n = self.steps
        turned = sum(((plane // 2**i) % 2) * 2 ** (n - 1 - i) for i in range(n))
        return (1 - self.core) * plane + self.core * turned

    def across(self, d):
        return (self.r, (self.s + d) % self.shards)

    def source(self, d):
        return (self.s + self.shards - d) % self.shards

    def greet(self):
        barrier = pltpu.get_barrier_semaphore()
        peers = [self.across(d) for d in range(1, self.shards)] + self.partner + [self.twin]
        for peer in peers:
            pl.semaphore_signal(barrier, inc=1, device_id=peer, device_id_type=MESH)
        pl.semaphore_wait(barrier, len(peers))


def remote(src, dst, send, recv, peer):
    return pltpu.make_async_remote_copy(
        src_ref=src, dst_ref=dst, send_sem=send, recv_sem=recv, device_id=peer, device_id_type=MESH
    )


class Gather:
    def __init__(self, place, wg, send, recv):
        self.p, self.wg, self.send, self.recv = place, wg, send, recv
        self.chunks = wg.shape[0]
        self.rows = wg.shape[2] // place.replicas
        self.stages = place.steps + 2
        self.n = place.shards - 1
        self.units = self.chunks * self.n
        self.ticks = self.units + (self.stages - 1) * LAG

    def span(self, t, shard, first, count):
        start = pl.multiple_of(first * self.rows, self.rows)
        return self.wg.at[t, shard, pl.ds(start, count * self.rows), :]

    def copy(self, stage, t, d):
        p = self.p
        if stage == 0:
            ref, peer = self.span(t, p.s, p.piece, 1), p.across(d)
        elif stage <= p.steps:
            k = stage - 1
            ref, peer = self.span(t, p.source(d), p.base + p.mine[k], 2**k), p.partner[k]
        else:
            ref, peer = self.span(t, p.source(d), p.base, p.half), p.twin
        u = t * self.n + d - 1
        return remote(ref, ref, self.send.at[stage, u], self.recv.at[stage, u], peer)

    def launch(self, t):
        for d in range(1, self.n + 1):
            self.copy(0, t, d).start()

    def ready(self, t):
        return (t + 1) * self.n + (self.stages - 1) * LAG

    def tick(self, u):
        for stage in range(self.stages):
            v = u - stage * LAG

            @pl.when((v >= 0) & (v < self.units))
            def _(stage=stage, v=v):
                t, d = v // self.n, v % self.n + 1
                self.copy(stage, t, d).wait_recv()
                if stage + 1 < self.stages:
                    self.copy(stage + 1, t, d).start()

        @pl.when((u % self.n == self.n - 1) & (u // self.n + AHEAD < self.chunks))
        def _():
            self.launch(u // self.n + AHEAD)

    def finish(self):
        @pl.loop(0, self.chunks)
        def _(t):
            for d in range(1, self.n + 1):
                for stage in range(self.stages):
                    self.copy(stage, t, d).wait_send()


def dot(a, b, dims=((1,), (0,))):
    return lax.dot_general(a, b, (dims, ((), ())), preferred_element_type=f32)


def column(row):
    return jnp.broadcast_to(row.astype(f32), (8, row.shape[1])).T[:, :1]


def rotary_rows(seg, seg_row, start, freq):
    shape = (seg.shape[0], seg_row.shape[1])
    row = lax.broadcasted_iota(jnp.int32, shape, 0) + start
    col = lax.broadcasted_iota(jnp.int32, shape, 1)
    before = (seg == seg_row.astype(f32)) & (col < row)
    position = jnp.sum(before.astype(f32), axis=1, keepdims=True)
    angles = position * freq
    lane = lax.broadcasted_iota(jnp.int32, angles.shape, 1)
    cosine, sine = jnp.cos(angles), jnp.sin(angles)
    sine = jnp.where(lane < ROT // 2, -sine, sine)
    return jnp.where(lane < ROT, cosine, 1.0), jnp.where(lane < ROT, sine, 0.0)


def flat_columns(tile, j, rows, wide):
    per_tile = TILE // rows
    return [pl.multiple_of((tile * per_tile + i) * wide + j * rows, rows) for i in range(per_tile)]


def feed_forward(up, down, flats, rows, o_up, grad_scale, mlp_in, mlp_in_t, gout, vg, vgrad, mlp, gmlp, between, keep):
    bias = jnp.concatenate([vg[:, pl.ds(o_up + f, rows)] for f in flats], axis=1)
    h = dot(mlp_in[...], up) + bias
    cum = 0.5 * (1.0 + lax.erf(h * root_half))
    density = jnp.exp(-0.5 * h * h) * inv_root_tau
    act = (h * cum).astype(bf16)
    gh = dot(gout[...], down, ((1,), (1,))) * (cum + h * density)
    ghh = gh.astype(bf16)
    total = jnp.sum(gh, axis=0, keepdims=True) * grad_scale
    for i, f in enumerate(flats):
        vgrad[:, pl.ds(o_up + f, rows)] = total[:, i * rows : (i + 1) * rows]
    between()
    mlp[...] += dot(act, down)
    keep(1, (dot(act, gout[...], ((0,), (0,))) * grad_scale).astype(bf16))
    gmlp[...] += dot(ghh, up, ((1,), (1,)))
    keep(0, (dot(mlp_in_t[...], ghh) * grad_scale).astype(bf16))


def turned(x, cosines, sines, sign):
    first = x[:, :LANES]
    lane = lax.broadcasted_iota(jnp.int32, first.shape, 1)
    other = jnp.where(lane < ROT // 2, pltpu.roll(first, LANES - ROT // 2, 1), pltpu.roll(first, ROT // 2, 1))
    return jnp.concatenate([first * cosines + sign * (other * sines), x[:, LANES:]], axis=1)


def one_head(band, q, k, v, gctx, ctx, dq, dk, dv, seg_row, scale):
    dk[...] = jnp.zeros_like(dk)
    dv[...] = jnp.zeros_like(dv)
    for i in range(q.shape[0] // band):
        at, end = slice(i * band, (i + 1) * band), (i + 1) * band
        qi, gi, ki, vi = q[at, :], gctx[at, :], k[:end, :], v[:end, :]
        row = lax.broadcasted_iota(jnp.int32, (band, end), 0) + i * band
        col = lax.broadcasted_iota(jnp.int32, (band, end), 1)
        allowed = (column(seg_row[:, at]) == seg_row[:, :end].astype(f32)) & (col <= row)
        masked = jnp.where(allowed, dot(qi, ki, ((1,), (1,))) * scale, -jnp.inf)
        largest = jnp.max(masked, axis=1, keepdims=True)
        log_total = largest + jnp.log(jnp.sum(jnp.exp(masked - largest), axis=1, keepdims=True))
        prob = jnp.exp(masked - log_total)
        half = prob.astype(bf16)
        ctx[at, :] = dot(half, vi).astype(bf16)
        gp = dot(gi, vi, ((1,), (1,)))
        delta = jnp.sum(prob * gp, axis=1, keepdims=True)
        gs = (prob * (gp - delta) * scale).astype(bf16)
        dq[at, :] = dot(gs, ki)
        dk[:end, :] += dot(gs, qi, ((0,), (0,)))
        dv[:end, :] += dot(half, gi, ((0,), (0,)))


class Reduce:
    def __init__(self, place, grads, rc, total, acc, lo, r, rz, tp, sems):
        self.p, self.grads, self.rc, self.total = place, grads, rc, total
        self.acc, self.lo, self.r, self.rz, self.tp = acc, lo, r, rz, tp
        self.csem, self.ksem, self.zsem, self.gsem, self.lsem, self.tsem = sems
        self.cols = acc.shape[3]
        self.parts = total.shape[2] // self.cols
        self.rows = total.shape[1] // place.replicas
        self.units = total.shape[0] * self.parts
        self.n = place.shards - 1
        self.stages = 2 * place.steps + 5
        self.ticks = self.units + (self.stages - 1) * RLAG

    def where(self, u):
        t, part = u // self.parts, u % self.parts
        return t, pl.ds(pl.multiple_of(part * self.cols, self.cols), self.cols)

    def band(self, first, count):
        return pl.ds(pl.multiple_of(first * self.rows, self.rows), count * self.rows)

    def loads(self, u):
        t, cols = self.where(u)
        a, b = u % self.acc.shape[0], u % self.lo.shape[0]
        own = self.grads.at[t, :, self.band(self.p.base, self.p.half), cols]
        return (
            pltpu.make_async_copy(self.rc.at[u], self.acc.at[a], self.lsem.at[0, a]),
            pltpu.make_async_copy(own, self.lo.at[b], self.lsem.at[1, b]),
        )

    def core_copy(self, u):
        t, cols = self.where(u)
        src = self.grads.at[t, :, self.band(self.p.twin_base, self.p.half), cols]
        return remote(src, self.rc.at[u], self.csem.at[0, u], self.csem.at[1, u], self.p.twin)

    def held(self, k, u):
        p = self.p
        return (self.acc.at[u % self.acc.shape[0]], 0) if k == p.steps else (self.r[k].at[u], p.mine[k])

    def plane_copy(self, k, u):
        ref, first = self.held(k + 1, u)
        src = ref.at[:, self.band(self.p.theirs[k] - first, 2**k), :]
        return remote(src, self.r[k].at[u], self.ksem.at[0, k, u], self.ksem.at[1, k, u], self.p.partner[k])

    def shard_copy(self, u, d):
        to = self.p.across(d)
        src = self.held(0, u)[0].at[to[1]]
        return remote(src, self.rz.at[u, d - 1], self.zsem.at[0, u, d - 1], self.zsem.at[1, u, d - 1], to)

    def piece_copy(self, u):
        t, cols = self.where(u)
        return pltpu.make_async_copy(self.tp.at[u], self.total.at[t, self.band(self.p.piece, 1), cols], self.tsem.at[u])

    def total_copy(self, k, u):
        p = self.p
        t, cols = self.where(u)
        first, count, peer = (
            (p.base + p.mine[k], 2**k, p.partner[k]) if k < p.steps else (p.base, p.half, p.twin)
        )
        ref = self.total.at[t, self.band(first, count), cols]
        return remote(ref if k else self.tp.at[u], ref, self.gsem.at[0, k, u], self.gsem.at[1, k, u], peer)

    def add(self, stage, u):
        p = self.p
        if stage == 1:
            self.core_copy(u).wait_recv()
            ring = self.acc.shape[0]

            @pl.when(u >= ring)
            def _():
                self.plane_copy(p.steps - 1, u - ring).wait_send()

            for c in self.loads(u):
                c.start()
        elif stage == 2:
            for c in self.loads(u):
                c.wait()
            a = u % self.acc.shape[0]
            self.acc[a] = self.acc[a] + self.lo[u % self.lo.shape[0]]
        elif 2 < stage < 3 + p.steps:
            k = p.steps - (stage - 2)
            self.plane_copy(k, u).wait_recv()
            ref, first = self.held(k + 1, u)
            self.r[k][u] = self.r[k][u] + ref[:, self.band(p.mine[k] - first, 2**k), :]
        elif stage == 3 + p.steps:
            for d in range(1, self.n + 1):
                self.shard_copy(u, d).wait_recv()
            acc = self.held(0, u)[0][p.s].astype(f32)
            for d in range(1, self.n + 1):
                acc += self.rz[u, d - 1].astype(f32)
            self.tp[u] = acc.astype(bf16)
        elif stage > 3 + p.steps:
            k = stage - 4 - p.steps
            self.total_copy(k, u).wait_recv()
            if k == 0:
                self.piece_copy(u).wait()

    def send(self, stage, u):
        p = self.p
        if stage == 0:
            self.core_copy(u).start()
        elif 2 <= stage < 2 + p.steps:
            self.plane_copy(p.steps - 1 - (stage - 2), u).start()
        elif stage == 2 + p.steps:
            for d in range(1, self.n + 1):
                self.shard_copy(u, d).start()
        elif 3 + p.steps <= stage < self.stages - 1:
            if stage == 3 + p.steps:
                self.piece_copy(u).start()
            self.total_copy(stage - 3 - p.steps, u).start()

    def tick(self, u):
        for do in (self.add, self.send):
            for stage in range(self.stages):
                v = u - stage * RLAG

                @pl.when((v >= 0) & (v < self.units))
                def _(stage=stage, v=v):
                    do(stage, v)

    def finish(self):
        @pl.loop(0, self.units)
        def _(u):
            self.core_copy(u).wait_send()
            for k in range(self.p.steps - 1):
                self.plane_copy(k, u).wait_send()

            @pl.when(u >= self.units - self.acc.shape[0])
            def _():
                self.plane_copy(self.p.steps - 1, u).wait_send()

            for d in range(1, self.n + 1):
                self.shard_copy(u, d).wait_send()
            for k in range(self.p.steps + 1):
                self.total_copy(k, u).wait_send()


def step_kernel(
    replicas, shards, hidden, grad_scale,
    qkv_w, out_w, up_w, down_w, cot, vec, tok, seg_row, freq,
    grads, rc, total, bout, ig, vshare,
    wg, acc, lo, *rest,
):
    steps = int(math.log2(replicas)) - 1
    r, rest = rest[:steps], rest[steps:]
    rz, tp, x_in, x_in_t, gout, out_acc, gmlp, gattn, gtile, grows, cosines, sines, mean, inverse, *rest = rest
    qb, kb, vb, gb, ctx, dq, dk, dv, vg, vgrad, vz, vx, *rest = rest
    gsend, grecv, csem, ksem, zsem, tsem, lsem, psem, own_sem, ssem, vsem, vzsem, vxsem, isem = rest
    p = Place(replicas, shards)
    g = Gather(p, wg, gsend, grecv)
    red = Reduce(p, grads, rc, total, acc, lo, r, rz, tp, (csem, ksem, zsem, tsem, lsem, psem))
    chunks, _, rows, model = wg.shape
    tokens = tok.shape[0]
    ff_chunks = hidden // model
    tiles = model // TILE
    per_tile = TILE // rows
    head = model // H
    scale = head ** (-0.5)
    per_head = head // rows
    chunk0 = 2 * ff_chunks
    width = vec.shape[1]
    wide = hidden // shards
    o_out, o_up, o_down = 7 * model, 8 * model, 8 * model + hidden
    band = 64

    def start(copies):
        for c in copies:
            c.start()

    def wait(copies):
        for c in copies:
            c.wait()

    def bands(body):
        @pl.loop(0, tokens // band)
        def _(i):
            body(pl.ds(pl.multiple_of(i * band, band), band))

    def lanes(body):
        for i in range(tokens // LANES):
            body(slice(i * LANES, (i + 1) * LANES))

    def loads(t):
        slot, j = t % RAW, t // 2
        dst, sem = gattn.at[slot * rows : (slot + 1) * rows, :], own_sem.at[slot]
        if t >= chunk0:
            i = t - chunk0
            src = qkv_w.at[:, i * model : (i + 1) * model] if i < 3 else out_w
            return [pltpu.make_async_copy(src, dst, sem.at[0])]
        if t % 2:
            return [pltpu.make_async_copy(down_w.at[j * rows : (j + 1) * rows, :], dst, sem.at[0])]
        return [
            pltpu.make_async_copy(
                up_w.at[:, i * wide + j * rows : i * wide + (j + 1) * rows],
                dst.at[:, i * rows : (i + 1) * rows],
                sem.at[i],
            )
            for i in range(shards)
        ]

    def part(shard):
        return pl.ds(pl.multiple_of(shard * width, LANES), width)

    def gather_vec(d):
        ref = vg.at[:, part(p.s)]
        return remote(ref, ref, vsem.at[0, d - 1], vsem.at[1, d - 1], p.across(d))

    cot_copy = pltpu.make_async_copy(cot, gout, isem.at[0])
    for t in range(RAW):
        start(loads(t))
    cot_copy.start()
    vg[:, part(p.s)] = vec[...].astype(bf16).astype(f32)
    p.greet()
    start([gather_vec(d) for d in range(1, shards)])
    for t in range(chunks):
        wait(loads(t))

        @pl.loop(0, rows // CAST)
        def _(i, t=t):
            at = pl.multiple_of(i * CAST, CAST)
            wg[t, p.s, pl.ds(at, CAST), :] = gattn[pl.ds((t % RAW) * rows + at, CAST), :].astype(bf16)

        if t + RAW < chunks:
            start(loads(t + RAW))
        if 1 <= t <= AHEAD:
            g.launch(t - 1)

    def statistics(at):
        x = tok[at, :].astype(f32)
        m = jnp.mean(x, axis=1, keepdims=True)
        centred = x - m
        mean[at, :] = m
        inverse[at, :] = lax.rsqrt(jnp.mean(centred * centred, axis=1, keepdims=True) + norm_eps)

    def normed(at):
        return (tok[at, :].astype(f32) - mean[at, :]) * inverse[at, :]

    bands(statistics)
    cot_copy.wait()

    def tables(at):
        seg = column(seg_row[:, at])
        gout[at, :] = (gout[at, :].astype(f32) * (seg >= 0.0).astype(f32)).astype(bf16)
        cosines[at, :], sines[at, :] = rotary_rows(seg, seg_row[...], at.start, freq[...])

    lanes(tables)
    for d in range(1, shards):
        gather_vec(d).wait_recv()

    def enter_mlp(at):
        x_in[at, :] = (normed(at) * vg[:, 2 * model : 3 * model] + vg[:, 3 * model : 4 * model]).astype(bf16)
        bias = vg[:, o_down : o_down + model] + vg[:, o_out : o_out + model]
        out_acc[at, :] = tok[at, :].astype(f32) + bias
        gmlp[at, :] = jnp.zeros((band, model), f32)

    def turn(at):
        x_in_t[:, at] = x_in[at, :].T

    bands(enter_mlp)
    lanes(turn)
    vgrad[...] = jnp.zeros_like(vgrad)

    first = g.ready(1)
    per_block = 2 * g.n

    @pl.loop(0, first)
    def _(u):
        g.tick(u)

    def tile_stores(i):
        slot, j, n = i % 2, i // tiles, i % tiles
        cols = pl.ds(pl.multiple_of(n * TILE, TILE), TILE)
        return (
            pltpu.make_async_copy(gtile.at[slot, 0], grads.at[2 * j, :, :, cols], ssem.at[slot, 0]),
            pltpu.make_async_copy(
                grows.at[slot], grads.at[2 * j + 1, pl.ds(n * per_tile, per_tile)], ssem.at[slot, 3]
            ),
        )

    def head_stores(h):
        slot = h % 2
        cols = pl.ds(pl.multiple_of(h * head, head), head)
        out = [
            pltpu.make_async_copy(gtile.at[slot, w], grads.at[chunk0 + w, :, :, cols], ssem.at[slot, w])
            for w in range(3)
        ]
        last = grads.at[chunk0 + 3, pl.ds(h * per_head, per_head)]
        return (*out, pltpu.make_async_copy(grows.at[slot], last, ssem.at[slot, 3]))

    def reduced(i):
        return jnp.maximum(i - EARLY, 0) * TICKS_8 // 8

    @pl.loop(0, ff_chunks * tiles)
    def _(i):
        slot, j, n = i % 2, i // tiles, i % tiles
        lo_tick, hi_tick = first + (i * per_block) // tiles, first + ((i + 1) * per_block) // tiles
        most = -(-per_block // tiles)
        cols = pl.ds(pl.multiple_of(n * TILE, TILE), TILE)

        def maybe(a):
            @pl.when((lo_tick + a < hi_tick) & (lo_tick + a < g.ticks))
            def _():
                g.tick(lo_tick + a)

        @pl.when(i >= 2)
        def _():
            wait(tile_stores(i - 2))

        maybe(0)

        @pl.when(reduced(i) < reduced(i + 1))
        def _():
            red.tick(reduced(i))

        def between():
            for a in range(1, most):
                maybe(a)

        def keep(which, x):
            if which:
                grows[slot] = x.reshape(per_tile, rows, model)
            else:
                gtile[slot, 0] = x.reshape(shards, rows, TILE)

        feed_forward(
            wg[2 * j, :, :, cols].reshape(model, TILE),
            wg[2 * j + 1, pl.ds(n * per_tile, per_tile)].reshape(TILE, model),
            flat_columns(n, j, rows, wide),
            rows, o_up, grad_scale, x_in, x_in_t, gout, vg, vgrad, out_acc, gmlp, between, keep,
        )
        start(tile_stores(i))

    items = ff_chunks * tiles
    done = max(items - EARLY, 0) * TICKS_8 // 8

    def enter_attention(at):
        x_in[at, :] = (normed(at) * vg[:, :model] + vg[:, model : 2 * model]).astype(bf16)
        gattn[at, :] = jnp.zeros((band, model), f32)

    bands(enter_attention)
    lanes(turn)

    @pl.loop(first + ff_chunks * per_block, g.ticks)
    def _(u):
        g.tick(u)

    @pl.loop(0, H)
    def _(h):
        slot = h % 2

        @pl.when(h < 2)
        def _():
            wait(tile_stores(items - 2 + h))

        @pl.when(h >= 2)
        def _():
            wait(head_stores(h - 2))

        red.tick(done + 2 * h)
        cols = pl.ds(pl.multiple_of(h * head, head), head)
        mine = pl.ds(h * per_head, per_head)

        def weight(i):
            return wg[chunk0 + i, :, :, cols].reshape(model, head)

        def at_head(base):
            return pl.ds(pl.multiple_of(base + h * head, head), head)

        def project(i):
            return dot(x_in[...], weight(i)) + vg[:, at_head((4 + i) * model)]

        wo = wg[chunk0 + 3, mine].reshape(head, model)
        qb[...] = turned(project(0), cosines[...], sines[...], 1.0).astype(bf16)
        kb[...] = turned(project(1), cosines[...], sines[...], 1.0).astype(bf16)
        vb[...] = project(2).astype(bf16)
        gb[...] = dot(gout[...], wo, ((1,), (1,))).astype(bf16)
        one_head(LANES, qb, kb, vb, gb, ctx, dq, dk, dv, seg_row, scale)
        red.tick(done + 2 * h + 1)
        back = (
            turned(dq[...], cosines[...], sines[...], -1.0),
            turned(dk[...], cosines[...], sines[...], -1.0),
            dv[...],
        )
        sums = gattn[...]
        for i, d in enumerate(back):
            vgrad[:, at_head((4 + i) * model)] = jnp.sum(d, axis=0, keepdims=True) * grad_scale
            half = d.astype(bf16)
            sums += dot(half, weight(i), ((1,), (1,)))
            gtile[slot, i] = (dot(x_in_t[...], half) * grad_scale).astype(bf16).reshape(shards, rows, head)
        gattn[...] = sums
        out_acc[...] += dot(ctx[...], wo)
        grows[slot] = (
            (dot(ctx[...], gout[...], ((0,), (0,))) * grad_scale).astype(bf16).reshape(per_head, rows, model)
        )
        start(head_stores(h))

    done += 2 * H
    gain_one, gain_two = vg[:, :model], vg[:, 2 * model : 3 * model]

    def last(i, carry):
        at = pl.ds(pl.multiple_of(i * band, band), band)
        x, ga, gm, go = normed(at), gattn[at, :], gmlp[at, :], gout[at, :].astype(f32)
        gn = ga * gain_one + gm * gain_two
        m1 = jnp.mean(gn, axis=1, keepdims=True)
        m2 = jnp.mean(gn * x, axis=1, keepdims=True)
        gout[at, :] = (go + inverse[at, :] * (gn - m1 - x * m2)).astype(bf16)
        terms = (ga * x, ga, gm * x, gm, go)
        return tuple(a + jnp.sum(b, axis=0, keepdims=True) for a, b in zip(carry, terms))

    zero = jnp.zeros((1, model), f32)
    sums = lax.fori_loop(0, tokens // band, last, (zero,) * 5)
    for x, place in zip((*sums, sums[4]), (0, model, 2 * model, 3 * model, o_out, o_down)):
        vgrad[:, place : place + model] = x * grad_scale

    def leave(at):
        live = (column(seg_row[:, at]) >= 0.0).astype(f32)
        x_in[at, :] = (live * out_acc[at, :]).astype(bf16)

    lanes(leave)
    vgrad[...] = vgrad[...].astype(bf16).astype(f32)
    results = (pltpu.make_async_copy(x_in, bout, isem.at[0]), pltpu.make_async_copy(gout, ig, isem.at[1]))
    start(results)
    for h in range(H - 2, H):
        wait(head_stores(h))

    def vcopy(d):
        to = p.across(d)
        return remote(vgrad.at[:, part(to[1])], vz.at[d - 1], vzsem.at[0, d - 1], vzsem.at[1, d - 1], to)

    peers = [*p.partner, p.twin]

    def vexchange(k):
        return remote(vx.at[2 * k], vx.at[2 * k + 1], vxsem.at[0, k], vxsem.at[1, k], peers[k])

    def vstart(i):
        start([vcopy(d) for d in range(1, shards)] if i == 0 else [vexchange(i - 1)])

    def vfinish(i):
        if i == 0:
            acc = vgrad[:, part(p.s)]
            for d in range(1, shards):
                vcopy(d).wait_recv()
                acc += vz[d - 1]
        else:
            vexchange(i - 1).wait_recv()
            acc = vx[2 * i - 2] + vx[2 * i - 1]
        if i < len(peers):
            vx[2 * i] = acc
        else:
            vshare[...] = acc

    for i in range(len(peers) + 1):
        vstart(i)
        red.tick(done + i)
        vfinish(i)
    done += len(peers) + 1

    @pl.loop(done, red.ticks)
    def _(u):
        red.tick(u)

    for d in range(1, shards):
        gather_vec(d).wait_send()
        vcopy(d).wait_send()
    for i in range(len(peers)):
        vexchange(i).wait_send()
    g.finish()
    red.finish()
    wait(results)


def step_call(mesh, qkv, out, up, down, vec, tok, cot, seg_row, grad_scale):
    replicas, shards = mesh.shape["replica"], mesh.shape["shard"]
    rows, hidden = up.shape
    tokens, model = tok.shape
    chunks = 2 * (hidden // model) + 4
    steps = int(math.log2(replicas)) - 1
    stages = steps + 2
    width = vec.shape[1]
    gather_units = chunks * (shards - 1)
    units, cols, piece = chunks * PARTS, model // PARTS, rows // replicas
    part = 2**steps * piece
    head = model // H
    freq = rope_base ** (-2.0 * (jnp.arange(LANES) % (ROT // 2)).astype(f32) / ROT)[None]
    sds, vm = jax.ShapeDtypeStruct, pltpu.VMEM
    return pl.pallas_call(
        functools.partial(step_kernel, replicas, shards, hidden, grad_scale),
        out_shape=[
            sds((chunks, shards, rows, model), bf16),
            sds((units, shards, part, cols), bf16),
            sds((chunks, rows, model), bf16),
            sds((tokens, model), bf16),
            sds((tokens, model), bf16),
            sds((1, width), f32),
        ],
        in_specs=[ANY] * 5 + [VMEM] * 4,
        out_specs=[ANY] * 5 + [VMEM],
        scratch_shapes=[
            vm((chunks, shards, rows, model), bf16),
            vm((2 * RLAG + 1, shards, part, cols), bf16),
            vm((RLAG + 1, shards, part, cols), bf16),
            *(vm((units, shards, 2**k * piece, cols), bf16) for k in range(steps)),
            vm((units, shards - 1, piece, cols), bf16),
            vm((units, piece, cols), bf16),
            vm((tokens, model), bf16),
            vm((model, tokens), bf16),
            vm((tokens, model), bf16),
            *[vm((tokens, model), f32)] * 3,
            vm((2, 3, shards, rows, head), bf16),
            vm((2, head // rows, rows, model), bf16),
            *[vm((tokens, LANES), f32)] * 2,
            *[vm((tokens, 1), f32)] * 2,
            *[vm((tokens, head), bf16)] * 5,
            *[vm((tokens, head), f32)] * 3,
            *[vm((1, width * shards), f32)] * 2,
            vm((shards - 1, 1, width), f32),
            vm((2 * steps + 2, 1, width), f32),
            DMA((stages, gather_units)),
            DMA((stages, gather_units)),
            DMA((2, units)),
            DMA((2, steps, units)),
            DMA((2, units, shards - 1)),
            DMA((2, steps + 1, units)),
            DMA((2, 2 * RLAG + 1)),
            DMA((units,)),
            DMA((RAW, shards)),
            DMA((2, 4)),
            DMA((2, shards - 1)),
            DMA((2, shards - 1)),
            DMA((2, steps + 1)),
            DMA((2,)),
        ],
        compiler_params=pltpu.CompilerParams(
            collective_id=0, has_side_effects=True, vmem_limit_bytes=67043328
        ),
        name="step",
    )(qkv, out, up, down, cot, vec, tok, seg_row, freq)


def adam(master, first, second, gradient, decay):
    first = beta_first * first + (1.0 - beta_first) * gradient
    second = beta_second * second + (1.0 - beta_second) * gradient * gradient
    a = first / (1.0 - beta_first**STEP)
    b = second / (1.0 - beta_second**STEP)
    return master - learn_rate * (a / (jnp.sqrt(b) + adam_eps) + decay * master), first, second


class Weight:
    def __init__(self, band, count, blocks, chunks_of, refs, bufs, sems):
        self.band, self.count, self.blocks, self.chunks_of = band, count, blocks, chunks_of
        self.total, self.w, self.m, self.grad, self.new_w, self.new_m = refs
        self.gbuf, self.wbuf, self.mbuf, self.outbuf = bufs
        self.isem, self.osem = sems

    def loads(self, i):
        slot, at = i % 2, slice(i * self.band, (i + 1) * self.band)
        pairs = [(self.w.at[at, :], self.wbuf.at[slot]), (self.m.at[:, at, :], self.mbuf.at[slot])]
        for n, (chunk, row) in enumerate(self.chunks_of(i)):
            pairs.append((self.total.at[chunk, row : row + self.band, :], self.gbuf.at[slot, n]))
        return [pltpu.make_async_copy(a, b, self.isem.at[slot, n]) for n, (a, b) in enumerate(pairs)]

    def stores(self, i):
        slot, at = i % 2, slice(i * self.band, (i + 1) * self.band)
        pairs = [
            (self.wbuf.at[slot], self.new_w.at[at, :]),
            (self.mbuf.at[slot], self.new_m.at[:, at, :]),
            (self.outbuf.at[slot], self.grad.at[at, :]),
        ]
        return [pltpu.make_async_copy(a, b, self.osem.at[slot, n]) for n, (a, b) in enumerate(pairs)]

    def compute(self, i):
        slot = i % 2
        for col, width, n, gcol in self.blocks:
            high = min(self.band, max(16, 16384 // width))

            @pl.loop(0, self.band // high)
            def _(b, col=col, width=width, n=n, gcol=gcol, high=high):
                at, cols = pl.ds(pl.multiple_of(b * high, high), high), slice(col, col + width)
                g = self.gbuf[slot, n, at, gcol : gcol + width].astype(f32)
                self.outbuf[slot, at, cols] = g
                w, first, second = adam(
                    self.wbuf[slot, at, cols], self.mbuf[slot, 0, at, cols], self.mbuf[slot, 1, at, cols], g, weight_decay
                )
                self.wbuf[slot, at, cols] = w
                self.mbuf[slot, 0, at, cols] = first
                self.mbuf[slot, 1, at, cols] = second


def adam_plans(rows, model, hidden, shards):
    ff = hidden // model
    wide = hidden // shards
    band = min(rows, 64)
    return (
        (band, rows // band, [(i * model, model, i, 0) for i in range(3)],
         lambda b: [(2 * ff + i, b * band) for i in range(3)], 3, 3 * model),
        (rows, 1, [(0, model, 0, 0)], lambda b: [(2 * ff + 3, 0)], 1, model),
        (band, rows // band,
         [(i * wide + j * rows, rows, j, i * rows) for i in range(shards) for j in range(ff)],
         lambda b: [(2 * j, b * band) for j in range(ff)], ff, hidden),
        (rows, ff, [(0, model, 0, 0)], lambda b: [(2 * b + 1, 0)], 1, model),
    )


def adam_kernel(plans, total, *refs):
    ws, ms, grads, new_ws, new_ms, rest = refs[:4], refs[4:8], refs[8:12], refs[12:16], refs[16:20], refs[20:]
    weights = []
    for n, (band, count, blocks, chunks_of, _, _) in enumerate(plans):
        bufs, sems = rest[6 * n : 6 * n + 4], rest[6 * n + 4 : 6 * n + 6]
        weights.append(
            Weight(band, count, blocks, chunks_of, (total, ws[n], ms[n], grads[n], new_ws[n], new_ms[n]), bufs, sems)
        )
    most = max(w.count for w in weights)
    order = [(w, i) for i in range(most) for w in weights if i < w.count]
    for w, i in order:
        if i < 2:
            for c in w.loads(i):
                c.start()
    for w, i in order:
        if i >= 1 and i + 1 < w.count:
            for c in w.stores(i - 1):
                c.wait()
            for c in w.loads(i + 1):
                c.start()
        for c in w.loads(i):
            c.wait()
        w.compute(i)
        for c in w.stores(i):
            c.start()
    for w, i in order:
        if i + 2 >= w.count:
            for c in w.stores(i):
                c.wait()


def adam_call(total, ws, ms, hidden, shards):
    _, rows, model = total.shape
    plans = adam_plans(rows, model, hidden, shards)
    sds = jax.ShapeDtypeStruct
    scratch = []
    for band, _, _, _, parts, cols in plans:
        scratch += [
            pltpu.VMEM((2, parts, band, model), bf16),
            pltpu.VMEM((2, band, cols), f32),
            pltpu.VMEM((2, 2, band, cols), f32),
            pltpu.VMEM((2, band, cols), f32),
            DMA((2, 2 + parts)),
            DMA((2, 3)),
        ]
    like = [sds(w.shape, f32) for w in ws]
    out = pl.pallas_call(
        functools.partial(adam_kernel, plans),
        out_shape=like + like + [sds(m.shape, f32) for m in ms],
        in_specs=[ANY] * 9,
        out_specs=[ANY] * 12,
        scratch_shapes=scratch,
        compiler_params=pltpu.CompilerParams(vmem_limit_bytes=60 << 20),
        name="adam",
    )(total, *ws, *ms)
    return out[:4], out[4:8], out[8:]


def local(mesh, tokens, cotangent, seg_ids, qkv, out, up, down, vectors, *moments):
    shards = mesh.shape["shard"]
    hidden = up.shape[1]
    grad_scale = (tokens.shape[0] * mesh.shape["replica"] * shards) ** (-0.5)
    _, _, total, block_output, input_grad, vshare = step_call(
        mesh, qkv, out, up, down, vectors[None], tokens, cotangent, seg_ids[None], grad_scale
    )
    grads, updated, renewed = adam_call(total, (qkv, out, up, down), moments[:4], hidden, shards)
    vsum = vshare[0]
    new_v, *vm = adam(vectors, moments[4][0], moments[4][1], vsum, 0.0)
    return (block_output, input_grad, *grads, vsum, *updated, new_v, *renewed, jnp.stack(vm))


def solution(mesh):
    rows = P(("replica", "shard"), None)
    first, second = P("shard", None), P(None, "shard", None)
    weights, moments = (first,) * 4 + (P("shard"),), (second,) * 4 + (P(None, "shard"),)
    return jax.shard_map(
        functools.partial(local, mesh),
        mesh=mesh,
        in_specs=(rows, rows, P(("replica", "shard")), *weights, *moments),
        out_specs=(rows, rows, *weights, *weights, *moments),
        check_vma=False,
    )
```

```python
import functools
import math

import jax
import jax.numpy as jnp
from jax import lax
from jax.experimental import pallas as pl
from jax.experimental.pallas import tpu as pltpu
from jax.sharding import PartitionSpec as P

H = 4
ROT = 64
STEP = 3
norm_eps = 1e-05
rope_base = 10000.0
learn_rate = 0.01
beta_first = 0.9
beta_second = 0.95
adam_eps = 1e-08
weight_decay = 0.1
root_half = 0.7071067811865476
inv_root_tau = 0.3989422804014327

MESH = pl.DeviceIdType.MESH
f32, bf16 = jnp.float32, jnp.bfloat16
ANY = pl.BlockSpec(memory_space=pl.ANY)
VMEM = pl.BlockSpec(memory_space=pltpu.VMEM)
DMA = pltpu.SemaphoreType.DMA
TILE = 256
LANES = 128
PARTS = 2
SLOW, QUICK = 2, 1
RAW = 2
CAST = 64
EARLY = 5
TICKS_8 = 6
HEAD_TICKS = 1
LAG = 2
AHEAD = 3


class Place:
    def __init__(self, replicas, shards):
        self.replicas, self.shards = replicas, shards
        self.steps = int(math.log2(replicas)) - 1
        self.half = 2**self.steps
        self.r = lax.axis_index("replica")
        self.s = lax.axis_index("shard")
        self.core = self.r % 2
        self.m = self.mixed(self.r // 2)
        self.base = self.core * self.half
        self.twin_base = (1 - self.core) * self.half
        self.piece = self.base + self.m
        self.twin = (self.r + 1 - 2 * self.core, self.s)
        self.partner, self.mine, self.theirs = [], [], []
        for k in range(self.steps):
            flip = 2**k
            other = self.m + flip * (1 - 2 * ((self.m // flip) % 2))
            self.partner.append((2 * self.mixed(other) + self.core, self.s))
            self.mine.append((self.m // flip) * flip)
            self.theirs.append((other // flip) * flip)

    def mixed(self, plane):
        n = self.steps
        turned = sum(((plane // 2**i) % 2) * 2 ** (n - 1 - i) for i in range(n))
        return (1 - self.core) * plane + self.core * turned

    def across(self, d):
        return (self.r, (self.s + d) % self.shards)

    def source(self, d):
        return (self.s + self.shards - d) % self.shards

    def greet(self):
        barrier = pltpu.get_barrier_semaphore()
        peers = [self.across(d) for d in range(1, self.shards)] + self.partner + [self.twin]
        for peer in peers:
            pl.semaphore_signal(barrier, inc=1, device_id=peer, device_id_type=MESH)
        pl.semaphore_wait(barrier, len(peers))


def remote(src, dst, send, recv, peer):
    return pltpu.make_async_remote_copy(
        src_ref=src, dst_ref=dst, send_sem=send, recv_sem=recv, device_id=peer, device_id_type=MESH
    )


class Gather:
    def __init__(self, place, wg, send, recv):
        self.p, self.wg, self.send, self.recv = place, wg, send, recv
        self.chunks = wg.shape[0]
        self.rows = wg.shape[2] // place.replicas
        self.stages = place.steps + 2
        self.n = place.shards - 1
        self.units = self.chunks * self.n
        self.ticks = self.units + (self.stages - 1) * LAG

    def span(self, t, shard, first, count):
        start = pl.multiple_of(first * self.rows, self.rows)
        return self.wg.at[t, shard, pl.ds(start, count * self.rows), :]

    def copy(self, stage, t, d):
        p = self.p
        if stage == 0:
            ref, peer = self.span(t, p.s, p.piece, 1), p.across(d)
        elif stage <= p.steps:
            k = stage - 1
            ref, peer = self.span(t, p.source(d), p.base + p.mine[k], 2**k), p.partner[k]
        else:
            ref, peer = self.span(t, p.source(d), p.base, p.half), p.twin
        u = t * self.n + d - 1
        return remote(ref, ref, self.send.at[stage, u], self.recv.at[stage, u], peer)

    def launch(self, t):
        for d in range(1, self.n + 1):
            self.copy(0, t, d).start()

    def ready(self, t):
        return (t + 1) * self.n + (self.stages - 1) * LAG

    def tick(self, u):
        for stage in range(self.stages):
            v = u - stage * LAG

            @pl.when((v >= 0) & (v < self.units))
            def _(stage=stage, v=v):
                t, d = v // self.n, v % self.n + 1
                self.copy(stage, t, d).wait_recv()
                if stage + 1 < self.stages:
                    self.copy(stage + 1, t, d).start()

        @pl.when((u % self.n == self.n - 1) & (u // self.n + AHEAD < self.chunks))
        def _():
            self.launch(u // self.n + AHEAD)

    def finish(self):
        @pl.loop(0, self.chunks)
        def _(t):
            for d in range(1, self.n + 1):
                for stage in range(self.stages):
                    self.copy(stage, t, d).wait_send()


def dot(a, b, dims=((1,), (0,))):
    return lax.dot_general(a, b, (dims, ((), ())), preferred_element_type=f32)


def column(row):
    return jnp.broadcast_to(row.astype(f32), (8, row.shape[1])).T[:, :1]


def rotary_rows(seg, seg_row, start, freq):
    shape = (seg.shape[0], seg_row.shape[1])
    row = lax.broadcasted_iota(jnp.int32, shape, 0) + start
    col = lax.broadcasted_iota(jnp.int32, shape, 1)
    before = (seg == seg_row.astype(f32)) & (col < row)
    position = jnp.sum(before.astype(f32), axis=1, keepdims=True)
    angles = position * freq
    lane = lax.broadcasted_iota(jnp.int32, angles.shape, 1)
    cosine, sine = jnp.cos(angles), jnp.sin(angles)
    sine = jnp.where(lane < ROT // 2, -sine, sine)
    return jnp.where(lane < ROT, cosine, 1.0), jnp.where(lane < ROT, sine, 0.0)


def flat_columns(tile, j, rows, wide):
    per_tile = TILE // rows
    return [pl.multiple_of((tile * per_tile + i) * wide + j * rows, rows) for i in range(per_tile)]


def feed_forward(up, down, flats, rows, o_up, grad_scale, mlp_in, mlp_in_t, gout, vg, vgrad, mlp, gmlp, between, keep):
    bias = jnp.concatenate([vg[:, pl.ds(o_up + f, rows)] for f in flats], axis=1)
    h = dot(mlp_in[...], up) + bias
    cum = 0.5 * (1.0 + lax.erf(h * root_half))
    density = jnp.exp(-0.5 * h * h) * inv_root_tau
    act = (h * cum).astype(bf16)
    gh = dot(gout[...], down, ((1,), (1,))) * (cum + h * density)
    ghh = gh.astype(bf16)
    total = jnp.sum(gh, axis=0, keepdims=True) * grad_scale
    for i, f in enumerate(flats):
        vgrad[:, pl.ds(o_up + f, rows)] = total[:, i * rows : (i + 1) * rows]
    between()
    mlp[...] += dot(act, down)
    keep(1, (dot(act, gout[...], ((0,), (0,))) * grad_scale).astype(bf16))
    gmlp[...] += dot(ghh, up, ((1,), (1,)))
    keep(0, (dot(mlp_in_t[...], ghh) * grad_scale).astype(bf16))


def turned(x, cosines, sines, sign):
    first = x[:, :LANES]
    lane = lax.broadcasted_iota(jnp.int32, first.shape, 1)
    other = jnp.where(lane < ROT // 2, pltpu.roll(first, LANES - ROT // 2, 1), pltpu.roll(first, ROT // 2, 1))
    return jnp.concatenate([first * cosines + sign * (other * sines), x[:, LANES:]], axis=1)


def one_head(band, q, k, v, gctx, ctx, dq, dk, dv, seg_row, scale):
    dk[...] = jnp.zeros_like(dk)
    dv[...] = jnp.zeros_like(dv)
    for i in range(q.shape[0] // band):
        at, end = slice(i * band, (i + 1) * band), (i + 1) * band
        qi, gi, ki, vi = q[at, :], gctx[at, :], k[:end, :], v[:end, :]
        row = lax.broadcasted_iota(jnp.int32, (band, end), 0) + i * band
        col = lax.broadcasted_iota(jnp.int32, (band, end), 1)
        allowed = (column(seg_row[:, at]) == seg_row[:, :end].astype(f32)) & (col <= row)
        masked = jnp.where(allowed, dot(qi, ki, ((1,), (1,))) * scale, -jnp.inf)
        largest = jnp.max(masked, axis=1, keepdims=True)
        log_total = largest + jnp.log(jnp.sum(jnp.exp(masked - largest), axis=1, keepdims=True))
        prob = jnp.exp(masked - log_total)
        half = prob.astype(bf16)
        ctx[at, :] = dot(half, vi).astype(bf16)
        gp = dot(gi, vi, ((1,), (1,)))
        delta = jnp.sum(prob * gp, axis=1, keepdims=True)
        gs = (prob * (gp - delta) * scale).astype(bf16)
        dq[at, :] = dot(gs, ki)
        dk[:end, :] += dot(gs, qi, ((0,), (0,)))
        dv[:end, :] += dot(half, gi, ((0,), (0,)))


def reduce_lags(steps):
    lags = [0]
    for gap in [QUICK] * 2 + [SLOW] * (2 * steps + 2):
        lags.append(lags[-1] + gap)
    return lags


class Reduce:
    def __init__(self, place, grads, rc, total, acc, lo, r, rz, tp, sems):
        self.p, self.grads, self.rc, self.total = place, grads, rc, total
        self.acc, self.lo, self.r, self.rz, self.tp = acc, lo, r, rz, tp
        self.csem, self.ksem, self.zsem, self.gsem, self.lsem, self.tsem = sems
        self.cols = acc.shape[3]
        self.parts = total.shape[2] // self.cols
        self.rows = total.shape[1] // place.replicas
        self.units = total.shape[0] * self.parts
        self.n = place.shards - 1
        self.lags = reduce_lags(place.steps)
        self.stages = len(self.lags)
        self.ticks = self.units + self.lags[-1]

    def where(self, u):
        t, part = u // self.parts, u % self.parts
        return t, pl.ds(pl.multiple_of(part * self.cols, self.cols), self.cols)

    def band(self, first, count):
        return pl.ds(pl.multiple_of(first * self.rows, self.rows), count * self.rows)

    def loads(self, u):
        t, cols = self.where(u)
        a, b = u % self.acc.shape[0], u % self.lo.shape[0]
        own = self.grads.at[t, :, self.band(self.p.base, self.p.half), cols]
        return (
            pltpu.make_async_copy(self.rc.at[u], self.acc.at[a], self.lsem.at[0, a]),
            pltpu.make_async_copy(own, self.lo.at[b], self.lsem.at[1, b]),
        )

    def core_copy(self, u):
        t, cols = self.where(u)
        src = self.grads.at[t, :, self.band(self.p.twin_base, self.p.half), cols]
        return remote(src, self.rc.at[u], self.csem.at[0, u], self.csem.at[1, u], self.p.twin)

    def held(self, k, u):
        p = self.p
        return (self.acc.at[u % self.acc.shape[0]], 0) if k == p.steps else (self.r[k].at[u], p.mine[k])

    def plane_copy(self, k, u):
        ref, first = self.held(k + 1, u)
        src = ref.at[:, self.band(self.p.theirs[k] - first, 2**k), :]
        return remote(src, self.r[k].at[u], self.ksem.at[0, k, u], self.ksem.at[1, k, u], self.p.partner[k])

    def shard_copy(self, u, d):
        to = self.p.across(d)
        src = self.held(0, u)[0].at[to[1]]
        return remote(src, self.rz.at[u, d - 1], self.zsem.at[0, u, d - 1], self.zsem.at[1, u, d - 1], to)

    def piece_copy(self, u):
        t, cols = self.where(u)
        return pltpu.make_async_copy(self.tp.at[u], self.total.at[t, self.band(self.p.piece, 1), cols], self.tsem.at[u])

    def total_copy(self, k, u):
        p = self.p
        t, cols = self.where(u)
        first, count, peer = (
            (p.base + p.mine[k], 2**k, p.partner[k]) if k < p.steps else (p.base, p.half, p.twin)
        )
        ref = self.total.at[t, self.band(first, count), cols]
        return remote(ref if k else self.tp.at[u], ref, self.gsem.at[0, k, u], self.gsem.at[1, k, u], peer)

    def add(self, stage, u):
        p = self.p
        if stage == 1:
            self.core_copy(u).wait_recv()
            ring = self.acc.shape[0]

            @pl.when(u >= ring)
            def _():
                self.plane_copy(p.steps - 1, u - ring).wait_send()

            for c in self.loads(u):
                c.start()
        elif stage == 2:
            for c in self.loads(u):
                c.wait()
            a = u % self.acc.shape[0]
            self.acc[a] = self.acc[a] + self.lo[u % self.lo.shape[0]]
        elif 2 < stage < 3 + p.steps:
            k = p.steps - (stage - 2)
            self.plane_copy(k, u).wait_recv()
            ref, first = self.held(k + 1, u)
            self.r[k][u] = self.r[k][u] + ref[:, self.band(p.mine[k] - first, 2**k), :]
        elif stage == 3 + p.steps:
            for d in range(1, self.n + 1):
                self.shard_copy(u, d).wait_recv()
            acc = self.held(0, u)[0][p.s].astype(f32)
            for d in range(1, self.n + 1):
                acc += self.rz[u, d - 1].astype(f32)
            self.tp[u] = acc.astype(bf16)
        elif stage > 3 + p.steps:
            k = stage - 4 - p.steps
            self.total_copy(k, u).wait_recv()
            if k == 0:
                self.piece_copy(u).wait()

    def send(self, stage, u):
        p = self.p
        if stage == 0:
            self.core_copy(u).start()
        elif 2 <= stage < 2 + p.steps:
            self.plane_copy(p.steps - 1 - (stage - 2), u).start()
        elif stage == 2 + p.steps:
            for d in range(1, self.n + 1):
                self.shard_copy(u, d).start()
        elif 3 + p.steps <= stage < self.stages - 1:
            if stage == 3 + p.steps:
                self.piece_copy(u).start()
            self.total_copy(stage - 3 - p.steps, u).start()

    def tick(self, u):
        for do in (self.add, self.send):
            for stage in (range(self.stages) if do == self.add else reversed(range(self.stages))):
                v = u - self.lags[stage]

                @pl.when((v >= 0) & (v < self.units))
                def _(stage=stage, v=v):
                    do(stage, v)

        v = u - self.lags[-1] - 1

        @pl.when((v >= 0) & (v < self.units))
        def _():
            self.sent(v)

    def run(self, first, last):
        @pl.loop(first, last)
        def _(u):
            self.tick(u)

    def sent(self, u):
        self.core_copy(u).wait_send()
        for k in range(self.p.steps - 1):
            self.plane_copy(k, u).wait_send()

        @pl.when(u >= self.units - self.acc.shape[0])
        def _():
            self.plane_copy(self.p.steps - 1, u).wait_send()

        for d in range(1, self.n + 1):
            self.shard_copy(u, d).wait_send()
        for k in range(self.p.steps + 1):
            self.total_copy(k, u).wait_send()

    def finish(self):
        @pl.loop(self.units - 1, self.units)
        def _(u):
            self.sent(u)


def step_kernel(
    replicas, shards, hidden, grad_scale,
    qkv_w, out_w, up_w, down_w, cot, vec, tok, seg_row, freq,
    grads, rc, total, bout, ig, vshare,
    wg, acc, lo, *rest,
):
    steps = int(math.log2(replicas)) - 1
    r, rest = rest[:steps], rest[steps:]
    rz, tp, x_in, x_in_t, gout, out_acc, gmlp, gattn, gtile, grows, cosines, sines, mean, inverse, *rest = rest
    qb, kb, vb, gb, ctx, dq, dk, dv, vg, vgrad, vz, vx, *rest = rest
    gsend, grecv, csem, ksem, zsem, tsem, lsem, psem, own_sem, ssem, vsem, vzsem, vxsem, isem = rest
    p = Place(replicas, shards)
    g = Gather(p, wg, gsend, grecv)
    red = Reduce(p, grads, rc, total, acc, lo, r, rz, tp, (csem, ksem, zsem, tsem, lsem, psem))
    chunks, _, rows, model = wg.shape
    tokens = tok.shape[0]
    ff_chunks = hidden // model
    tiles = model // TILE
    per_tile = TILE // rows
    head = model // H
    scale = head ** (-0.5)
    per_head = head // rows
    chunk0 = 2 * ff_chunks
    width = vec.shape[1]
    wide = hidden // shards
    o_out, o_up, o_down = 7 * model, 8 * model, 8 * model + hidden
    band = 64

    def start(copies):
        for c in copies:
            c.start()

    def wait(copies):
        for c in copies:
            c.wait()

    def bands(body):
        @pl.loop(0, tokens // band)
        def _(i):
            body(pl.ds(pl.multiple_of(i * band, band), band))

    def lanes(body):
        for i in range(tokens // LANES):
            body(slice(i * LANES, (i + 1) * LANES))

    def loads(t):
        slot, j = t % RAW, t // 2
        dst, sem = gattn.at[slot * rows : (slot + 1) * rows, :], own_sem.at[slot]
        if t >= chunk0:
            i = t - chunk0
            src = qkv_w.at[:, i * model : (i + 1) * model] if i < 3 else out_w
            return [pltpu.make_async_copy(src, dst, sem.at[0])]
        if t % 2:
            return [pltpu.make_async_copy(down_w.at[j * rows : (j + 1) * rows, :], dst, sem.at[0])]
        return [
            pltpu.make_async_copy(
                up_w.at[:, i * wide + j * rows : i * wide + (j + 1) * rows],
                dst.at[:, i * rows : (i + 1) * rows],
                sem.at[i],
            )
            for i in range(shards)
        ]

    def part(shard):
        return pl.ds(pl.multiple_of(shard * width, LANES), width)

    def gather_vec(d):
        ref = vg.at[:, part(p.s)]
        return remote(ref, ref, vsem.at[0, d - 1], vsem.at[1, d - 1], p.across(d))

    cot_copy = pltpu.make_async_copy(cot, gout, isem.at[0])
    for t in range(RAW):
        start(loads(t))
    cot_copy.start()
    vg[:, part(p.s)] = vec[...].astype(bf16).astype(f32)
    p.greet()
    start([gather_vec(d) for d in range(1, shards)])
    for t in range(chunks):
        wait(loads(t))

        @pl.loop(0, rows // CAST)
        def _(i, t=t):
            at = pl.multiple_of(i * CAST, CAST)
            wg[t, p.s, pl.ds(at, CAST), :] = gattn[pl.ds((t % RAW) * rows + at, CAST), :].astype(bf16)

        if t + RAW < chunks:
            start(loads(t + RAW))
        if 1 <= t <= AHEAD:
            g.launch(t - 1)
        if t == (AHEAD + chunks) // 2:
            g.tick(0)
    g.tick(1)

    def statistics(at):
        x = tok[at, :].astype(f32)
        m = jnp.mean(x, axis=1, keepdims=True)
        centred = x - m
        mean[at, :] = m
        inverse[at, :] = lax.rsqrt(jnp.mean(centred * centred, axis=1, keepdims=True) + norm_eps)

    def normed(at):
        return (tok[at, :].astype(f32) - mean[at, :]) * inverse[at, :]

    bands(statistics)
    g.tick(2)
    cot_copy.wait()

    def tables(at):
        seg = column(seg_row[:, at])
        gout[at, :] = (gout[at, :].astype(f32) * (seg >= 0.0).astype(f32)).astype(bf16)
        cosines[at, :], sines[at, :] = rotary_rows(seg, seg_row[...], at.start, freq[...])

    for i in range(tokens // LANES):
        tables(slice(i * LANES, (i + 1) * LANES))
        if i % 2:
            g.tick(3 + i // 2)
    for d in range(1, shards):
        gather_vec(d).wait_recv()
    ticked = 3 + tokens // LANES // 2

    def enter_mlp(at):
        x_in[at, :] = (normed(at) * vg[:, 2 * model : 3 * model] + vg[:, 3 * model : 4 * model]).astype(bf16)
        bias = vg[:, o_down : o_down + model] + vg[:, o_out : o_out + model]
        out_acc[at, :] = tok[at, :].astype(f32) + bias
        gmlp[at, :] = jnp.zeros((band, model), f32)

    def turn(at):
        x_in_t[:, at] = x_in[at, :].T

    bands(enter_mlp)
    g.tick(ticked)
    lanes(turn)
    vgrad[...] = jnp.zeros_like(vgrad)

    first = g.ready(1)
    per_block = 2 * g.n

    @pl.loop(ticked + 1, first)
    def _(u):
        g.tick(u)

    def tile_stores(i):
        slot, j, n = i % 2, i // tiles, i % tiles
        cols = pl.ds(pl.multiple_of(n * TILE, TILE), TILE)
        return (
            pltpu.make_async_copy(gtile.at[slot, 0], grads.at[2 * j, :, :, cols], ssem.at[slot, 0]),
            pltpu.make_async_copy(
                grows.at[slot], grads.at[2 * j + 1, pl.ds(n * per_tile, per_tile)], ssem.at[slot, 3]
            ),
        )

    def head_stores(h):
        slot = h % 2
        cols = pl.ds(pl.multiple_of(h * head, head), head)
        out = [
            pltpu.make_async_copy(gtile.at[slot, w], grads.at[chunk0 + w, :, :, cols], ssem.at[slot, w])
            for w in range(3)
        ]
        last = grads.at[chunk0 + 3, pl.ds(h * per_head, per_head)]
        return (*out, pltpu.make_async_copy(grows.at[slot], last, ssem.at[slot, 3]))

    def reduced(i):
        return jnp.maximum(i - EARLY, 0) * TICKS_8 // 8

    @pl.loop(0, ff_chunks * tiles)
    def _(i):
        slot, j, n = i % 2, i // tiles, i % tiles
        lo_tick, hi_tick = first + (i * per_block) // tiles, first + ((i + 1) * per_block) // tiles
        most = -(-per_block // tiles)
        cols = pl.ds(pl.multiple_of(n * TILE, TILE), TILE)

        def maybe(a):
            @pl.when((lo_tick + a < hi_tick) & (lo_tick + a < g.ticks))
            def _():
                g.tick(lo_tick + a)

        @pl.when(i >= 2)
        def _():
            wait(tile_stores(i - 2))

        maybe(0)

        red.run(reduced(i), reduced(i + 1))

        def between():
            for a in range(1, most):
                maybe(a)

        def keep(which, x):
            if which:
                grows[slot] = x.reshape(per_tile, rows, model)
            else:
                gtile[slot, 0] = x.reshape(shards, rows, TILE)

        feed_forward(
            wg[2 * j, :, :, cols].reshape(model, TILE),
            wg[2 * j + 1, pl.ds(n * per_tile, per_tile)].reshape(TILE, model),
            flat_columns(n, j, rows, wide),
            rows, o_up, grad_scale, x_in, x_in_t, gout, vg, vgrad, out_acc, gmlp, between, keep,
        )
        start(tile_stores(i))

    items = ff_chunks * tiles
    done = max(items - EARLY, 0) * TICKS_8 // 8

    def enter_attention(at):
        x_in[at, :] = (normed(at) * vg[:, :model] + vg[:, model : 2 * model]).astype(bf16)
        gattn[at, :] = jnp.zeros((band, model), f32)

    bands(enter_attention)
    lanes(turn)

    @pl.loop(first + ff_chunks * per_block, g.ticks)
    def _(u):
        g.tick(u)

    @pl.loop(0, H)
    def _(h):
        slot = h % 2

        @pl.when(h < 2)
        def _():
            wait(tile_stores(items - 2 + h))

        @pl.when(h >= 2)
        def _():
            wait(head_stores(h - 2))

        red.run(done + 2 * HEAD_TICKS * h, done + 2 * HEAD_TICKS * h + HEAD_TICKS)
        cols = pl.ds(pl.multiple_of(h * head, head), head)
        mine = pl.ds(h * per_head, per_head)

        def weight(i):
            return wg[chunk0 + i, :, :, cols].reshape(model, head)

        def at_head(base):
            return pl.ds(pl.multiple_of(base + h * head, head), head)

        def project(i):
            return dot(x_in[...], weight(i)) + vg[:, at_head((4 + i) * model)]

        wo = wg[chunk0 + 3, mine].reshape(head, model)
        qb[...] = turned(project(0), cosines[...], sines[...], 1.0).astype(bf16)
        kb[...] = turned(project(1), cosines[...], sines[...], 1.0).astype(bf16)
        vb[...] = project(2).astype(bf16)
        gb[...] = dot(gout[...], wo, ((1,), (1,))).astype(bf16)
        one_head(LANES, qb, kb, vb, gb, ctx, dq, dk, dv, seg_row, scale)
        red.run(done + 2 * HEAD_TICKS * h + HEAD_TICKS, done + 2 * HEAD_TICKS * (h + 1))
        back = (
            turned(dq[...], cosines[...], sines[...], -1.0),
            turned(dk[...], cosines[...], sines[...], -1.0),
            dv[...],
        )
        sums = gattn[...]
        for i, d in enumerate(back):
            vgrad[:, at_head((4 + i) * model)] = jnp.sum(d, axis=0, keepdims=True) * grad_scale
            half = d.astype(bf16)
            sums += dot(half, weight(i), ((1,), (1,)))
            gtile[slot, i] = (dot(x_in_t[...], half) * grad_scale).astype(bf16).reshape(shards, rows, head)
        gattn[...] = sums
        out_acc[...] += dot(ctx[...], wo)
        grows[slot] = (
            (dot(ctx[...], gout[...], ((0,), (0,))) * grad_scale).astype(bf16).reshape(per_head, rows, model)
        )
        start(head_stores(h))

    done += 2 * HEAD_TICKS * H
    gain_one, gain_two = vg[:, :model], vg[:, 2 * model : 3 * model]

    def last(i, carry):
        at = pl.ds(pl.multiple_of(i * band, band), band)
        x, ga, gm, go = normed(at), gattn[at, :], gmlp[at, :], gout[at, :].astype(f32)
        gn = ga * gain_one + gm * gain_two
        m1 = jnp.mean(gn, axis=1, keepdims=True)
        m2 = jnp.mean(gn * x, axis=1, keepdims=True)
        gout[at, :] = (go + inverse[at, :] * (gn - m1 - x * m2)).astype(bf16)
        terms = (ga * x, ga, gm * x, gm, go)
        return tuple(a + jnp.sum(b, axis=0, keepdims=True) for a, b in zip(carry, terms))

    zero = jnp.zeros((1, model), f32)
    sums = lax.fori_loop(0, tokens // band, last, (zero,) * 5)
    for x, place in zip((*sums, sums[4]), (0, model, 2 * model, 3 * model, o_out, o_down)):
        vgrad[:, place : place + model] = x * grad_scale

    def leave(at):
        live = (column(seg_row[:, at]) >= 0.0).astype(f32)
        x_in[at, :] = (live * out_acc[at, :]).astype(bf16)

    lanes(leave)
    vgrad[...] = vgrad[...].astype(bf16).astype(f32)
    results = (pltpu.make_async_copy(x_in, bout, isem.at[0]), pltpu.make_async_copy(gout, ig, isem.at[1]))
    start(results)
    for h in range(H - 2, H):
        wait(head_stores(h))

    def vcopy(d):
        to = p.across(d)
        return remote(vgrad.at[:, part(to[1])], vz.at[d - 1], vzsem.at[0, d - 1], vzsem.at[1, d - 1], to)

    peers = [*p.partner, p.twin]

    def vexchange(k):
        return remote(vx.at[2 * k], vx.at[2 * k + 1], vxsem.at[0, k], vxsem.at[1, k], peers[k])

    def vstart(i):
        start([vcopy(d) for d in range(1, shards)] if i == 0 else [vexchange(i - 1)])

    def vfinish(i):
        if i == 0:
            acc = vgrad[:, part(p.s)]
            for d in range(1, shards):
                vcopy(d).wait_recv()
                acc += vz[d - 1]
        else:
            vexchange(i - 1).wait_recv()
            acc = vx[2 * i - 2] + vx[2 * i - 1]
        if i < len(peers):
            vx[2 * i] = acc
        else:
            vshare[...] = acc

    for i in range(len(peers) + 1):
        vstart(i)
        red.run(done + i, done + i + 1)
        vfinish(i)
    done += len(peers) + 1
    red.run(done, done + 4)
    g.finish()
    red.run(done + 4, red.ticks)
    for d in range(1, shards):
        gather_vec(d).wait_send()
        vcopy(d).wait_send()
    for i in range(len(peers)):
        vexchange(i).wait_send()
    red.finish()
    wait(results)


def step_call(mesh, qkv, out, up, down, vec, tok, cot, seg_row, grad_scale):
    replicas, shards = mesh.shape["replica"], mesh.shape["shard"]
    rows, hidden = up.shape
    tokens, model = tok.shape
    chunks = 2 * (hidden // model) + 4
    steps = int(math.log2(replicas)) - 1
    stages = steps + 2
    width = vec.shape[1]
    gather_units = chunks * (shards - 1)
    units, cols, piece = chunks * PARTS, model // PARTS, rows // replicas
    part = 2**steps * piece
    head = model // H
    lags = reduce_lags(steps)
    freq = rope_base ** (-2.0 * (jnp.arange(LANES) % (ROT // 2)).astype(f32) / ROT)[None]
    sds, vm = jax.ShapeDtypeStruct, pltpu.VMEM
    return pl.pallas_call(
        functools.partial(step_kernel, replicas, shards, hidden, grad_scale),
        out_shape=[
            sds((chunks, shards, rows, model), bf16),
            sds((units, shards, part, cols), bf16),
            sds((chunks, rows, model), bf16),
            sds((tokens, model), bf16),
            sds((tokens, model), bf16),
            sds((1, width), f32),
        ],
        in_specs=[ANY] * 5 + [VMEM] * 4,
        out_specs=[ANY] * 5 + [VMEM],
        scratch_shapes=[
            vm((chunks, shards, rows, model), bf16),
            vm((lags[3] - lags[1] + 1, shards, part, cols), bf16),
            vm((lags[2] - lags[1] + 1, shards, part, cols), bf16),
            *(vm((units, shards, 2**k * piece, cols), bf16) for k in range(steps)),
            vm((units, shards - 1, piece, cols), bf16),
            vm((units, piece, cols), bf16),
            vm((tokens, model), bf16),
            vm((model, tokens), bf16),
            vm((tokens, model), bf16),
            *[vm((tokens, model), f32)] * 3,
            vm((2, 3, shards, rows, head), bf16),
            vm((2, head // rows, rows, model), bf16),
            *[vm((tokens, LANES), f32)] * 2,
            *[vm((tokens, 1), f32)] * 2,
            *[vm((tokens, head), bf16)] * 5,
            *[vm((tokens, head), f32)] * 3,
            *[vm((1, width * shards), f32)] * 2,
            vm((shards - 1, 1, width), f32),
            vm((2 * steps + 2, 1, width), f32),
            DMA((stages, gather_units)),
            DMA((stages, gather_units)),
            DMA((2, units)),
            DMA((2, steps, units)),
            DMA((2, units, shards - 1)),
            DMA((2, steps + 1, units)),
            DMA((2, lags[3] - lags[1] + 1)),
            DMA((units,)),
            DMA((RAW, shards)),
            DMA((2, 4)),
            DMA((2, shards - 1)),
            DMA((2, shards - 1)),
            DMA((2, steps + 1)),
            DMA((2,)),
        ],
        compiler_params=pltpu.CompilerParams(
            collective_id=0, has_side_effects=True, vmem_limit_bytes=67043328
        ),
        name="step",
    )(qkv, out, up, down, cot, vec, tok, seg_row, freq)


def adam(master, first, second, gradient, decay):
    first = beta_first * first + (1.0 - beta_first) * gradient
    second = beta_second * second + (1.0 - beta_second) * gradient * gradient
    a = first / (1.0 - beta_first**STEP)
    b = second / (1.0 - beta_second**STEP)
    return master - learn_rate * (a / (jnp.sqrt(b) + adam_eps) + decay * master), first, second


class Weight:
    def __init__(self, band, count, blocks, chunks_of, refs, bufs, sems):
        self.band, self.count, self.blocks, self.chunks_of = band, count, blocks, chunks_of
        self.total, self.w, self.m, self.grad, self.new_w, self.new_m = refs
        self.gbuf, self.wbuf, self.mbuf, self.outbuf = bufs
        self.isem, self.osem = sems

    def loads(self, i):
        slot, at = i % 2, slice(i * self.band, (i + 1) * self.band)
        pairs = [(self.w.at[at, :], self.wbuf.at[slot]), (self.m.at[:, at, :], self.mbuf.at[slot])]
        for n, (chunk, row) in enumerate(self.chunks_of(i)):
            pairs.append((self.total.at[chunk, row : row + self.band, :], self.gbuf.at[slot, n]))
        return [pltpu.make_async_copy(a, b, self.isem.at[slot, n]) for n, (a, b) in enumerate(pairs)]

    def stores(self, i):
        slot, at = i % 2, slice(i * self.band, (i + 1) * self.band)
        pairs = [
            (self.wbuf.at[slot], self.new_w.at[at, :]),
            (self.mbuf.at[slot], self.new_m.at[:, at, :]),
            (self.outbuf.at[slot], self.grad.at[at, :]),
        ]
        return [pltpu.make_async_copy(a, b, self.osem.at[slot, n]) for n, (a, b) in enumerate(pairs)]

    def compute(self, i):
        slot = i % 2
        for col, width, n, gcol in self.blocks:
            high = min(self.band, max(16, 16384 // width))

            @pl.loop(0, self.band // high)
            def _(b, col=col, width=width, n=n, gcol=gcol, high=high):
                at, cols = pl.ds(pl.multiple_of(b * high, high), high), slice(col, col + width)
                g = self.gbuf[slot, n, at, gcol : gcol + width].astype(f32)
                self.outbuf[slot, at, cols] = g
                w, first, second = adam(
                    self.wbuf[slot, at, cols], self.mbuf[slot, 0, at, cols], self.mbuf[slot, 1, at, cols], g, weight_decay
                )
                self.wbuf[slot, at, cols] = w
                self.mbuf[slot, 0, at, cols] = first
                self.mbuf[slot, 1, at, cols] = second


def adam_plans(rows, model, hidden, shards):
    ff = hidden // model
    wide = hidden // shards
    band = min(rows, 64)
    return (
        (band, rows // band, [(i * model, model, i, 0) for i in range(3)],
         lambda b: [(2 * ff + i, b * band) for i in range(3)], 3, 3 * model),
        (rows, 1, [(0, model, 0, 0)], lambda b: [(2 * ff + 3, 0)], 1, model),
        (band, rows // band,
         [(i * wide + j * rows, rows, j, i * rows) for i in range(shards) for j in range(ff)],
         lambda b: [(2 * j, b * band) for j in range(ff)], ff, hidden),
        (rows, ff, [(0, model, 0, 0)], lambda b: [(2 * b + 1, 0)], 1, model),
    )


def adam_kernel(plans, total, *refs):
    ws, ms, passed, refs = refs[:4], refs[4:8], refs[8:10], refs[10:]
    grads, new_ws, new_ms, results, rest = refs[:4], refs[4:8], refs[8:12], refs[12:14], refs[14:]
    carry, csem = rest[-2:]
    inward = [pltpu.make_async_copy(a, carry.at[i], csem.at[0, i]) for i, a in enumerate(passed)]
    outward = [pltpu.make_async_copy(carry.at[i], a, csem.at[1, i]) for i, a in enumerate(results)]
    weights = []
    for n, (band, count, blocks, chunks_of, _, _) in enumerate(plans):
        bufs, sems = rest[6 * n : 6 * n + 4], rest[6 * n + 4 : 6 * n + 6]
        weights.append(
            Weight(band, count, blocks, chunks_of, (total, ws[n], ms[n], grads[n], new_ws[n], new_ms[n]), bufs, sems)
        )
    most = max(w.count for w in weights)
    order = [(w, i) for i in range(most) for w in weights if i < w.count]
    for w, i in order:
        if i < 2:
            for c in w.loads(i):
                c.start()
    for c in inward:
        c.start()
    for n, (w, i) in enumerate(order):
        if n == 4:
            for a, b in zip(inward, outward):
                a.wait()
                b.start()
        if i >= 1 and i + 1 < w.count:
            for c in w.stores(i - 1):
                c.wait()
            for c in w.loads(i + 1):
                c.start()
        for c in w.loads(i):
            c.wait()
        w.compute(i)
        for c in w.stores(i):
            c.start()
    for w, i in order:
        if i + 2 >= w.count:
            for c in w.stores(i):
                c.wait()
    for c in outward:
        c.wait()


def adam_call(total, ws, ms, passed, hidden, shards):
    _, rows, model = total.shape
    plans = adam_plans(rows, model, hidden, shards)
    sds = jax.ShapeDtypeStruct
    scratch = []
    for band, _, _, _, parts, cols in plans:
        scratch += [
            pltpu.VMEM((2, parts, band, model), bf16),
            pltpu.VMEM((2, band, cols), f32),
            pltpu.VMEM((2, 2, band, cols), f32),
            pltpu.VMEM((2, band, cols), f32),
            DMA((2, 2 + parts)),
            DMA((2, 3)),
        ]
    scratch += [pltpu.VMEM((2, *passed[0].shape), passed[0].dtype), DMA((2, 2))]
    like = [sds(w.shape, f32) for w in ws]
    out = pl.pallas_call(
        functools.partial(adam_kernel, plans),
        out_shape=like + like + [sds(m.shape, f32) for m in ms] + [sds(a.shape, a.dtype) for a in passed],
        in_specs=[ANY] * 11,
        out_specs=[ANY] * 14,
        scratch_shapes=scratch,
        compiler_params=pltpu.CompilerParams(vmem_limit_bytes=60 << 20),
        name="adam",
    )(total, *ws, *ms, *passed)
    return out[:4], out[4:8], out[8:12], out[12:]


def local(mesh, tokens, cotangent, seg_ids, qkv, out, up, down, vectors, *moments):
    shards = mesh.shape["shard"]
    hidden = up.shape[1]
    grad_scale = (tokens.shape[0] * mesh.shape["replica"] * shards) ** (-0.5)
    _, _, total, block_output, input_grad, vshare = step_call(
        mesh, qkv, out, up, down, vectors[None], tokens, cotangent, seg_ids[None], grad_scale
    )
    grads, updated, renewed, (block_output, input_grad) = adam_call(
        total, (qkv, out, up, down), moments[:4], (block_output, input_grad), hidden, shards
    )
    vsum = vshare[0]
    new_v, *vm = adam(vectors, moments[4][0], moments[4][1], vsum, 0.0)
    return (block_output, input_grad, *grads, vsum, *updated, new_v, *renewed, jnp.stack(vm))


def solution(mesh):
    rows = P(("replica", "shard"), None)
    first, second = P("shard", None), P(None, "shard", None)
    weights, moments = (first,) * 4 + (P("shard"),), (second,) * 4 + (P(None, "shard"),)
    return jax.shard_map(
        functools.partial(local, mesh),
        mesh=mesh,
        in_specs=(rows, rows, P(("replica", "shard")), *weights, *moments),
        out_specs=(rows, rows, *weights, *weights, *moments),
        check_vma=False,
    )
```

```python
import functools
import math

import jax
import jax.numpy as jnp
from jax import lax
from jax.experimental import pallas as pl
from jax.experimental.pallas import tpu as pltpu
from jax.sharding import PartitionSpec as P

H = 4
ROT = 64
STEP = 3
norm_eps = 1e-05
rope_base = 10000.0
learn_rate = 0.01
beta_first = 0.9
beta_second = 0.95
adam_eps = 1e-08
weight_decay = 0.1
root_half = 0.7071067811865476
inv_root_tau = 0.3989422804014327

MESH = pl.DeviceIdType.MESH
f32, bf16 = jnp.float32, jnp.bfloat16
ANY = pl.BlockSpec(memory_space=pl.ANY)
VMEM = pl.BlockSpec(memory_space=pltpu.VMEM)
DMA = pltpu.SemaphoreType.DMA
TILE = 256
LANES = 128
PARTS = 2
SLOW, QUICK = 2, 1
RAW = 2
CAST = 64
EARLY = 5
TICKS_8 = 6
HEAD_TICKS = 1
LAG = 2
AHEAD = 3


class Place:
    def __init__(self, replicas, shards):
        self.replicas, self.shards = replicas, shards
        self.steps = int(math.log2(replicas)) - 1
        self.half = 2**self.steps
        self.r = lax.axis_index("replica")
        self.s = lax.axis_index("shard")
        self.core = self.r % 2
        self.m = self.mixed(self.r // 2)
        self.base = self.core * self.half
        self.twin_base = (1 - self.core) * self.half
        self.piece = self.base + self.m
        self.twin = (self.r + 1 - 2 * self.core, self.s)
        self.partner, self.mine, self.theirs = [], [], []
        for k in range(self.steps):
            flip = 2**k
            other = self.m + flip * (1 - 2 * ((self.m // flip) % 2))
            self.partner.append((2 * self.mixed(other) + self.core, self.s))
            self.mine.append((self.m // flip) * flip)
            self.theirs.append((other // flip) * flip)

    def mixed(self, plane):
        n = self.steps
        turned = sum(((plane // 2**i) % 2) * 2 ** (n - 1 - i) for i in range(n))
        return (1 - self.core) * plane + self.core * turned

    def across(self, d):
        return (self.r, (self.s + d) % self.shards)

    def source(self, d):
        return (self.s + self.shards - d) % self.shards

    def greet(self):
        barrier = pltpu.get_barrier_semaphore()
        peers = [self.across(d) for d in range(1, self.shards)] + self.partner + [self.twin]
        for peer in peers:
            pl.semaphore_signal(barrier, inc=1, device_id=peer, device_id_type=MESH)
        pl.semaphore_wait(barrier, len(peers))


def remote(src, dst, send, recv, peer):
    return pltpu.make_async_remote_copy(
        src_ref=src, dst_ref=dst, send_sem=send, recv_sem=recv, device_id=peer, device_id_type=MESH
    )


class Gather:
    def __init__(self, place, wg, send, recv):
        self.p, self.wg, self.send, self.recv = place, wg, send, recv
        self.chunks = wg.shape[0]
        self.rows = wg.shape[2] // place.replicas
        self.stages = place.steps + 2
        self.n = place.shards - 1
        self.units = self.chunks * self.n
        self.ticks = self.units + (self.stages - 1) * LAG

    def span(self, t, shard, first, count):
        start = pl.multiple_of(first * self.rows, self.rows)
        return self.wg.at[t, shard, pl.ds(start, count * self.rows), :]

    def copy(self, stage, t, d):
        p = self.p
        if stage == 0:
            ref, peer = self.span(t, p.s, p.piece, 1), p.across(d)
        elif stage <= p.steps:
            k = stage - 1
            ref, peer = self.span(t, p.source(d), p.base + p.mine[k], 2**k), p.partner[k]
        else:
            ref, peer = self.span(t, p.source(d), p.base, p.half), p.twin
        u = t * self.n + d - 1
        return remote(ref, ref, self.send.at[stage, u], self.recv.at[stage, u], peer)

    def launch(self, t):
        for d in range(1, self.n + 1):
            self.copy(0, t, d).start()

    def ready(self, t):
        return (t + 1) * self.n + (self.stages - 1) * LAG

    def tick(self, u):
        for stage in range(self.stages):
            v = u - stage * LAG

            @pl.when((v >= 0) & (v < self.units))
            def _(stage=stage, v=v):
                t, d = v // self.n, v % self.n + 1
                self.copy(stage, t, d).wait_recv()
                if stage + 1 < self.stages:
                    self.copy(stage + 1, t, d).start()

        @pl.when((u % self.n == self.n - 1) & (u // self.n + AHEAD < self.chunks))
        def _():
            self.launch(u // self.n + AHEAD)

    def finish(self):
        @pl.loop(0, self.chunks)
        def _(t):
            for d in range(1, self.n + 1):
                for stage in range(self.stages):
                    self.copy(stage, t, d).wait_send()


def dot(a, b, dims=((1,), (0,))):
    return lax.dot_general(a, b, (dims, ((), ())), preferred_element_type=f32)


def column(row):
    return jnp.broadcast_to(row.astype(f32), (8, row.shape[1])).T[:, :1]


def rotary_rows(seg, seg_row, start):
    shape = (seg.shape[0], seg_row.shape[1])
    row = lax.broadcasted_iota(jnp.int32, shape, 0) + start
    col = lax.broadcasted_iota(jnp.int32, shape, 1)
    before = (seg == seg_row.astype(f32)) & (col < row)
    position = jnp.sum(before.astype(f32), axis=1, keepdims=True)
    lane = lax.broadcasted_iota(jnp.int32, (1, LANES), 1)
    order = (lane % (ROT // 2)).astype(f32)
    angles = position * jnp.exp(order * (-2.0 / ROT * math.log(rope_base)))
    lane = lax.broadcasted_iota(jnp.int32, angles.shape, 1)
    cosine, sine = jnp.cos(angles), jnp.sin(angles)
    sine = jnp.where(lane < ROT // 2, -sine, sine)
    return jnp.where(lane < ROT, cosine, 1.0), jnp.where(lane < ROT, sine, 0.0)


def flat_columns(tile, j, rows, wide):
    per_tile = TILE // rows
    return [pl.multiple_of((tile * per_tile + i) * wide + j * rows, rows) for i in range(per_tile)]


def feed_forward(up, down, flats, rows, o_up, grad_scale, mlp_in, mlp_in_t, gout, vg, vgrad, mlp, gmlp, between, keep):
    bias = jnp.concatenate([vg[:, pl.ds(o_up + f, rows)] for f in flats], axis=1)
    h = dot(mlp_in[...], up) + bias
    cum = 0.5 * (1.0 + lax.erf(h * root_half))
    density = jnp.exp(-0.5 * h * h) * inv_root_tau
    act = (h * cum).astype(bf16)
    gh = dot(gout[...], down, ((1,), (1,))) * (cum + h * density)
    ghh = gh.astype(bf16)
    total = jnp.sum(gh, axis=0, keepdims=True) * grad_scale
    for i, f in enumerate(flats):
        vgrad[:, pl.ds(o_up + f, rows)] = total[:, i * rows : (i + 1) * rows]
    between()
    mlp[...] += dot(act, down)
    keep(1, (dot(act, gout[...], ((0,), (0,))) * grad_scale).astype(bf16))
    gmlp[...] += dot(ghh, up, ((1,), (1,)))
    keep(0, (dot(mlp_in_t[...], ghh) * grad_scale).astype(bf16))


def turned(x, cosines, sines, sign):
    first = x[:, :LANES]
    lane = lax.broadcasted_iota(jnp.int32, first.shape, 1)
    other = jnp.where(lane < ROT // 2, pltpu.roll(first, LANES - ROT // 2, 1), pltpu.roll(first, ROT // 2, 1))
    return jnp.concatenate([first * cosines + sign * (other * sines), x[:, LANES:]], axis=1)


def one_head(band, q, k, v, gctx, ctx, dq, dk, dv, seg_row, scale):
    dk[...] = jnp.zeros_like(dk)
    dv[...] = jnp.zeros_like(dv)
    for i in range(q.shape[0] // band):
        at, end = slice(i * band, (i + 1) * band), (i + 1) * band
        qi, gi, ki, vi = q[at, :], gctx[at, :], k[:end, :], v[:end, :]
        row = lax.broadcasted_iota(jnp.int32, (band, end), 0) + i * band
        col = lax.broadcasted_iota(jnp.int32, (band, end), 1)
        allowed = (column(seg_row[:, at]) == seg_row[:, :end].astype(f32)) & (col <= row)
        masked = jnp.where(allowed, dot(qi, ki, ((1,), (1,))) * scale, -jnp.inf)
        largest = jnp.max(masked, axis=1, keepdims=True)
        log_total = largest + jnp.log(jnp.sum(jnp.exp(masked - largest), axis=1, keepdims=True))
        prob = jnp.exp(masked - log_total)
        half = prob.astype(bf16)
        ctx[at, :] = dot(half, vi).astype(bf16)
        gp = dot(gi, vi, ((1,), (1,)))
        delta = jnp.sum(prob * gp, axis=1, keepdims=True)
        gs = (prob * (gp - delta) * scale).astype(bf16)
        dq[at, :] = dot(gs, ki)
        dk[:end, :] += dot(gs, qi, ((0,), (0,)))
        dv[:end, :] += dot(half, gi, ((0,), (0,)))


def reduce_lags(steps):
    lags = [0]
    for gap in [QUICK] * 2 + [SLOW] * (2 * steps + 2):
        lags.append(lags[-1] + gap)
    return lags


class Reduce:
    def __init__(self, place, grads, rc, total, acc, lo, r, rz, tp, sems):
        self.p, self.grads, self.rc, self.total = place, grads, rc, total
        self.acc, self.lo, self.r, self.rz, self.tp = acc, lo, r, rz, tp
        self.csem, self.ksem, self.zsem, self.gsem, self.lsem, self.tsem = sems
        self.cols = acc.shape[3]
        self.parts = total.shape[2] // self.cols
        self.rows = total.shape[1] // place.replicas
        self.units = total.shape[0] * self.parts
        self.n = place.shards - 1
        self.lags = reduce_lags(place.steps)
        self.stages = len(self.lags)
        self.ticks = self.units + self.lags[-1]

    def where(self, u):
        t, part = u // self.parts, u % self.parts
        return t, pl.ds(pl.multiple_of(part * self.cols, self.cols), self.cols)

    def band(self, first, count):
        return pl.ds(pl.multiple_of(first * self.rows, self.rows), count * self.rows)

    def loads(self, u):
        t, cols = self.where(u)
        a, b = u % self.acc.shape[0], u % self.lo.shape[0]
        own = self.grads.at[t, :, self.band(self.p.base, self.p.half), cols]
        return (
            pltpu.make_async_copy(self.rc.at[u], self.acc.at[a], self.lsem.at[0, a]),
            pltpu.make_async_copy(own, self.lo.at[b], self.lsem.at[1, b]),
        )

    def core_copy(self, u):
        t, cols = self.where(u)
        src = self.grads.at[t, :, self.band(self.p.twin_base, self.p.half), cols]
        return remote(src, self.rc.at[u], self.csem.at[0, u], self.csem.at[1, u], self.p.twin)

    def held(self, k, u):
        p = self.p
        return (self.acc.at[u % self.acc.shape[0]], 0) if k == p.steps else (self.r[k].at[u], p.mine[k])

    def plane_copy(self, k, u):
        ref, first = self.held(k + 1, u)
        src = ref.at[:, self.band(self.p.theirs[k] - first, 2**k), :]
        return remote(src, self.r[k].at[u], self.ksem.at[0, k, u], self.ksem.at[1, k, u], self.p.partner[k])

    def shard_copy(self, u, d):
        to = self.p.across(d)
        src = self.held(0, u)[0].at[to[1]]
        return remote(src, self.rz.at[u, d - 1], self.zsem.at[0, u, d - 1], self.zsem.at[1, u, d - 1], to)

    def piece_copy(self, u):
        t, cols = self.where(u)
        return pltpu.make_async_copy(self.tp.at[u], self.total.at[t, self.band(self.p.piece, 1), cols], self.tsem.at[u])

    def total_copy(self, k, u):
        p = self.p
        t, cols = self.where(u)
        first, count, peer = (
            (p.base + p.mine[k], 2**k, p.partner[k]) if k < p.steps else (p.base, p.half, p.twin)
        )
        ref = self.total.at[t, self.band(first, count), cols]
        return remote(ref if k else self.tp.at[u], ref, self.gsem.at[0, k, u], self.gsem.at[1, k, u], peer)

    def add(self, stage, u):
        p = self.p
        if stage == 1:
            self.core_copy(u).wait_recv()
            ring = self.acc.shape[0]

            @pl.when(u >= ring)
            def _():
                self.plane_copy(p.steps - 1, u - ring).wait_send()

            for c in self.loads(u):
                c.start()
        elif stage == 2:
            for c in self.loads(u):
                c.wait()
            a = u % self.acc.shape[0]
            self.acc[a] = self.acc[a] + self.lo[u % self.lo.shape[0]]
        elif 2 < stage < 3 + p.steps:
            k = p.steps - (stage - 2)
            self.plane_copy(k, u).wait_recv()
            ref, first = self.held(k + 1, u)
            self.r[k][u] = self.r[k][u] + ref[:, self.band(p.mine[k] - first, 2**k), :]
        elif stage == 3 + p.steps:
            for d in range(1, self.n + 1):
                self.shard_copy(u, d).wait_recv()
            acc = self.held(0, u)[0][p.s].astype(f32)
            for d in range(1, self.n + 1):
                acc += self.rz[u, d - 1].astype(f32)
            self.tp[u] = acc.astype(bf16)
        elif stage > 3 + p.steps:
            k = stage - 4 - p.steps
            self.total_copy(k, u).wait_recv()
            if k == 0:
                self.piece_copy(u).wait()

    def send(self, stage, u):
        p = self.p
        if stage == 0:
            self.core_copy(u).start()
        elif 2 <= stage < 2 + p.steps:
            self.plane_copy(p.steps - 1 - (stage - 2), u).start()
        elif stage == 2 + p.steps:
            for d in range(1, self.n + 1):
                self.shard_copy(u, d).start()
        elif 3 + p.steps <= stage < self.stages - 1:
            if stage == 3 + p.steps:
                self.piece_copy(u).start()
            self.total_copy(stage - 3 - p.steps, u).start()

    def tick(self, u):
        for do in (self.add, self.send):
            for stage in (range(self.stages) if do == self.add else reversed(range(self.stages))):
                v = u - self.lags[stage]

                @pl.when((v >= 0) & (v < self.units))
                def _(stage=stage, v=v):
                    do(stage, v)

        v = u - self.lags[-1] - 1

        @pl.when((v >= 0) & (v < self.units))
        def _():
            self.sent(v)

    def run(self, first, last):
        @pl.loop(first, last)
        def _(u):
            self.tick(u)

    def sent(self, u):
        self.core_copy(u).wait_send()
        for k in range(self.p.steps - 1):
            self.plane_copy(k, u).wait_send()

        @pl.when(u >= self.units - self.acc.shape[0])
        def _():
            self.plane_copy(self.p.steps - 1, u).wait_send()

        for d in range(1, self.n + 1):
            self.shard_copy(u, d).wait_send()
        for k in range(self.p.steps + 1):
            self.total_copy(k, u).wait_send()

    def finish(self):
        @pl.loop(self.units - 1, self.units)
        def _(u):
            self.sent(u)


def step_kernel(
    replicas, shards, hidden, grad_scale,
    qkv_w, out_w, up_w, down_w, cot, vec, tok, seg_row,
    grads, rc, total, bout, ig, vshare,
    wg, acc, lo, *rest,
):
    steps = int(math.log2(replicas)) - 1
    r, rest = rest[:steps], rest[steps:]
    rz, tp, x_in, x_in_t, gout, out_acc, gmlp, gattn, gtile, grows, cosines, sines, mean, inverse, *rest = rest
    qb, kb, vb, gb, ctx, dq, dk, dv, vg, vgrad, vz, vx, *rest = rest
    gsend, grecv, csem, ksem, zsem, tsem, lsem, psem, own_sem, ssem, vsem, vzsem, vxsem, isem = rest
    p = Place(replicas, shards)
    g = Gather(p, wg, gsend, grecv)
    red = Reduce(p, grads, rc, total, acc, lo, r, rz, tp, (csem, ksem, zsem, tsem, lsem, psem))
    chunks, _, rows, model = wg.shape
    tokens = tok.shape[0]
    ff_chunks = hidden // model
    tiles = model // TILE
    per_tile = TILE // rows
    head = model // H
    scale = head ** (-0.5)
    per_head = head // rows
    chunk0 = 2 * ff_chunks
    width = vec.shape[0]
    wide = hidden // shards
    o_out, o_up, o_down = 7 * model, 8 * model, 8 * model + hidden
    band = 64

    def start(copies):
        for c in copies:
            c.start()

    def wait(copies):
        for c in copies:
            c.wait()

    def bands(body):
        @pl.loop(0, tokens // band)
        def _(i):
            body(pl.ds(pl.multiple_of(i * band, band), band))

    def lanes(body):
        for i in range(tokens // LANES):
            body(slice(i * LANES, (i + 1) * LANES))

    def loads(t):
        slot, j = t % RAW, t // 2
        dst, sem = gattn.at[slot * rows : (slot + 1) * rows, :], own_sem.at[slot]
        if t >= chunk0:
            i = t - chunk0
            src = qkv_w.at[:, i * model : (i + 1) * model] if i < 3 else out_w
            return [pltpu.make_async_copy(src, dst, sem.at[0])]
        if t % 2:
            return [pltpu.make_async_copy(down_w.at[j * rows : (j + 1) * rows, :], dst, sem.at[0])]
        return [
            pltpu.make_async_copy(
                up_w.at[:, i * wide + j * rows : i * wide + (j + 1) * rows],
                dst.at[:, i * rows : (i + 1) * rows],
                sem.at[i],
            )
            for i in range(shards)
        ]

    def part(shard):
        return pl.ds(pl.multiple_of(shard * width, LANES), width)

    def gather_vec(d):
        ref = vg.at[:, part(p.s)]
        return remote(ref, ref, vsem.at[0, d - 1], vsem.at[1, d - 1], p.across(d))

    cot_copy = pltpu.make_async_copy(cot, gout, isem.at[0])
    for t in range(RAW):
        start(loads(t))
    cot_copy.start()
    vg[:, part(p.s)] = vec[...].reshape(1, width).astype(bf16).astype(f32)
    p.greet()
    start([gather_vec(d) for d in range(1, shards)])
    for t in range(chunks):
        wait(loads(t))

        @pl.loop(0, rows // CAST)
        def _(i, t=t):
            at = pl.multiple_of(i * CAST, CAST)
            wg[t, p.s, pl.ds(at, CAST), :] = gattn[pl.ds((t % RAW) * rows + at, CAST), :].astype(bf16)

        if t + RAW < chunks:
            start(loads(t + RAW))
        if 1 <= t <= AHEAD:
            g.launch(t - 1)
        if t == (AHEAD + chunks) // 2:
            g.tick(0)
    g.tick(1)

    def statistics(at):
        x = tok[at, :].astype(f32)
        m = jnp.mean(x, axis=1, keepdims=True)
        centred = x - m
        mean[at, :] = m
        inverse[at, :] = lax.rsqrt(jnp.mean(centred * centred, axis=1, keepdims=True) + norm_eps)

    def normed(at):
        return (tok[at, :].astype(f32) - mean[at, :]) * inverse[at, :]

    bands(statistics)
    g.tick(2)
    cot_copy.wait()

    def tables(at):
        seg = column(seg_row[:, at])
        gout[at, :] = (gout[at, :].astype(f32) * (seg >= 0.0).astype(f32)).astype(bf16)
        cosines[at, :], sines[at, :] = rotary_rows(seg, seg_row[...], at.start)

    for i in range(tokens // LANES):
        tables(slice(i * LANES, (i + 1) * LANES))
        if i % 2:
            g.tick(3 + i // 2)
    for d in range(1, shards):
        gather_vec(d).wait_recv()
    ticked = 3 + tokens // LANES // 2

    def enter_mlp(at):
        x_in[at, :] = (normed(at) * vg[:, 2 * model : 3 * model] + vg[:, 3 * model : 4 * model]).astype(bf16)
        bias = vg[:, o_down : o_down + model] + vg[:, o_out : o_out + model]
        out_acc[at, :] = tok[at, :].astype(f32) + bias
        gmlp[at, :] = jnp.zeros((band, model), f32)

    def turn(at):
        x_in_t[:, at] = x_in[at, :].T

    bands(enter_mlp)
    g.tick(ticked)
    lanes(turn)
    vgrad[...] = jnp.zeros_like(vgrad)

    first = g.ready(1)
    per_block = 2 * g.n

    @pl.loop(ticked + 1, first)
    def _(u):
        g.tick(u)

    def tile_stores(i):
        slot, j, n = i % 2, i // tiles, i % tiles
        cols = pl.ds(pl.multiple_of(n * TILE, TILE), TILE)
        return (
            pltpu.make_async_copy(gtile.at[slot, 0], grads.at[2 * j, :, :, cols], ssem.at[slot, 0]),
            pltpu.make_async_copy(
                grows.at[slot], grads.at[2 * j + 1, pl.ds(n * per_tile, per_tile)], ssem.at[slot, 3]
            ),
        )

    def head_stores(h):
        slot = h % 2
        cols = pl.ds(pl.multiple_of(h * head, head), head)
        out = [
            pltpu.make_async_copy(gtile.at[slot, w], grads.at[chunk0 + w, :, :, cols], ssem.at[slot, w])
            for w in range(3)
        ]
        last = grads.at[chunk0 + 3, pl.ds(h * per_head, per_head)]
        return (*out, pltpu.make_async_copy(grows.at[slot], last, ssem.at[slot, 3]))

    def reduced(i):
        return jnp.maximum(i - EARLY, 0) * TICKS_8 // 8

    @pl.loop(0, ff_chunks * tiles)
    def _(i):
        slot, j, n = i % 2, i // tiles, i % tiles
        lo_tick, hi_tick = first + (i * per_block) // tiles, first + ((i + 1) * per_block) // tiles
        most = -(-per_block // tiles)
        cols = pl.ds(pl.multiple_of(n * TILE, TILE), TILE)

        def maybe(a):
            @pl.when((lo_tick + a < hi_tick) & (lo_tick + a < g.ticks))
            def _():
                g.tick(lo_tick + a)

        @pl.when(i >= 2)
        def _():
            wait(tile_stores(i - 2))

        maybe(0)

        red.run(reduced(i), reduced(i + 1))

        def between():
            for a in range(1, most):
                maybe(a)

        def keep(which, x):
            if which:
                grows[slot] = x.reshape(per_tile, rows, model)
            else:
                gtile[slot, 0] = x.reshape(shards, rows, TILE)

        feed_forward(
            wg[2 * j, :, :, cols].reshape(model, TILE),
            wg[2 * j + 1, pl.ds(n * per_tile, per_tile)].reshape(TILE, model),
            flat_columns(n, j, rows, wide),
            rows, o_up, grad_scale, x_in, x_in_t, gout, vg, vgrad, out_acc, gmlp, between, keep,
        )
        start(tile_stores(i))

    items = ff_chunks * tiles
    done = max(items - EARLY, 0) * TICKS_8 // 8

    def enter_attention(at):
        x_in[at, :] = (normed(at) * vg[:, :model] + vg[:, model : 2 * model]).astype(bf16)
        gattn[at, :] = jnp.zeros((band, model), f32)

    bands(enter_attention)
    lanes(turn)

    @pl.loop(first + ff_chunks * per_block, g.ticks)
    def _(u):
        g.tick(u)

    @pl.loop(0, H)
    def _(h):
        slot = h % 2

        @pl.when(h < 2)
        def _():
            wait(tile_stores(items - 2 + h))

        @pl.when(h >= 2)
        def _():
            wait(head_stores(h - 2))

        red.run(done + 2 * HEAD_TICKS * h, done + 2 * HEAD_TICKS * h + HEAD_TICKS)
        cols = pl.ds(pl.multiple_of(h * head, head), head)
        mine = pl.ds(h * per_head, per_head)

        def weight(i):
            return wg[chunk0 + i, :, :, cols].reshape(model, head)

        def at_head(base):
            return pl.ds(pl.multiple_of(base + h * head, head), head)

        def project(i):
            return dot(x_in[...], weight(i)) + vg[:, at_head((4 + i) * model)]

        wo = wg[chunk0 + 3, mine].reshape(head, model)
        qb[...] = turned(project(0), cosines[...], sines[...], 1.0).astype(bf16)
        kb[...] = turned(project(1), cosines[...], sines[...], 1.0).astype(bf16)
        vb[...] = project(2).astype(bf16)
        gb[...] = dot(gout[...], wo, ((1,), (1,))).astype(bf16)
        one_head(LANES, qb, kb, vb, gb, ctx, dq, dk, dv, seg_row, scale)
        red.run(done + 2 * HEAD_TICKS * h + HEAD_TICKS, done + 2 * HEAD_TICKS * (h + 1))
        back = (
            turned(dq[...], cosines[...], sines[...], -1.0),
            turned(dk[...], cosines[...], sines[...], -1.0),
            dv[...],
        )
        sums = gattn[...]
        for i, d in enumerate(back):
            vgrad[:, at_head((4 + i) * model)] = jnp.sum(d, axis=0, keepdims=True) * grad_scale
            half = d.astype(bf16)
            sums += dot(half, weight(i), ((1,), (1,)))
            gtile[slot, i] = (dot(x_in_t[...], half) * grad_scale).astype(bf16).reshape(shards, rows, head)
        gattn[...] = sums
        out_acc[...] += dot(ctx[...], wo)
        grows[slot] = (
            (dot(ctx[...], gout[...], ((0,), (0,))) * grad_scale).astype(bf16).reshape(per_head, rows, model)
        )
        start(head_stores(h))

    done += 2 * HEAD_TICKS * H
    gain_one, gain_two = vg[:, :model], vg[:, 2 * model : 3 * model]

    def last(i, carry):
        at = pl.ds(pl.multiple_of(i * band, band), band)
        x, ga, gm, go = normed(at), gattn[at, :], gmlp[at, :], gout[at, :].astype(f32)
        gn = ga * gain_one + gm * gain_two
        m1 = jnp.mean(gn, axis=1, keepdims=True)
        m2 = jnp.mean(gn * x, axis=1, keepdims=True)
        gout[at, :] = (go + inverse[at, :] * (gn - m1 - x * m2)).astype(bf16)
        terms = (ga * x, ga, gm * x, gm, go)
        return tuple(a + jnp.sum(b, axis=0, keepdims=True) for a, b in zip(carry, terms))

    zero = jnp.zeros((1, model), f32)
    sums = lax.fori_loop(0, tokens // band, last, (zero,) * 5)
    for x, place in zip((*sums, sums[4]), (0, model, 2 * model, 3 * model, o_out, o_down)):
        vgrad[:, place : place + model] = x * grad_scale

    def leave(at):
        live = (column(seg_row[:, at]) >= 0.0).astype(f32)
        x_in[at, :] = (live * out_acc[at, :]).astype(bf16)

    lanes(leave)
    vgrad[...] = vgrad[...].astype(bf16).astype(f32)
    results = (pltpu.make_async_copy(x_in, bout, isem.at[0]), pltpu.make_async_copy(gout, ig, isem.at[1]))
    start(results)
    for h in range(H - 2, H):
        wait(head_stores(h))

    def vcopy(d):
        to = p.across(d)
        return remote(vgrad.at[:, part(to[1])], vz.at[d - 1], vzsem.at[0, d - 1], vzsem.at[1, d - 1], to)

    peers = [*p.partner, p.twin]

    def vexchange(k):
        return remote(vx.at[2 * k], vx.at[2 * k + 1], vxsem.at[0, k], vxsem.at[1, k], peers[k])

    def vstart(i):
        start([vcopy(d) for d in range(1, shards)] if i == 0 else [vexchange(i - 1)])

    def vfinish(i):
        if i == 0:
            acc = vgrad[:, part(p.s)]
            for d in range(1, shards):
                vcopy(d).wait_recv()
                acc += vz[d - 1]
        else:
            vexchange(i - 1).wait_recv()
            acc = vx[2 * i - 2] + vx[2 * i - 1]
        if i < len(peers):
            vx[2 * i] = acc
        else:
            vshare[...] = acc

    for i in range(len(peers) + 1):
        vstart(i)
        red.run(done + i, done + i + 1)
        vfinish(i)
    done += len(peers) + 1
    red.run(done, done + 4)
    g.finish()
    red.run(done + 4, red.ticks)
    for d in range(1, shards):
        gather_vec(d).wait_send()
        vcopy(d).wait_send()
    for i in range(len(peers)):
        vexchange(i).wait_send()
    red.finish()
    wait(results)


def step_call(mesh, qkv, out, up, down, vec, tok, cot, seg_row, grad_scale):
    replicas, shards = mesh.shape["replica"], mesh.shape["shard"]
    rows, hidden = up.shape
    tokens, model = tok.shape
    chunks = 2 * (hidden // model) + 4
    steps = int(math.log2(replicas)) - 1
    stages = steps + 2
    width = vec.shape[0]
    gather_units = chunks * (shards - 1)
    units, cols, piece = chunks * PARTS, model // PARTS, rows // replicas
    part = 2**steps * piece
    head = model // H
    lags = reduce_lags(steps)
    sds, vm = jax.ShapeDtypeStruct, pltpu.VMEM
    return pl.pallas_call(
        functools.partial(step_kernel, replicas, shards, hidden, grad_scale),
        out_shape=[
            sds((chunks, shards, rows, model), bf16),
            sds((units, shards, part, cols), bf16),
            sds((chunks, rows, model), bf16),
            sds((tokens, model), bf16),
            sds((tokens, model), bf16),
            sds((1, width), f32),
        ],
        in_specs=[ANY] * 5 + [VMEM] * 3,
        out_specs=[ANY] * 5 + [VMEM],
        scratch_shapes=[
            vm((chunks, shards, rows, model), bf16),
            vm((lags[3] - lags[1] + 1, shards, part, cols), bf16),
            vm((lags[2] - lags[1] + 1, shards, part, cols), bf16),
            *(vm((units, shards, 2**k * piece, cols), bf16) for k in range(steps)),
            vm((units, shards - 1, piece, cols), bf16),
            vm((units, piece, cols), bf16),
            vm((tokens, model), bf16),
            vm((model, tokens), bf16),
            vm((tokens, model), bf16),
            *[vm((tokens, model), f32)] * 3,
            vm((2, 3, shards, rows, head), bf16),
            vm((2, head // rows, rows, model), bf16),
            *[vm((tokens, LANES), f32)] * 2,
            *[vm((tokens, 1), f32)] * 2,
            *[vm((tokens, head), bf16)] * 5,
            *[vm((tokens, head), f32)] * 3,
            *[vm((1, width * shards), f32)] * 2,
            vm((shards - 1, 1, width), f32),
            vm((2 * steps + 2, 1, width), f32),
            DMA((stages, gather_units)),
            DMA((stages, gather_units)),
            DMA((2, units)),
            DMA((2, steps, units)),
            DMA((2, units, shards - 1)),
            DMA((2, steps + 1, units)),
            DMA((2, lags[3] - lags[1] + 1)),
            DMA((units,)),
            DMA((RAW, shards)),
            DMA((2, 4)),
            DMA((2, shards - 1)),
            DMA((2, shards - 1)),
            DMA((2, steps + 1)),
            DMA((2,)),
        ],
        compiler_params=pltpu.CompilerParams(
            collective_id=0, has_side_effects=True, vmem_limit_bytes=67043328
        ),
        name="step",
    )(qkv, out, up, down, cot, vec, tok, seg_row)


def adam(master, first, second, gradient, decay):
    first = beta_first * first + (1.0 - beta_first) * gradient
    second = beta_second * second + (1.0 - beta_second) * gradient * gradient
    a = first / (1.0 - beta_first**STEP)
    b = second / (1.0 - beta_second**STEP)
    return master - learn_rate * (a / (jnp.sqrt(b) + adam_eps) + decay * master), first, second


class Weight:
    def __init__(self, band, count, blocks, chunks_of, refs, bufs, sems):
        self.band, self.count, self.blocks, self.chunks_of = band, count, blocks, chunks_of
        self.total, self.w, self.m, self.grad, self.new_w, self.new_m = refs
        self.gbuf, self.wbuf, self.mbuf, self.outbuf = bufs
        self.isem, self.osem = sems

    def loads(self, i):
        slot, at = i % 2, slice(i * self.band, (i + 1) * self.band)
        pairs = [(self.w.at[at, :], self.wbuf.at[slot]), (self.m.at[:, at, :], self.mbuf.at[slot])]
        for n, (chunk, row) in enumerate(self.chunks_of(i)):
            pairs.append((self.total.at[chunk, row : row + self.band, :], self.gbuf.at[slot, n]))
        return [pltpu.make_async_copy(a, b, self.isem.at[slot, n]) for n, (a, b) in enumerate(pairs)]

    def stores(self, i):
        slot, at = i % 2, slice(i * self.band, (i + 1) * self.band)
        pairs = [
            (self.wbuf.at[slot], self.new_w.at[at, :]),
            (self.mbuf.at[slot], self.new_m.at[:, at, :]),
            (self.outbuf.at[slot], self.grad.at[at, :]),
        ]
        return [pltpu.make_async_copy(a, b, self.osem.at[slot, n]) for n, (a, b) in enumerate(pairs)]

    def compute(self, i):
        slot = i % 2
        for col, width, n, gcol in self.blocks:
            high = min(self.band, max(16, 16384 // width))

            @pl.loop(0, self.band // high)
            def _(b, col=col, width=width, n=n, gcol=gcol, high=high):
                at, cols = pl.ds(pl.multiple_of(b * high, high), high), slice(col, col + width)
                g = self.gbuf[slot, n, at, gcol : gcol + width].astype(f32)
                self.outbuf[slot, at, cols] = g
                w, first, second = adam(
                    self.wbuf[slot, at, cols], self.mbuf[slot, 0, at, cols], self.mbuf[slot, 1, at, cols], g, weight_decay
                )
                self.wbuf[slot, at, cols] = w
                self.mbuf[slot, 0, at, cols] = first
                self.mbuf[slot, 1, at, cols] = second


def adam_plans(rows, model, hidden, shards):
    ff = hidden // model
    wide = hidden // shards
    band = min(rows, 64)
    return (
        (band, rows // band, [(i * model, model, i, 0) for i in range(3)],
         lambda b: [(2 * ff + i, b * band) for i in range(3)], 3, 3 * model),
        (rows, 1, [(0, model, 0, 0)], lambda b: [(2 * ff + 3, 0)], 1, model),
        (band, rows // band,
         [(i * wide + j * rows, rows, j, i * rows) for i in range(shards) for j in range(ff)],
         lambda b: [(2 * j, b * band) for j in range(ff)], ff, hidden),
        (rows, ff, [(0, model, 0, 0)], lambda b: [(2 * b + 1, 0)], 1, model),
    )


def adam_kernel(plans, total, *refs):
    ws, ms, passed, refs = refs[:4], refs[4:8], refs[8:10], refs[10:]
    grads, new_ws, new_ms, results, rest = refs[:4], refs[4:8], refs[8:12], refs[12:14], refs[14:]
    carry, csem = rest[-2:]
    inward = [pltpu.make_async_copy(a, carry.at[i], csem.at[0, i]) for i, a in enumerate(passed)]
    outward = [pltpu.make_async_copy(carry.at[i], a, csem.at[1, i]) for i, a in enumerate(results)]
    weights = []
    for n, (band, count, blocks, chunks_of, _, _) in enumerate(plans):
        bufs, sems = rest[6 * n : 6 * n + 4], rest[6 * n + 4 : 6 * n + 6]
        weights.append(
            Weight(band, count, blocks, chunks_of, (total, ws[n], ms[n], grads[n], new_ws[n], new_ms[n]), bufs, sems)
        )
    most = max(w.count for w in weights)
    order = [(w, i) for i in range(most) for w in weights if i < w.count]
    for w, i in order:
        if i < 2:
            for c in w.loads(i):
                c.start()
    for c in inward:
        c.start()
    for n, (w, i) in enumerate(order):
        if n == 4:
            for a, b in zip(inward, outward):
                a.wait()
                b.start()
        if i >= 1 and i + 1 < w.count:
            for c in w.stores(i - 1):
                c.wait()
            for c in w.loads(i + 1):
                c.start()
        for c in w.loads(i):
            c.wait()
        w.compute(i)
        for c in w.stores(i):
            c.start()
    for w, i in order:
        if i + 2 >= w.count:
            for c in w.stores(i):
                c.wait()
    for c in outward:
        c.wait()


def adam_call(total, ws, ms, passed, hidden, shards):
    _, rows, model = total.shape
    plans = adam_plans(rows, model, hidden, shards)
    sds = jax.ShapeDtypeStruct
    scratch = []
    for band, _, _, _, parts, cols in plans:
        scratch += [
            pltpu.VMEM((2, parts, band, model), bf16),
            pltpu.VMEM((2, band, cols), f32),
            pltpu.VMEM((2, 2, band, cols), f32),
            pltpu.VMEM((2, band, cols), f32),
            DMA((2, 2 + parts)),
            DMA((2, 3)),
        ]
    scratch += [pltpu.VMEM((2, *passed[0].shape), passed[0].dtype), DMA((2, 2))]
    like = [sds(w.shape, f32) for w in ws]
    out = pl.pallas_call(
        functools.partial(adam_kernel, plans),
        out_shape=like + like + [sds(m.shape, f32) for m in ms] + [sds(a.shape, a.dtype) for a in passed],
        in_specs=[ANY] * 11,
        out_specs=[ANY] * 14,
        scratch_shapes=scratch,
        compiler_params=pltpu.CompilerParams(vmem_limit_bytes=60 << 20),
        name="adam",
    )(total, *ws, *ms, *passed)
    return out[:4], out[4:8], out[8:12], out[12:]


def local(mesh, tokens, cotangent, seg_ids, qkv, out, up, down, vectors, *moments):
    shards = mesh.shape["shard"]
    hidden = up.shape[1]
    grad_scale = (tokens.shape[0] * mesh.shape["replica"] * shards) ** (-0.5)
    _, _, total, block_output, input_grad, vshare = step_call(
        mesh, qkv, out, up, down, vectors, tokens, cotangent, seg_ids[None], grad_scale
    )
    grads, updated, renewed, (block_output, input_grad) = adam_call(
        total, (qkv, out, up, down), moments[:4], (block_output, input_grad), hidden, shards
    )
    vsum = vshare[0]
    new_v, *vm = adam(vectors, moments[4][0], moments[4][1], vsum, 0.0)
    return (block_output, input_grad, *grads, vsum, *updated, new_v, *renewed, jnp.stack(vm))


def solution(mesh):
    rows = P(("replica", "shard"), None)
    first, second = P("shard", None), P(None, "shard", None)
    weights, moments = (first,) * 4 + (P("shard"),), (second,) * 4 + (P(None, "shard"),)
    return jax.shard_map(
        functools.partial(local, mesh),
        mesh=mesh,
        in_specs=(rows, rows, P(("replica", "shard")), *weights, *moments),
        out_specs=(rows, rows, *weights, *weights, *moments),
        check_vma=False,
    )
```

```python
import functools
import math

import jax
import jax.numpy as jnp
from jax import lax
from jax.experimental import pallas as pl
from jax.experimental.pallas import tpu as pltpu
from jax.sharding import PartitionSpec as P

H = 4
ROT = 64
STEP = 3
norm_eps = 1e-05
rope_base = 10000.0
learn_rate = 0.01
beta_first = 0.9
beta_second = 0.95
adam_eps = 1e-08
weight_decay = 0.1
root_half = 0.7071067811865476
inv_root_tau = 0.3989422804014327

MESH = pl.DeviceIdType.MESH
f32, bf16 = jnp.float32, jnp.bfloat16
ANY = pl.BlockSpec(memory_space=pl.ANY)
VMEM = pl.BlockSpec(memory_space=pltpu.VMEM)
DMA = pltpu.SemaphoreType.DMA
TILE = 256
LANES = 128
PARTS = 2
SLOW, QUICK = 2, 1
RAW = 2
CAST = 64
EARLY = 5
TICKS_8 = 6
HEAD_TICKS = 1
LAG = 3
AHEAD = 3


class Place:
    def __init__(self, replicas, shards):
        self.replicas, self.shards = replicas, shards
        self.steps = int(math.log2(replicas)) - 1
        self.half = 2**self.steps
        self.r = lax.axis_index("replica")
        self.s = lax.axis_index("shard")
        self.core = self.r % 2
        self.m = self.mixed(self.r // 2)
        self.base = self.core * self.half
        self.twin_base = (1 - self.core) * self.half
        self.piece = self.base + self.m
        self.twin = (self.r + 1 - 2 * self.core, self.s)
        self.partner, self.mine, self.theirs = [], [], []
        for k in range(self.steps):
            flip = 2**k
            other = self.m + flip * (1 - 2 * ((self.m // flip) % 2))
            self.partner.append((2 * self.mixed(other) + self.core, self.s))
            self.mine.append((self.m // flip) * flip)
            self.theirs.append((other // flip) * flip)

    def mixed(self, plane):
        n = self.steps
        turned = sum(((plane // 2**i) % 2) * 2 ** (n - 1 - i) for i in range(n))
        return (1 - self.core) * plane + self.core * turned

    def across(self, d):
        return (self.r, (self.s + d) % self.shards)

    def source(self, d):
        return (self.s + self.shards - d) % self.shards

    def greet(self):
        barrier = pltpu.get_barrier_semaphore()
        peers = [self.across(d) for d in range(1, self.shards)] + self.partner + [self.twin]
        for peer in peers:
            pl.semaphore_signal(barrier, inc=1, device_id=peer, device_id_type=MESH)
        pl.semaphore_wait(barrier, len(peers))


def remote(src, dst, send, recv, peer):
    return pltpu.make_async_remote_copy(
        src_ref=src, dst_ref=dst, send_sem=send, recv_sem=recv, device_id=peer, device_id_type=MESH
    )


class Gather:
    def __init__(self, place, wg, send, recv):
        self.p, self.wg, self.send, self.recv = place, wg, send, recv
        self.chunks = wg.shape[0]
        self.rows = wg.shape[2] // place.replicas
        self.stages = place.steps + 2
        self.n = place.shards - 1
        self.units = self.chunks * self.n
        self.ticks = self.units + (self.stages - 1) * LAG

    def span(self, t, shard, first, count):
        start = pl.multiple_of(first * self.rows, self.rows)
        return self.wg.at[t, shard, pl.ds(start, count * self.rows), :]

    def copy(self, stage, t, d):
        p = self.p
        if stage == 0:
            ref, peer = self.span(t, p.s, p.piece, 1), p.across(d)
        elif stage <= p.steps:
            k = stage - 1
            ref, peer = self.span(t, p.source(d), p.base + p.mine[k], 2**k), p.partner[k]
        else:
            ref, peer = self.span(t, p.source(d), p.base, p.half), p.twin
        u = t * self.n + d - 1
        return remote(ref, ref, self.send.at[stage, u], self.recv.at[stage, u], peer)

    def launch(self, t):
        for d in range(1, self.n + 1):
            self.copy(0, t, d).start()

    def ready(self, t):
        return (t + 1) * self.n + (self.stages - 1) * LAG

    def tick(self, u):
        for stage in range(self.stages):
            v = u - stage * LAG

            @pl.when((v >= 0) & (v < self.units))
            def _(stage=stage, v=v):
                t, d = v // self.n, v % self.n + 1
                self.copy(stage, t, d).wait_recv()
                if stage + 1 < self.stages:
                    self.copy(stage + 1, t, d).start()

        @pl.when((u % self.n == self.n - 1) & (u // self.n + AHEAD < self.chunks))
        def _():
            self.launch(u // self.n + AHEAD)

    def finish(self):
        @pl.loop(0, self.chunks)
        def _(t):
            for d in range(1, self.n + 1):
                for stage in range(self.stages):
                    self.copy(stage, t, d).wait_send()


def dot(a, b, dims=((1,), (0,))):
    return lax.dot_general(a, b, (dims, ((), ())), preferred_element_type=f32)


def column(row):
    return jnp.broadcast_to(row.astype(f32), (8, row.shape[1])).T[:, :1]


def rotary_rows(seg, seg_row, start):
    shape = (seg.shape[0], seg_row.shape[1])
    row = lax.broadcasted_iota(jnp.int32, shape, 0) + start
    col = lax.broadcasted_iota(jnp.int32, shape, 1)
    before = (seg == seg_row.astype(f32)) & (col < row)
    position = jnp.sum(before.astype(f32), axis=1, keepdims=True)
    lane = lax.broadcasted_iota(jnp.int32, (1, LANES), 1)
    order = (lane % (ROT // 2)).astype(f32)
    angles = position * jnp.exp(order * (-2.0 / ROT * math.log(rope_base)))
    lane = lax.broadcasted_iota(jnp.int32, angles.shape, 1)
    cosine, sine = jnp.cos(angles), jnp.sin(angles)
    sine = jnp.where(lane < ROT // 2, -sine, sine)
    return jnp.where(lane < ROT, cosine, 1.0), jnp.where(lane < ROT, sine, 0.0)


def flat_columns(tile, j, rows, wide):
    per_tile = TILE // rows
    return [pl.multiple_of((tile * per_tile + i) * wide + j * rows, rows) for i in range(per_tile)]


def feed_forward(up, down, flats, rows, o_up, grad_scale, mlp_in, mlp_in_t, gout, vg, vgrad, mlp, gmlp, between, keep):
    bias = jnp.concatenate([vg[:, pl.ds(o_up + f, rows)] for f in flats], axis=1)
    h = dot(mlp_in[...], up) + bias
    cum = 0.5 * (1.0 + lax.erf(h * root_half))
    density = jnp.exp(-0.5 * h * h) * inv_root_tau
    act = (h * cum).astype(bf16)
    gh = dot(gout[...], down, ((1,), (1,))) * (cum + h * density)
    ghh = gh.astype(bf16)
    total = jnp.sum(gh, axis=0, keepdims=True) * grad_scale
    for i, f in enumerate(flats):
        vgrad[:, pl.ds(o_up + f, rows)] = total[:, i * rows : (i + 1) * rows]
    between()
    mlp[...] += dot(act, down)
    keep(1, (dot(act, gout[...], ((0,), (0,))) * grad_scale).astype(bf16))
    gmlp[...] += dot(ghh, up, ((1,), (1,)))
    keep(0, (dot(mlp_in_t[...], ghh) * grad_scale).astype(bf16))


def turned(x, cosines, sines, sign):
    first = x[:, :LANES]
    lane = lax.broadcasted_iota(jnp.int32, first.shape, 1)
    other = jnp.where(lane < ROT // 2, pltpu.roll(first, LANES - ROT // 2, 1), pltpu.roll(first, ROT // 2, 1))
    return jnp.concatenate([first * cosines + sign * (other * sines), x[:, LANES:]], axis=1)


def one_head(band, q, k, v, gctx, ctx, dq, dk, dv, seg_row, scale):
    dk[...] = jnp.zeros_like(dk)
    dv[...] = jnp.zeros_like(dv)
    for i in range(q.shape[0] // band):
        at, end = slice(i * band, (i + 1) * band), (i + 1) * band
        qi, gi, ki, vi = q[at, :], gctx[at, :], k[:end, :], v[:end, :]
        row = lax.broadcasted_iota(jnp.int32, (band, end), 0) + i * band
        col = lax.broadcasted_iota(jnp.int32, (band, end), 1)
        allowed = (column(seg_row[:, at]) == seg_row[:, :end].astype(f32)) & (col <= row)
        masked = jnp.where(allowed, dot(qi, ki, ((1,), (1,))) * scale, -jnp.inf)
        largest = jnp.max(masked, axis=1, keepdims=True)
        log_total = largest + jnp.log(jnp.sum(jnp.exp(masked - largest), axis=1, keepdims=True))
        prob = jnp.exp(masked - log_total)
        half = prob.astype(bf16)
        ctx[at, :] = dot(half, vi).astype(bf16)
        gp = dot(gi, vi, ((1,), (1,)))
        delta = jnp.sum(prob * gp, axis=1, keepdims=True)
        gs = (prob * (gp - delta) * scale).astype(bf16)
        dq[at, :] = dot(gs, ki)
        dk[:end, :] += dot(gs, qi, ((0,), (0,)))
        dv[:end, :] += dot(half, gi, ((0,), (0,)))


def reduce_lags(steps):
    lags = [0]
    for gap in [QUICK] * 2 + [SLOW] * (2 * steps + 2):
        lags.append(lags[-1] + gap)
    return lags


class Reduce:
    def __init__(self, place, grads, rc, total, acc, lo, r, rz, tp, sems):
        self.p, self.grads, self.rc, self.total = place, grads, rc, total
        self.acc, self.lo, self.r, self.rz, self.tp = acc, lo, r, rz, tp
        self.csem, self.ksem, self.zsem, self.gsem, self.lsem, self.tsem = sems
        self.cols = acc.shape[3]
        self.parts = total.shape[2] // self.cols
        self.rows = total.shape[1] // place.replicas
        self.units = total.shape[0] * self.parts
        self.n = place.shards - 1
        self.lags = reduce_lags(place.steps)
        self.stages = len(self.lags)
        self.ticks = self.units + self.lags[-1]

    def where(self, u):
        t, part = u // self.parts, u % self.parts
        return t, pl.ds(pl.multiple_of(part * self.cols, self.cols), self.cols)

    def band(self, first, count):
        return pl.ds(pl.multiple_of(first * self.rows, self.rows), count * self.rows)

    def loads(self, u):
        t, cols = self.where(u)
        a, b = u % self.acc.shape[0], u % self.lo.shape[0]
        own = self.grads.at[t, :, self.band(self.p.base, self.p.half), cols]
        return (
            pltpu.make_async_copy(self.rc.at[u], self.acc.at[a], self.lsem.at[0, a]),
            pltpu.make_async_copy(own, self.lo.at[b], self.lsem.at[1, b]),
        )

    def core_copy(self, u):
        t, cols = self.where(u)
        src = self.grads.at[t, :, self.band(self.p.twin_base, self.p.half), cols]
        return remote(src, self.rc.at[u], self.csem.at[0, u], self.csem.at[1, u], self.p.twin)

    def held(self, k, u):
        p = self.p
        return (self.acc.at[u % self.acc.shape[0]], 0) if k == p.steps else (self.r[k].at[u], p.mine[k])

    def plane_copy(self, k, u):
        ref, first = self.held(k + 1, u)
        src = ref.at[:, self.band(self.p.theirs[k] - first, 2**k), :]
        return remote(src, self.r[k].at[u], self.ksem.at[0, k, u], self.ksem.at[1, k, u], self.p.partner[k])

    def shard_copy(self, u, d):
        to = self.p.across(d)
        src = self.held(0, u)[0].at[to[1]]
        return remote(src, self.rz.at[u, d - 1], self.zsem.at[0, u, d - 1], self.zsem.at[1, u, d - 1], to)

    def piece_copy(self, u):
        t, cols = self.where(u)
        return pltpu.make_async_copy(self.tp.at[u], self.total.at[t, self.band(self.p.piece, 1), cols], self.tsem.at[u])

    def total_copy(self, k, u):
        p = self.p
        t, cols = self.where(u)
        first, count, peer = (
            (p.base + p.mine[k], 2**k, p.partner[k]) if k < p.steps else (p.base, p.half, p.twin)
        )
        ref = self.total.at[t, self.band(first, count), cols]
        return remote(ref if k else self.tp.at[u], ref, self.gsem.at[0, k, u], self.gsem.at[1, k, u], peer)

    def add(self, stage, u):
        p = self.p
        if stage == 1:
            self.core_copy(u).wait_recv()
            ring = self.acc.shape[0]

            @pl.when(u >= ring)
            def _():
                self.plane_copy(p.steps - 1, u - ring).wait_send()

            for c in self.loads(u):
                c.start()
        elif stage == 2:
            for c in self.loads(u):
                c.wait()
            a = u % self.acc.shape[0]
            self.acc[a] = self.acc[a] + self.lo[u % self.lo.shape[0]]
        elif 2 < stage < 3 + p.steps:
            k = p.steps - (stage - 2)
            self.plane_copy(k, u).wait_recv()
            ref, first = self.held(k + 1, u)
            self.r[k][u] = self.r[k][u] + ref[:, self.band(p.mine[k] - first, 2**k), :]
        elif stage == 3 + p.steps:
            for d in range(1, self.n + 1):
                self.shard_copy(u, d).wait_recv()
            acc = self.held(0, u)[0][p.s].astype(f32)
            for d in range(1, self.n + 1):
                acc += self.rz[u, d - 1].astype(f32)
            self.tp[u] = acc.astype(bf16)
        elif stage > 3 + p.steps:
            k = stage - 4 - p.steps
            self.total_copy(k, u).wait_recv()
            if k == 0:
                self.piece_copy(u).wait()

    def send(self, stage, u):
        p = self.p
        if stage == 0:
            self.core_copy(u).start()
        elif 2 <= stage < 2 + p.steps:
            self.plane_copy(p.steps - 1 - (stage - 2), u).start()
        elif stage == 2 + p.steps:
            for d in range(1, self.n + 1):
                self.shard_copy(u, d).start()
        elif 3 + p.steps <= stage < self.stages - 1:
            if stage == 3 + p.steps:
                self.piece_copy(u).start()
            self.total_copy(stage - 3 - p.steps, u).start()

    def tick(self, u):
        for do in (self.add, self.send):
            for stage in (range(self.stages) if do == self.add else reversed(range(self.stages))):
                v = u - self.lags[stage]

                @pl.when((v >= 0) & (v < self.units))
                def _(stage=stage, v=v):
                    do(stage, v)

        v = u - self.lags[-1] - 1

        @pl.when((v >= 0) & (v < self.units))
        def _():
            self.sent(v)

    def run(self, first, last):
        @pl.loop(first, last)
        def _(u):
            self.tick(u)

    def sent(self, u):
        self.core_copy(u).wait_send()
        for k in range(self.p.steps - 1):
            self.plane_copy(k, u).wait_send()

        @pl.when(u >= self.units - self.acc.shape[0])
        def _():
            self.plane_copy(self.p.steps - 1, u).wait_send()

        for d in range(1, self.n + 1):
            self.shard_copy(u, d).wait_send()
        for k in range(self.p.steps + 1):
            self.total_copy(k, u).wait_send()

    def finish(self):
        @pl.loop(self.units - 1, self.units)
        def _(u):
            self.sent(u)


def step_kernel(
    replicas, shards, hidden, grad_scale,
    qkv_w, out_w, up_w, down_w, cot, vec, tok, seg_row,
    grads, rc, total, bout, ig, vshare,
    wg, acc, lo, *rest,
):
    steps = int(math.log2(replicas)) - 1
    r, rest = rest[:steps], rest[steps:]
    rz, tp, x_in, x_in_t, gout, out_acc, gmlp, gattn, gtile, grows, cosines, sines, mean, inverse, *rest = rest
    qb, kb, vb, gb, ctx, dq, dk, dv, vg, vgrad, vz, vx, *rest = rest
    gsend, grecv, csem, ksem, zsem, tsem, lsem, psem, own_sem, ssem, vsem, vzsem, vxsem, isem = rest
    p = Place(replicas, shards)
    g = Gather(p, wg, gsend, grecv)
    red = Reduce(p, grads, rc, total, acc, lo, r, rz, tp, (csem, ksem, zsem, tsem, lsem, psem))
    chunks, _, rows, model = wg.shape
    tokens = tok.shape[0]
    ff_chunks = hidden // model
    tiles = model // TILE
    per_tile = TILE // rows
    head = model // H
    scale = head ** (-0.5)
    per_head = head // rows
    chunk0 = 2 * ff_chunks
    width = vec.shape[0]
    wide = hidden // shards
    o_out, o_up, o_down = 7 * model, 8 * model, 8 * model + hidden
    band = 64

    def start(copies):
        for c in copies:
            c.start()

    def wait(copies):
        for c in copies:
            c.wait()

    def bands(body):
        @pl.loop(0, tokens // band)
        def _(i):
            body(pl.ds(pl.multiple_of(i * band, band), band))

    def lanes(body):
        for i in range(tokens // LANES):
            body(slice(i * LANES, (i + 1) * LANES))

    def loads(t):
        slot, j = t % RAW, t // 2
        dst, sem = gattn.at[slot * rows : (slot + 1) * rows, :], own_sem.at[slot]
        if t >= chunk0:
            i = t - chunk0
            src = qkv_w.at[:, i * model : (i + 1) * model] if i < 3 else out_w
            return [pltpu.make_async_copy(src, dst, sem.at[0])]
        if t % 2:
            return [pltpu.make_async_copy(down_w.at[j * rows : (j + 1) * rows, :], dst, sem.at[0])]
        return [
            pltpu.make_async_copy(
                up_w.at[:, i * wide + j * rows : i * wide + (j + 1) * rows],
                dst.at[:, i * rows : (i + 1) * rows],
                sem.at[i],
            )
            for i in range(shards)
        ]

    def part(shard):
        return pl.ds(pl.multiple_of(shard * width, LANES), width)

    def gather_vec(d):
        ref = vg.at[:, part(p.s)]
        return remote(ref, ref, vsem.at[0, d - 1], vsem.at[1, d - 1], p.across(d))

    cot_copy = pltpu.make_async_copy(cot, gout, isem.at[0])
    for t in range(RAW):
        start(loads(t))
    cot_copy.start()
    vg[:, part(p.s)] = vec[...].reshape(1, width).astype(bf16).astype(f32)
    p.greet()
    start([gather_vec(d) for d in range(1, shards)])
    for t in range(chunks):
        wait(loads(t))

        @pl.loop(0, rows // CAST)
        def _(i, t=t):
            at = pl.multiple_of(i * CAST, CAST)
            wg[t, p.s, pl.ds(at, CAST), :] = gattn[pl.ds((t % RAW) * rows + at, CAST), :].astype(bf16)

        if t + RAW < chunks:
            start(loads(t + RAW))
        if 1 <= t <= AHEAD:
            g.launch(t - 1)
        if t == (AHEAD + chunks) // 2:
            g.tick(0)
    g.tick(1)

    def statistics(at):
        x = tok[at, :].astype(f32)
        m = jnp.mean(x, axis=1, keepdims=True)
        centred = x - m
        mean[at, :] = m
        inverse[at, :] = lax.rsqrt(jnp.mean(centred * centred, axis=1, keepdims=True) + norm_eps)

    def normed(at):
        return (tok[at, :].astype(f32) - mean[at, :]) * inverse[at, :]

    bands(statistics)
    g.tick(2)
    cot_copy.wait()

    def tables(at):
        seg = column(seg_row[:, at])
        gout[at, :] = (gout[at, :].astype(f32) * (seg >= 0.0).astype(f32)).astype(bf16)
        cosines[at, :], sines[at, :] = rotary_rows(seg, seg_row[...], at.start)

    for i in range(tokens // LANES):
        tables(slice(i * LANES, (i + 1) * LANES))
        if i % 2:
            g.tick(3 + i // 2)
    for d in range(1, shards):
        gather_vec(d).wait_recv()
    ticked = 3 + tokens // LANES // 2

    def enter_mlp(at):
        x_in[at, :] = (normed(at) * vg[:, 2 * model : 3 * model] + vg[:, 3 * model : 4 * model]).astype(bf16)
        bias = vg[:, o_down : o_down + model] + vg[:, o_out : o_out + model]
        out_acc[at, :] = tok[at, :].astype(f32) + bias
        gmlp[at, :] = jnp.zeros((band, model), f32)

    def turn(at):
        x_in_t[:, at] = x_in[at, :].T

    bands(enter_mlp)
    g.tick(ticked)
    lanes(turn)
    vgrad[...] = jnp.zeros_like(vgrad)

    first = g.ready(1)
    per_block = 2 * g.n

    @pl.loop(ticked + 1, first)
    def _(u):
        g.tick(u)

    def tile_stores(i):
        slot, j, n = i % 2, i // tiles, i % tiles
        cols = pl.ds(pl.multiple_of(n * TILE, TILE), TILE)
        return (
            pltpu.make_async_copy(gtile.at[slot, 0], grads.at[2 * j, :, :, cols], ssem.at[slot, 0]),
            pltpu.make_async_copy(
                grows.at[slot], grads.at[2 * j + 1, pl.ds(n * per_tile, per_tile)], ssem.at[slot, 3]
            ),
        )

    def head_stores(h):
        slot = h % 2
        cols = pl.ds(pl.multiple_of(h * head, head), head)
        out = [
            pltpu.make_async_copy(gtile.at[slot, w], grads.at[chunk0 + w, :, :, cols], ssem.at[slot, w])
            for w in range(3)
        ]
        last = grads.at[chunk0 + 3, pl.ds(h * per_head, per_head)]
        return (*out, pltpu.make_async_copy(grows.at[slot], last, ssem.at[slot, 3]))

    def reduced(i):
        return jnp.maximum(i - EARLY, 0) * TICKS_8 // 8

    @pl.loop(0, ff_chunks * tiles)
    def _(i):
        slot, j, n = i % 2, i // tiles, i % tiles
        lo_tick, hi_tick = first + (i * per_block) // tiles, first + ((i + 1) * per_block) // tiles
        most = -(-per_block // tiles)
        cols = pl.ds(pl.multiple_of(n * TILE, TILE), TILE)

        def maybe(a):
            @pl.when((lo_tick + a < hi_tick) & (lo_tick + a < g.ticks))
            def _():
                g.tick(lo_tick + a)

        @pl.when(i >= 2)
        def _():
            wait(tile_stores(i - 2))

        maybe(0)

        red.run(reduced(i), reduced(i + 1))

        def between():
            for a in range(1, most):
                maybe(a)

        def keep(which, x):
            if which:
                grows[slot] = x.reshape(per_tile, rows, model)
            else:
                gtile[slot, 0] = x.reshape(shards, rows, TILE)

        feed_forward(
            wg[2 * j, :, :, cols].reshape(model, TILE),
            wg[2 * j + 1, pl.ds(n * per_tile, per_tile)].reshape(TILE, model),
            flat_columns(n, j, rows, wide),
            rows, o_up, grad_scale, x_in, x_in_t, gout, vg, vgrad, out_acc, gmlp, between, keep,
        )
        start(tile_stores(i))

    items = ff_chunks * tiles
    done = max(items - EARLY, 0) * TICKS_8 // 8

    def enter_attention(at):
        x_in[at, :] = (normed(at) * vg[:, :model] + vg[:, model : 2 * model]).astype(bf16)
        gattn[at, :] = jnp.zeros((band, model), f32)

    bands(enter_attention)
    lanes(turn)

    @pl.loop(first + ff_chunks * per_block, g.ticks)
    def _(u):
        g.tick(u)

    @pl.loop(0, H)
    def _(h):
        slot = h % 2

        @pl.when(h < 2)
        def _():
            wait(tile_stores(items - 2 + h))

        @pl.when(h >= 2)
        def _():
            wait(head_stores(h - 2))

        red.run(done + 2 * HEAD_TICKS * h, done + 2 * HEAD_TICKS * h + HEAD_TICKS)
        cols = pl.ds(pl.multiple_of(h * head, head), head)
        mine = pl.ds(h * per_head, per_head)

        def weight(i):
            return wg[chunk0 + i, :, :, cols].reshape(model, head)

        def at_head(base):
            return pl.ds(pl.multiple_of(base + h * head, head), head)

        def project(i):
            return dot(x_in[...], weight(i)) + vg[:, at_head((4 + i) * model)]

        wo = wg[chunk0 + 3, mine].reshape(head, model)
        qb[...] = turned(project(0), cosines[...], sines[...], 1.0).astype(bf16)
        kb[...] = turned(project(1), cosines[...], sines[...], 1.0).astype(bf16)
        vb[...] = project(2).astype(bf16)
        gb[...] = dot(gout[...], wo, ((1,), (1,))).astype(bf16)
        one_head(LANES, qb, kb, vb, gb, ctx, dq, dk, dv, seg_row, scale)
        red.run(done + 2 * HEAD_TICKS * h + HEAD_TICKS, done + 2 * HEAD_TICKS * (h + 1))
        back = (
            turned(dq[...], cosines[...], sines[...], -1.0),
            turned(dk[...], cosines[...], sines[...], -1.0),
            dv[...],
        )
        sums = gattn[...]
        for i, d in enumerate(back):
            vgrad[:, at_head((4 + i) * model)] = jnp.sum(d, axis=0, keepdims=True) * grad_scale
            half = d.astype(bf16)
            sums += dot(half, weight(i), ((1,), (1,)))
            gtile[slot, i] = (dot(x_in_t[...], half) * grad_scale).astype(bf16).reshape(shards, rows, head)
        gattn[...] = sums
        out_acc[...] += dot(ctx[...], wo)
        grows[slot] = (
            (dot(ctx[...], gout[...], ((0,), (0,))) * grad_scale).astype(bf16).reshape(per_head, rows, model)
        )
        start(head_stores(h))

    done += 2 * HEAD_TICKS * H
    gain_one, gain_two = vg[:, :model], vg[:, 2 * model : 3 * model]

    def last(i, carry):
        at = pl.ds(pl.multiple_of(i * band, band), band)
        x, ga, gm, go = normed(at), gattn[at, :], gmlp[at, :], gout[at, :].astype(f32)
        gn = ga * gain_one + gm * gain_two
        m1 = jnp.mean(gn, axis=1, keepdims=True)
        m2 = jnp.mean(gn * x, axis=1, keepdims=True)
        gout[at, :] = (go + inverse[at, :] * (gn - m1 - x * m2)).astype(bf16)
        terms = (ga * x, ga, gm * x, gm, go)
        return tuple(a + jnp.sum(b, axis=0, keepdims=True) for a, b in zip(carry, terms))

    zero = jnp.zeros((1, model), f32)
    sums = lax.fori_loop(0, tokens // band, last, (zero,) * 5)
    for x, place in zip((*sums, sums[4]), (0, model, 2 * model, 3 * model, o_out, o_down)):
        vgrad[:, place : place + model] = x * grad_scale

    def leave(at):
        live = (column(seg_row[:, at]) >= 0.0).astype(f32)
        x_in[at, :] = (live * out_acc[at, :]).astype(bf16)

    lanes(leave)
    vgrad[...] = vgrad[...].astype(bf16).astype(f32)
    results = (pltpu.make_async_copy(x_in, bout, isem.at[0]), pltpu.make_async_copy(gout, ig, isem.at[1]))
    start(results)
    for h in range(H - 2, H):
        wait(head_stores(h))

    def vcopy(d):
        to = p.across(d)
        return remote(vgrad.at[:, part(to[1])], vz.at[d - 1], vzsem.at[0, d - 1], vzsem.at[1, d - 1], to)

    peers = [*p.partner, p.twin]

    def vexchange(k):
        return remote(vx.at[2 * k], vx.at[2 * k + 1], vxsem.at[0, k], vxsem.at[1, k], peers[k])

    def vstart(i):
        start([vcopy(d) for d in range(1, shards)] if i == 0 else [vexchange(i - 1)])

    def vfinish(i):
        if i == 0:
            acc = vgrad[:, part(p.s)]
            for d in range(1, shards):
                vcopy(d).wait_recv()
                acc += vz[d - 1]
        else:
            vexchange(i - 1).wait_recv()
            acc = vx[2 * i - 2] + vx[2 * i - 1]
        if i < len(peers):
            vx[2 * i] = acc
        else:
            vshare[...] = acc

    for i in range(len(peers) + 1):
        vstart(i)
        red.run(done + i, done + i + 1)
        vfinish(i)
    done += len(peers) + 1
    red.run(done, done + 4)
    g.finish()
    red.run(done + 4, red.ticks)
    for d in range(1, shards):
        gather_vec(d).wait_send()
        vcopy(d).wait_send()
    for i in range(len(peers)):
        vexchange(i).wait_send()
    red.finish()
    wait(results)


def step_call(mesh, qkv, out, up, down, vec, tok, cot, seg_row, grad_scale):
    replicas, shards = mesh.shape["replica"], mesh.shape["shard"]
    rows, hidden = up.shape
    tokens, model = tok.shape
    chunks = 2 * (hidden // model) + 4
    steps = int(math.log2(replicas)) - 1
    stages = steps + 2
    width = vec.shape[0]
    gather_units = chunks * (shards - 1)
    units, cols, piece = chunks * PARTS, model // PARTS, rows // replicas
    part = 2**steps * piece
    head = model // H
    lags = reduce_lags(steps)
    sds, vm = jax.ShapeDtypeStruct, pltpu.VMEM
    return pl.pallas_call(
        functools.partial(step_kernel, replicas, shards, hidden, grad_scale),
        out_shape=[
            sds((chunks, shards, rows, model), bf16),
            sds((units, shards, part, cols), bf16),
            sds((chunks, rows, model), bf16),
            sds((tokens, model), bf16),
            sds((tokens, model), bf16),
            sds((1, width), f32),
        ],
        in_specs=[ANY] * 5 + [VMEM] * 3,
        out_specs=[ANY] * 5 + [VMEM],
        scratch_shapes=[
            vm((chunks, shards, rows, model), bf16),
            vm((lags[3] - lags[1] + 1, shards, part, cols), bf16),
            vm((lags[2] - lags[1] + 1, shards, part, cols), bf16),
            *(vm((units, shards, 2**k * piece, cols), bf16) for k in range(steps)),
            vm((units, shards - 1, piece, cols), bf16),
            vm((units, piece, cols), bf16),
            vm((tokens, model), bf16),
            vm((model, tokens), bf16),
            vm((tokens, model), bf16),
            *[vm((tokens, model), f32)] * 3,
            vm((2, 3, shards, rows, head), bf16),
            vm((2, head // rows, rows, model), bf16),
            *[vm((tokens, LANES), f32)] * 2,
            *[vm((tokens, 1), f32)] * 2,
            *[vm((tokens, head), bf16)] * 5,
            *[vm((tokens, head), f32)] * 3,
            *[vm((1, width * shards), f32)] * 2,
            vm((shards - 1, 1, width), f32),
            vm((2 * steps + 2, 1, width), f32),
            DMA((stages, gather_units)),
            DMA((stages, gather_units)),
            DMA((2, units)),
            DMA((2, steps, units)),
            DMA((2, units, shards - 1)),
            DMA((2, steps + 1, units)),
            DMA((2, lags[3] - lags[1] + 1)),
            DMA((units,)),
            DMA((RAW, shards)),
            DMA((2, 4)),
            DMA((2, shards - 1)),
            DMA((2, shards - 1)),
            DMA((2, steps + 1)),
            DMA((2,)),
        ],
        compiler_params=pltpu.CompilerParams(
            collective_id=0, has_side_effects=True, vmem_limit_bytes=67043328
        ),
        name="step",
    )(qkv, out, up, down, cot, vec, tok, seg_row)


def adam(master, first, second, gradient, decay):
    first = beta_first * first + (1.0 - beta_first) * gradient
    second = beta_second * second + (1.0 - beta_second) * gradient * gradient
    a = first / (1.0 - beta_first**STEP)
    b = second / (1.0 - beta_second**STEP)
    return master - learn_rate * (a / (jnp.sqrt(b) + adam_eps) + decay * master), first, second


class Weight:
    def __init__(self, band, count, blocks, chunks_of, refs, bufs, sems):
        self.band, self.count, self.blocks, self.chunks_of = band, count, blocks, chunks_of
        self.total, self.w, self.m, self.grad, self.new_w, self.new_m = refs
        self.gbuf, self.wbuf, self.mbuf, self.outbuf = bufs
        self.isem, self.osem = sems

    def loads(self, i):
        slot, at = i % 2, slice(i * self.band, (i + 1) * self.band)
        pairs = [(self.w.at[at, :], self.wbuf.at[slot]), (self.m.at[:, at, :], self.mbuf.at[slot])]
        for n, (chunk, row) in enumerate(self.chunks_of(i)):
            pairs.append((self.total.at[chunk, row : row + self.band, :], self.gbuf.at[slot, n]))
        return [pltpu.make_async_copy(a, b, self.isem.at[slot, n]) for n, (a, b) in enumerate(pairs)]

    def stores(self, i):
        slot, at = i % 2, slice(i * self.band, (i + 1) * self.band)
        pairs = [
            (self.wbuf.at[slot], self.new_w.at[at, :]),
            (self.mbuf.at[slot], self.new_m.at[:, at, :]),
            (self.outbuf.at[slot], self.grad.at[at, :]),
        ]
        return [pltpu.make_async_copy(a, b, self.osem.at[slot, n]) for n, (a, b) in enumerate(pairs)]

    def compute(self, i):
        slot = i % 2
        for col, width, n, gcol in self.blocks:
            high = min(self.band, max(16, 16384 // width))

            @pl.loop(0, self.band // high)
            def _(b, col=col, width=width, n=n, gcol=gcol, high=high):
                at, cols = pl.ds(pl.multiple_of(b * high, high), high), slice(col, col + width)
                g = self.gbuf[slot, n, at, gcol : gcol + width].astype(f32)
                self.outbuf[slot, at, cols] = g
                w, first, second = adam(
                    self.wbuf[slot, at, cols], self.mbuf[slot, 0, at, cols], self.mbuf[slot, 1, at, cols], g, weight_decay
                )
                self.wbuf[slot, at, cols] = w
                self.mbuf[slot, 0, at, cols] = first
                self.mbuf[slot, 1, at, cols] = second


def adam_plans(rows, model, hidden, shards):
    ff = hidden // model
    wide = hidden // shards
    band = min(rows, 64)
    return (
        (band, rows // band, [(i * model, model, i, 0) for i in range(3)],
         lambda b: [(2 * ff + i, b * band) for i in range(3)], 3, 3 * model),
        (rows, 1, [(0, model, 0, 0)], lambda b: [(2 * ff + 3, 0)], 1, model),
        (band, rows // band,
         [(i * wide + j * rows, rows, j, i * rows) for i in range(shards) for j in range(ff)],
         lambda b: [(2 * j, b * band) for j in range(ff)], ff, hidden),
        (rows, ff, [(0, model, 0, 0)], lambda b: [(2 * b + 1, 0)], 1, model),
    )


def adam_kernel(plans, total, *refs):
    ws, ms, passed, refs = refs[:4], refs[4:8], refs[8:10], refs[10:]
    grads, new_ws, new_ms, results, rest = refs[:4], refs[4:8], refs[8:12], refs[12:14], refs[14:]
    carry, csem = rest[-2:]
    inward = [pltpu.make_async_copy(a, carry.at[i], csem.at[0, i]) for i, a in enumerate(passed)]
    outward = [pltpu.make_async_copy(carry.at[i], a, csem.at[1, i]) for i, a in enumerate(results)]
    weights = []
    for n, (band, count, blocks, chunks_of, _, _) in enumerate(plans):
        bufs, sems = rest[6 * n : 6 * n + 4], rest[6 * n + 4 : 6 * n + 6]
        weights.append(
            Weight(band, count, blocks, chunks_of, (total, ws[n], ms[n], grads[n], new_ws[n], new_ms[n]), bufs, sems)
        )
    most = max(w.count for w in weights)
    order = [(w, i) for i in range(most) for w in weights if i < w.count]
    for w, i in order:
        if i < 2:
            for c in w.loads(i):
                c.start()
    for c in inward:
        c.start()
    for n, (w, i) in enumerate(order):
        if n == 4:
            for a, b in zip(inward, outward):
                a.wait()
                b.start()
        if i >= 1 and i + 1 < w.count:
            for c in w.stores(i - 1):
                c.wait()
            for c in w.loads(i + 1):
                c.start()
        for c in w.loads(i):
            c.wait()
        w.compute(i)
        for c in w.stores(i):
            c.start()
    for w, i in order:
        if i + 2 >= w.count:
            for c in w.stores(i):
                c.wait()
    for c in outward:
        c.wait()


def adam_call(total, ws, ms, passed, hidden, shards):
    _, rows, model = total.shape
    plans = adam_plans(rows, model, hidden, shards)
    sds = jax.ShapeDtypeStruct
    scratch = []
    for band, _, _, _, parts, cols in plans:
        scratch += [
            pltpu.VMEM((2, parts, band, model), bf16),
            pltpu.VMEM((2, band, cols), f32),
            pltpu.VMEM((2, 2, band, cols), f32),
            pltpu.VMEM((2, band, cols), f32),
            DMA((2, 2 + parts)),
            DMA((2, 3)),
        ]
    scratch += [pltpu.VMEM((2, *passed[0].shape), passed[0].dtype), DMA((2, 2))]
    like = [sds(w.shape, f32) for w in ws]
    out = pl.pallas_call(
        functools.partial(adam_kernel, plans),
        out_shape=like + like + [sds(m.shape, f32) for m in ms] + [sds(a.shape, a.dtype) for a in passed],
        in_specs=[ANY] * 11,
        out_specs=[ANY] * 14,
        scratch_shapes=scratch,
        compiler_params=pltpu.CompilerParams(vmem_limit_bytes=60 << 20),
        name="adam",
    )(total, *ws, *ms, *passed)
    return out[:4], out[4:8], out[8:12], out[12:]


def local(mesh, tokens, cotangent, seg_ids, qkv, out, up, down, vectors, *moments):
    shards = mesh.shape["shard"]
    hidden = up.shape[1]
    grad_scale = (tokens.shape[0] * mesh.shape["replica"] * shards) ** (-0.5)
    _, _, total, block_output, input_grad, vshare = step_call(
        mesh, qkv, out, up, down, vectors, tokens, cotangent, seg_ids[None], grad_scale
    )
    grads, updated, renewed, (block_output, input_grad) = adam_call(
        total, (qkv, out, up, down), moments[:4], (block_output, input_grad), hidden, shards
    )
    vsum = vshare[0]
    new_v, *vm = adam(vectors, moments[4][0], moments[4][1], vsum, 0.0)
    return (block_output, input_grad, *grads, vsum, *updated, new_v, *renewed, jnp.stack(vm))


def solution(mesh):
    rows = P(("replica", "shard"), None)
    first, second = P("shard", None), P(None, "shard", None)
    weights, moments = (first,) * 4 + (P("shard"),), (second,) * 4 + (P(None, "shard"),)
    return jax.shard_map(
        functools.partial(local, mesh),
        mesh=mesh,
        in_specs=(rows, rows, P(("replica", "shard")), *weights, *moments),
        out_specs=(rows, rows, *weights, *weights, *moments),
        check_vma=False,
    )
```
